32 devices in a mesh: data: 1 (over z), model: 32 (over y, x, core).
Axes of the slice: x: 4, y: 4, z: 1, core: 2. Of those that a mesh axis runs over, the one named last changes fastest.
The devices are a block of a 4x4x8 slice.
Arguments:
- x_in: bfloat16 [1, 4096, 2048], P('data')
- seg_ids: int32 [1, 4096], P('data')
- gain_one: bfloat16 [2048], replicated
- w_qkv: bfloat16 [2048, 6144], P(None, 'model')
- w_out: bfloat16 [32, 64, 2048], P('model')
- gain_two: bfloat16 [2048], replicated
- w_up: bfloat16 [2048, 8192], P(None, 'model')
- w_down: bfloat16 [8192, 2048], P('model')
- d_y: bfloat16 [1, 4096, 2048], P('data')
Outputs:
- output 1: bfloat16 [1, 4096, 2048], P('data')
- output 2: bfloat16 [1, 4096, 2048], P('data')
- output 3: bfloat16 [2048, 6144], P('data', 'model')
- output 4: bfloat16 [32, 64, 2048], P(('data', 'model'))
- output 5: bfloat16 [2048, 8192], P('data', 'model')
- output 6: bfloat16 [8192, 2048], P(('data', 'model'))
- output 7: bfloat16 [2048], P('data')
- output 8: bfloat16 [2048], P('data')
All inputs are finite; a program needn't handle non-finite values.
Results may differ from the reference program's by a relative error of at most 0.02.
Values are sent between devices in bfloat16 or wider.
A program may use at most 768 MiB of HBM per device.

```python
import jax
import jax.numpy as jnp
from jax import lax

BATCH_ROWS = 1
SEQ_LEN = 4096
MODEL_DIM = 2048
NUM_HEADS = 32
HEAD_DIM = 64
FFN_DIM = 8192
LN_EPS = 1e-5
TOKEN_COUNT = BATCH_ROWS * SEQ_LEN
QKV_WIDTH = 3 * NUM_HEADS * HEAD_DIM
INNER_WIDTH = NUM_HEADS * HEAD_DIM


def draw_segments(seg_key):
    seg_keys = jax.random.split(seg_key, 3)
    rate_table = jnp.array([0, 2, 8, 32], jnp.int32)
    row_rate = rate_table[jax.random.randint(seg_keys[0], (BATCH_ROWS,), 0, 4)]
    pos_draws = jax.random.randint(seg_keys[1], (BATCH_ROWS, SEQ_LEN), 0, SEQ_LEN)
    forced_pos = jax.random.randint(seg_keys[2], (BATCH_ROWS,), 1, SEQ_LEN)
    positions = jnp.arange(SEQ_LEN, dtype=jnp.int32)
    breaks = ((pos_draws < row_rate[:, None]) | (positions[None, :] == forced_pos[:, None])).astype(jnp.int32)
    breaks = breaks.at[:, 0].set(0)
    return jnp.cumsum(breaks, axis=1).astype(jnp.int32)


def setup_inputs(seed: int = 0, part: int = 0) -> dict:
    base_key = jax.random.key(seed)
    part_key = jax.random.fold_in(base_key, part)
    weight_keys = jax.random.split(base_key, 6)
    part_keys = jax.random.split(part_key, 4)
    x_in = jax.random.normal(part_keys[0], (BATCH_ROWS, SEQ_LEN, MODEL_DIM), jnp.float32)
    seg_ids = draw_segments(part_keys[1])
    gain_one = 1.0 + 0.3 * jax.random.normal(weight_keys[0], (MODEL_DIM,), jnp.float32)
    gain_two = 1.0 + 0.3 * jax.random.normal(weight_keys[1], (MODEL_DIM,), jnp.float32)
    w_qkv = jax.random.normal(weight_keys[2], (MODEL_DIM, QKV_WIDTH), jnp.float32) * (1.5 * MODEL_DIM ** -0.5)
    w_out = jax.random.normal(weight_keys[3], (NUM_HEADS, HEAD_DIM, MODEL_DIM), jnp.float32) * INNER_WIDTH ** -0.5
    w_up = jax.random.normal(weight_keys[4], (MODEL_DIM, FFN_DIM), jnp.float32) * MODEL_DIM ** -0.5
    w_down = jax.random.normal(weight_keys[5], (FFN_DIM, MODEL_DIM), jnp.float32) * FFN_DIM ** -0.5
    d_y = jax.random.normal(part_keys[3], (BATCH_ROWS, SEQ_LEN, MODEL_DIM), jnp.float32)
    return {'x_in': x_in.astype(jnp.bfloat16), 'seg_ids': seg_ids, 'gain_one': gain_one.astype(jnp.bfloat16), 'w_qkv': w_qkv.astype(jnp.bfloat16), 'w_out': w_out.astype(jnp.bfloat16), 'gain_two': gain_two.astype(jnp.bfloat16), 'w_up': w_up.astype(jnp.bfloat16), 'w_down': w_down.astype(jnp.bfloat16), 'd_y': d_y.astype(jnp.bfloat16)}


def layer_norm(x_in, gain):
    x_wide = x_in.astype(jnp.float32)
    row_mean = jnp.mean(x_wide, axis=-1, keepdims=True)
    centered = x_wide - row_mean
    row_var = jnp.mean(centered * centered, axis=-1, keepdims=True)
    return (centered * lax.rsqrt(row_var + LN_EPS) * gain.astype(jnp.float32)).astype(jnp.bfloat16)


def head_attention(q_head, k_head, v_head, seg_ids):
    positions = jnp.arange(SEQ_LEN)
    allowed = (positions[:, None] >= positions[None, :])[None] & (seg_ids[:, :, None] == seg_ids[:, None, :])
    scores = jnp.einsum('bqd,bkd->bqk', q_head.astype(jnp.float32), k_head.astype(jnp.float32)) * (HEAD_DIM ** -0.5)
    scores = jnp.where(allowed, scores, -1e30)
    attn_prob = jax.nn.softmax(scores, axis=-1).astype(jnp.bfloat16)
    result = jnp.einsum('bqk,bkd->bqd', attn_prob.astype(jnp.float32), v_head.astype(jnp.float32))
    return result.astype(jnp.bfloat16)


def layer_forward(x_in, seg_ids, gain_one, w_qkv, w_out, gain_two, w_up, w_down):
    x_flat = x_in.reshape(TOKEN_COUNT, MODEL_DIM)
    normed_one = layer_norm(x_flat, gain_one)
    qkv_proj = jnp.dot(normed_one, w_qkv, preferred_element_type=jnp.float32).astype(jnp.bfloat16)
    qkv_heads = jnp.moveaxis(qkv_proj.reshape(BATCH_ROWS, SEQ_LEN, NUM_HEADS, 3, HEAD_DIM), 2, 0)

    def one_head(head_qkv):
        return head_attention(head_qkv[:, :, 0], head_qkv[:, :, 1], head_qkv[:, :, 2], seg_ids)

    attn_heads = lax.map(jax.checkpoint(one_head), qkv_heads)
    attn_flat = jnp.moveaxis(attn_heads, 0, 2).reshape(TOKEN_COUNT, INNER_WIDTH)
    proj_one = jnp.dot(attn_flat, w_out.reshape(INNER_WIDTH, MODEL_DIM), preferred_element_type=jnp.float32)
    resid = (x_flat.astype(jnp.float32) + proj_one).astype(jnp.bfloat16)
    normed_two = layer_norm(resid, gain_two)
    up_proj = jnp.dot(normed_two, w_up, preferred_element_type=jnp.float32).astype(jnp.bfloat16)
    gelu_out = jax.nn.gelu(up_proj.astype(jnp.float32), approximate=True).astype(jnp.bfloat16)
    proj_two = jnp.dot(gelu_out, w_down, preferred_element_type=jnp.float32)
    y_flat = (resid.astype(jnp.float32) + proj_two).astype(jnp.bfloat16)
    return y_flat.reshape(BATCH_ROWS, SEQ_LEN, MODEL_DIM)


def reference(x_in, seg_ids, gain_one, w_qkv, w_out, gain_two, w_up, w_down, d_y):
    def forward_fn(x_arg, g_one, wq_arg, wo_arg, g_two, wu_arg, wd_arg):
        return layer_forward(x_arg, seg_ids, g_one, wq_arg, wo_arg, g_two, wu_arg, wd_arg)

    y_out, pullback = jax.vjp(forward_fn, x_in, gain_one, w_qkv, w_out, gain_two, w_up, w_down)
    d_x, d_gain_one, d_w_qkv, d_w_out, d_gain_two, d_w_up, d_w_down = pullback(d_y)
    return (y_out, d_x, d_w_qkv, d_w_out, d_w_up, d_w_down, d_gain_one, d_gain_two)
```

```python
import functools

import jax
import jax.numpy as jnp
from jax import lax
from jax.experimental import pallas as pl
from jax.experimental.pallas import tpu as pltpu
from jax.sharding import PartitionSpec as P

LN_EPS = 1e-5
LOG2E = 1.4426950408889634
NEG = -1e30
MESH = pl.DeviceIdType.MESH
VMEM_LIMIT = 60 * 1024 * 1024
F32 = jnp.float32
BF16 = jnp.bfloat16


def mm(a, b, ca, cb):
    return lax.dot_general(a, b, (((ca,), (cb,)), ((), ())), preferred_element_type=F32)


def ln_qkv_kernel(x_ref, g_ref, w_ref, a_ref, q_ref, k_ref, v_ref, t_ref):
    x = x_ref[...].astype(F32)
    mean = jnp.mean(x, axis=-1, keepdims=True)
    cen = x - mean
    var = jnp.mean(cen * cen, axis=-1, keepdims=True)
    a = (cen * lax.rsqrt(var + LN_EPS) * g_ref[...].astype(F32)).astype(BF16)
    a_ref[...] = a
    qkv = mm(a, w_ref[...], 1, 1)
    t_ref[...] = qkv.T.astype(BF16)
    hd = q_ref.shape[1]
    qkv = qkv.astype(BF16)
    q_ref[...] = qkv[:, :hd]
    k_ref[...] = qkv[:, hd:2 * hd]
    v_ref[...] = qkv[:, 2 * hd:]


def ln_qkv(x, g, w):
    t, h = x.shape
    c = w.shape[0]
    hd = c // 3
    bt = min(512, t)
    row = lambda n: pl.BlockSpec((bt, n), lambda i: (i, 0))
    return pl.pallas_call(
        ln_qkv_kernel,
        grid=(t // bt,),
        in_specs=[row(h), pl.BlockSpec((1, h), lambda i: (0, 0)), pl.BlockSpec((c, h), lambda i: (0, 0))],
        out_specs=[row(h), row(hd), row(hd), row(hd), pl.BlockSpec((c, bt), lambda i: (0, i))],
        out_shape=[jax.ShapeDtypeStruct((t, h), BF16)] + [jax.ShapeDtypeStruct((t, hd), BF16)] * 3 + [jax.ShapeDtypeStruct((c, t), BF16)],
        compiler_params=pltpu.CompilerParams(vmem_limit_bytes=VMEM_LIMIT),
        cost_estimate=pl.CostEstimate(flops=2 * t * h * c + 20 * t * h, bytes_accessed=4 * t * h, transcendentals=0),
        name='ln_qkv',
    )(x, g.reshape(1, h), w)


def visible(kb, bk, q0, bq, start):
    k_pos = kb * bk + lax.broadcasted_iota(jnp.int32, (bk, bq), 0)
    q_pos = q0 + lax.broadcasted_iota(jnp.int32, (bk, bq), 1)
    return (k_pos <= q_pos) & (k_pos >= start)


def attn_fwd_kernel(bk, tab_ref, k_ref, qt_ref, vt_ref, start_ref, ot_ref, lse_ref):
    i = pl.program_id(0)
    bq = qt_ref.shape[1]
    hd = qt_ref.shape[0]
    scale = LOG2E * hd ** -0.5
    qt = qt_ref[...]
    start = start_ref[...]
    lo, mid, hi, top = tab_ref[0, i], tab_ref[1, i], tab_ref[2, i], tab_ref[3, i]

    def step(masked, kb, carry):
        m, l, acc = carry
        k0 = pl.multiple_of(kb * bk, bk)
        s = mm(k_ref[pl.ds(k0, bk), :], qt, 1, 0)
        if masked:
            s = jnp.where(visible(kb, bk, i * bq, bq, start), s, NEG)
        m_new = jnp.maximum(m, jnp.max(s, axis=0, keepdims=True))
        p = jnp.exp2((s - m_new) * scale)
        alpha = jnp.exp2((m - m_new) * scale)
        l = l * alpha + jnp.sum(p, axis=0, keepdims=True)
        acc = acc * alpha + mm(vt_ref[:, pl.ds(k0, bk)], p.astype(BF16), 1, 0)
        return m_new, l, acc

    carry = (jnp.full((1, bq), NEG, F32), jnp.zeros((1, bq), F32), jnp.zeros((hd, bq), F32))
    carry = lax.fori_loop(lo, mid, functools.partial(step, True), carry)
    carry = lax.fori_loop(mid, hi, functools.partial(step, False), carry)
    m, l, acc = lax.fori_loop(hi, top, functools.partial(step, True), carry)
    ot_ref[...] = (acc / l).astype(BF16)
    lse_ref[...] = m * scale + jnp.log2(l)


def document_starts(seg):
    t = seg.shape[0]
    wide = 128
    pos = jnp.arange(t, dtype=jnp.int32).reshape(t // wide, wide)
    before = jnp.concatenate([seg[:1], seg[:-1]])
    mark = jnp.where((seg != before).reshape(pos.shape), pos, 0)
    lane = jnp.arange(wide)
    inner = jnp.max(jnp.where(lane[None, :, None] >= lane[None, None, :], mark[:, None, :], 0), axis=-1)
    row = jnp.arange(t // wide)
    prior = jnp.max(jnp.where(row[:, None] > row[None, :], inner[:, -1][None, :], 0), axis=-1)
    return jnp.maximum(inner, prior[:, None]).reshape(t)


def block_table(seg, start, bq, bk):
    t = seg.shape[0]
    nq = t // bq
    q0 = jnp.arange(nq, dtype=jnp.int32) * bq
    first = start.reshape(nq, bq)[:, 0]
    last = start.reshape(nq, bq)[:, -1]
    lo = first // bk
    hi = q0 // bk
    top = (q0 + bq + bk - 1) // bk
    mid = jnp.clip((last + bk - 1) // bk, lo, hi)
    return jnp.stack([lo, mid, hi, top])


def attention_forward(k, qkvt, start, tab, bq, bk):
    t, hd = k.shape
    return pl.pallas_call(
        functools.partial(attn_fwd_kernel, bk),
        grid_spec=pltpu.PrefetchScalarGridSpec(
            num_scalar_prefetch=1,
            grid=(t // bq,),
            in_specs=[
                pl.BlockSpec((t, hd), lambda i, *_: (0, 0)),
                pl.BlockSpec((hd, bq), lambda i, *_: (0, i)),
                pl.BlockSpec((hd, t), lambda i, *_: (2, 0)),
                pl.BlockSpec((1, bq), lambda i, *_: (0, i)),
            ],
            out_specs=[pl.BlockSpec((hd, bq), lambda i, *_: (0, i)), pl.BlockSpec((1, bq), lambda i, *_: (0, i))],
        ),
        out_shape=[jax.ShapeDtypeStruct((hd, t), BF16), jax.ShapeDtypeStruct((1, t), F32)],
        compiler_params=pltpu.CompilerParams(vmem_limit_bytes=VMEM_LIMIT),
        cost_estimate=pl.CostEstimate(flops=16 * t * t * hd, bytes_accessed=8 * t * hd, transcendentals=t * t // 2),
        name='attn_fwd',
    )(tab, k, qkvt, qkvt, start)


def attn_bwd_kernel(bk, tab_ref, q_ref, k_ref, v_ref, t_ref, ot_ref, dot_ref, lse_ref, start_ref, d_ref, dk_acc, dv_acc):
    i = pl.program_id(0)
    bq, hd = q_ref.shape
    scale = LOG2E * hd ** -0.5
    t = k_ref.shape[0]

    @pl.when(i == 0)
    def _():
        dk_acc[...] = jnp.zeros_like(dk_acc)
        dv_acc[...] = jnp.zeros_like(dv_acc)

    c0 = pl.multiple_of(i * bq, bq)
    q = q_ref[...]
    qt = t_ref[:hd, pl.ds(c0, bq)]
    dot_blk = dot_ref[...]
    dot_wide = dot_blk.astype(F32)
    d_out = dot_wide.T.astype(BF16)
    delta = jnp.sum(dot_wide * ot_ref[...].astype(F32), axis=0, keepdims=True)
    lse = lse_ref[...]
    start = start_ref[...]
    lo, mid, hi, top = tab_ref[0, i], tab_ref[1, i], tab_ref[2, i], tab_ref[3, i]

    def step(masked, kb, dqt):
        k0 = pl.multiple_of(kb * bk, bk)
        rows = pl.ds(k0, bk)
        s = mm(k_ref[rows, :], qt, 1, 0)
        p = jnp.exp2(s * scale - lse)
        if masked:
            p = jnp.where(visible(kb, bk, i * bq, bq, start), p, 0.0)
        dp = mm(v_ref[rows, :], dot_blk, 1, 0)
        ds = (p * (dp - delta)).astype(BF16)
        dv_acc[rows, :] += mm(p.astype(BF16), d_out, 1, 0)
        dk_acc[rows, :] += mm(ds, q, 1, 0)
        return dqt + mm(t_ref[hd:2 * hd, rows], ds, 1, 0)

    dqt = jnp.zeros((hd, bq), F32)
    dqt = lax.fori_loop(lo, mid, functools.partial(step, True), dqt)
    dqt = lax.fori_loop(mid, hi, functools.partial(step, False), dqt)
    dqt = lax.fori_loop(hi, top, functools.partial(step, True), dqt)
    d_ref[pl.ds(c0, bq), :hd] = (dqt * hd ** -0.5).T.astype(BF16)

    @pl.when(i == pl.num_programs(0) - 1)
    def _():
        def put(r, _):
            rows = pl.ds(pl.multiple_of(r * bk, bk), bk)
            d_ref[rows, hd:2 * hd] = (dk_acc[rows, :] * hd ** -0.5).astype(BF16)
            d_ref[rows, 2 * hd:] = dv_acc[rows, :].astype(BF16)
            return 0

        lax.fori_loop(0, t // bk, put, 0)


def attention_backward(q, k, v, qkvt, ot, dot, lse, start, tab, bq, bk):
    t, hd = k.shape
    whole = lambda shape: pl.BlockSpec(shape, lambda i, *_: (0, 0))
    cols = lambda n: pl.BlockSpec((n, bq), lambda i, *_: (0, i))
    return pl.pallas_call(
        functools.partial(attn_bwd_kernel, bk),
        grid_spec=pltpu.PrefetchScalarGridSpec(
            num_scalar_prefetch=1,
            grid=(t // bq,),
            in_specs=[
                pl.BlockSpec((bq, hd), lambda i, *_: (i, 0)), whole((t, hd)), whole((t, hd)), whole((3 * hd, t)),
                cols(hd), cols(hd), cols(1), cols(1),
            ],
            out_specs=whole((t, 3 * hd)),
            scratch_shapes=[pltpu.VMEM((t, hd), F32), pltpu.VMEM((t, hd), F32)],
        ),
        out_shape=jax.ShapeDtypeStruct((t, 3 * hd), BF16),
        compiler_params=pltpu.CompilerParams(vmem_limit_bytes=VMEM_LIMIT),
        cost_estimate=pl.CostEstimate(flops=40 * t * t * hd, bytes_accessed=16 * t * hd, transcendentals=t * t // 2),
        name='attn_bwd',
    )(tab, q, k, v, qkvt, ot, dot, lse, start)


def exchange_kernel(n, src_of, dst_of, in_ref, out_ref, send_sem, recv_sem, own_sem):
    me = lax.axis_index('model')
    barrier = pltpu.get_barrier_semaphore()

    def hello(off, _):
        pl.semaphore_signal(barrier, inc=1, device_id={'model': lax.rem(me + off, n)}, device_id_type=MESH)
        return 0

    lax.fori_loop(1, n, hello, 0)
    own = pltpu.make_async_copy(src_of(in_ref, me), dst_of(out_ref, me), own_sem)
    own.start()
    pl.semaphore_wait(barrier, n - 1)

    def send(off, _):
        to = lax.rem(me + off, n)
        pltpu.make_async_remote_copy(
            src_ref=src_of(in_ref, to), dst_ref=dst_of(out_ref, me), send_sem=send_sem.at[off], recv_sem=recv_sem.at[off],
            device_id={'model': to}, device_id_type=MESH,
        ).start()
        return 0

    lax.fori_loop(1, n, send, 0)

    def finish(off, _):
        to = lax.rem(me + off, n)
        come = lax.rem(me - off + n, n)
        pltpu.make_async_remote_copy(
            src_ref=src_of(in_ref, to), dst_ref=dst_of(out_ref, come), send_sem=send_sem.at[off], recv_sem=recv_sem.at[off],
            device_id={'model': to}, device_id_type=MESH,
        ).wait()
        return 0

    lax.fori_loop(1, n, finish, 0)
    own.wait()


def exchange(n, value, out_shape, src_of, dst_of, collective_id, name):
    return pl.pallas_call(
        functools.partial(exchange_kernel, n, src_of, dst_of),
        out_shape=jax.ShapeDtypeStruct(out_shape, value.dtype),
        in_specs=[pl.BlockSpec(memory_space=pltpu.VMEM)],
        out_specs=pl.BlockSpec(memory_space=pltpu.VMEM),
        scratch_shapes=[pltpu.SemaphoreType.DMA((n,)), pltpu.SemaphoreType.DMA((n,)), pltpu.SemaphoreType.DMA],
        compiler_params=pltpu.CompilerParams(collective_id=collective_id, has_side_effects=True),
        cost_estimate=pl.CostEstimate(flops=2_000_000_000, bytes_accessed=2 * value.size * 2, transcendentals=0),
        name=name,
    )(value)


def column_block(width):
    return lambda ref, j: ref.at[:, pl.ds(pl.multiple_of(j * width, width), width)]


def leading(ref, j):
    return ref.at[j]


def whole_ref(ref, j):
    return ref


def ln_rows(z, gain):
    wide = z.astype(F32)
    mean = jnp.mean(wide, axis=-1, keepdims=True)
    cen = wide - mean
    rstd = lax.rsqrt(jnp.mean(cen * cen, axis=-1, keepdims=True) + LN_EPS)
    hat = cen * rstd
    return (hat * gain.astype(F32)).astype(BF16), hat, rstd


def ln_back(d_out, hat, rstd, gain):
    d_wide = d_out.astype(F32)
    d_hat = d_wide * gain.astype(F32)
    mean_a = jnp.mean(d_hat, axis=-1, keepdims=True)
    mean_b = jnp.mean(d_hat * hat, axis=-1, keepdims=True)
    return (rstd * (d_hat - mean_a - hat * mean_b)).astype(BF16), jnp.sum(d_wide * hat, axis=0)


def gelu_tanh(up_proj):
    return jax.nn.gelu(up_proj.astype(F32), approximate=True).astype(BF16)


def solution(mesh):
    n = mesh.shape['model']

    def local_step(x_in, seg_ids, gain_one, w_qkv, w_out, gain_two, w_up, w_down, d_y):
        x = x_in[0]
        dy = d_y[0]
        seg = seg_ids[0]
        t, h = x.shape
        n_local, hd = w_out.shape[:2]
        inner = n * n_local * hd
        ts = t // n
        bq = min(512, t)
        bk = min(512, t)
        me = lax.axis_index('model')

        wo_full = lax.all_gather(w_out, 'model', axis=0, tiled=True).reshape(inner, h)

        start = document_starts(seg)
        tab = block_table(seg, start, bq, bk)
        start_row = start.reshape(1, t)

        a_full, q, k, v, qkvt = ln_qkv(x, gain_one, w_qkv.T)
        ot, lse = attention_forward(k, qkvt, start_row, tab, bq, bk)
        o_mine = exchange(n, ot, (n, hd, ts), column_block(ts), leading, 0, 'heads_to_tokens')

        x_s = lax.dynamic_slice(x, (me * ts, 0), (ts, h))
        dy_s = lax.dynamic_slice(dy, (me * ts, 0), (ts, h))
        proj = mm(o_mine.reshape(inner, ts), wo_full, 0, 0)
        resid = (x_s.astype(F32) + proj).astype(BF16)
        b1_s, hat_two, rstd_two = ln_rows(resid, gain_two)
        b1 = lax.all_gather(b1_s, 'model', axis=0, tiled=True)

        d_gelu = mm(dy, w_down, 1, 1).astype(BF16)
        up = mm(b1, w_up, 1, 0).astype(BF16)
        gelu_out, gelu_pull = jax.vjp(gelu_tanh, up)
        (d_up,) = gelu_pull(d_gelu)
        d_b1 = mm(d_up, w_up, 1, 1).astype(BF16)
        late_gelu, d_b1 = lax.optimization_barrier((gelu_out, d_b1))
        d_b1 = lax.psum_scatter(d_b1, 'model', scatter_dimension=0, tiled=True)
        part_two = mm(late_gelu, w_down, 1, 0).astype(BF16)
        late_gelu, late_up, part_two = lax.optimization_barrier((late_gelu, d_up, part_two))
        part_two = lax.psum_scatter(part_two, 'model', scatter_dimension=0, tiled=True)
        d_w_down = mm(late_gelu, dy, 0, 0).astype(BF16)
        d_w_up = mm(b1, late_up, 0, 0).astype(BF16)

        d_ln, d_gain_two = ln_back(d_b1, hat_two, rstd_two, gain_two)
        d_resid_s = dy_s + d_ln
        d_heads = mm(wo_full, d_resid_s, 1, 1).astype(BF16).reshape(n, hd, ts)
        dot = exchange(n, d_heads, (hd, t), leading, column_block(ts), 1, 'tokens_to_heads')
        d_resid = lax.all_gather(d_resid_s, 'model', axis=0, tiled=True)

        d_qkv = attention_backward(q, k, v, qkvt, ot, dot, lse, start_row, tab, bq, bk)
        part_two, _ = lax.optimization_barrier((part_two, d_qkv))
        y_s = (resid.astype(F32) + part_two.astype(F32)).astype(BF16)
        y_out = lax.all_gather(y_s[None], 'model', axis=1, tiled=True)
        d_norm = lax.psum_scatter(mm(d_qkv, w_qkv, 1, 1).astype(BF16), 'model', scatter_dimension=0, tiled=True)
        d_w_qkv = mm(a_full, d_qkv, 0, 0).astype(BF16)
        d_w_out = mm(ot, d_resid, 1, 0).astype(BF16)

        _, hat_one, rstd_one = ln_rows(x_s, gain_one)
        d_ln, d_gain_one = ln_back(d_norm, hat_one, rstd_one, gain_one)
        d_x = lax.all_gather((d_resid_s + d_ln)[None], 'model', axis=1, tiled=True)
        gains = jnp.concatenate([d_gain_one, d_gain_two]).reshape(1, 2 * h)
        gains = exchange(n, gains, (n, 1, 2 * h), whole_ref, leading, 2, 'gain_sums')
        gains = jnp.sum(gains, axis=(0, 1)).astype(BF16)
        return (y_out, d_x, d_w_qkv, d_w_out.reshape(n_local, hd, h), d_w_up, d_w_down, gains[:h], gains[h:])

    in_specs = (P('data'), P('data'), P(), P(None, 'model'), P('model'), P(), P(None, 'model'), P('model'), P('data'))
    out_specs = (P('data'), P('data'), P('data', 'model'), P(('data', 'model')), P('data', 'model'), P(('data', 'model')), P('data'), P('data'))
    return jax.shard_map(local_step, mesh=mesh, in_specs=in_specs, out_specs=out_specs, check_vma=False)
```

```python
import functools
import math

import jax
import jax.numpy as jnp
from jax import lax
from jax.experimental import pallas as pl
from jax.experimental.pallas import tpu as pltpu
from jax.sharding import PartitionSpec as P

LN_EPS = 1e-5
LOG2E = 1.4426950408889634
NEG = -1e30
MESH = pl.DeviceIdType.MESH
VMEM_LIMIT = 60 * 1024 * 1024
F32 = jnp.float32
BF16 = jnp.bfloat16


def mm(a, b, ca, cb):
    return lax.dot_general(a, b, (((ca,), (cb,)), ((), ())), preferred_element_type=F32)


def ln_qkv_kernel(x_ref, g_ref, w_ref, a_ref, q_ref, k_ref, v_ref, t_ref):
    x = x_ref[...].astype(F32)
    mean = jnp.mean(x, axis=-1, keepdims=True)
    cen = x - mean
    var = jnp.mean(cen * cen, axis=-1, keepdims=True)
    a = (cen * lax.rsqrt(var + LN_EPS) * g_ref[...].astype(F32)).astype(BF16)
    a_ref[...] = a
    qkv = mm(a, w_ref[...], 1, 1)
    t_ref[...] = qkv.T.astype(BF16)
    hd = q_ref.shape[1]
    qkv = qkv.astype(BF16)
    q_ref[...] = qkv[:, :hd]
    k_ref[...] = qkv[:, hd:2 * hd]
    v_ref[...] = qkv[:, 2 * hd:]


def ln_qkv(x, g, w):
    t, h = x.shape
    c = w.shape[0]
    hd = c // 3
    bt = min(512, t)
    row = lambda n: pl.BlockSpec((bt, n), lambda i: (i, 0))
    return pl.pallas_call(
        ln_qkv_kernel,
        grid=(t // bt,),
        in_specs=[row(h), pl.BlockSpec((1, h), lambda i: (0, 0)), pl.BlockSpec((c, h), lambda i: (0, 0))],
        out_specs=[row(h), row(hd), row(hd), row(hd), pl.BlockSpec((c, bt), lambda i: (0, i))],
        out_shape=[jax.ShapeDtypeStruct((t, h), BF16)] + [jax.ShapeDtypeStruct((t, hd), BF16)] * 3 + [jax.ShapeDtypeStruct((c, t), BF16)],
        compiler_params=pltpu.CompilerParams(vmem_limit_bytes=VMEM_LIMIT),
        cost_estimate=pl.CostEstimate(flops=2 * t * h * c + 20 * t * h, bytes_accessed=4 * t * h, transcendentals=0),
        name='ln_qkv',
    )(x, g.reshape(1, h), w)


def visible(kb, bk, q0, bq, start):
    k_pos = kb * bk + lax.broadcasted_iota(jnp.int32, (bk, bq), 0)
    q_pos = q0 + lax.broadcasted_iota(jnp.int32, (bk, bq), 1)
    return (k_pos <= q_pos) & (k_pos >= start)


def attn_fwd_kernel(bk, tab_ref, k_ref, qt_ref, vt_ref, start_ref, ot_ref, lse_ref):
    i = pl.program_id(0)
    bq = qt_ref.shape[1]
    hd = qt_ref.shape[0]
    scale = LOG2E * hd ** -0.5
    qt = qt_ref[...]
    start = start_ref[...]
    lo, mid, hi, top = tab_ref[0, i], tab_ref[1, i], tab_ref[2, i], tab_ref[3, i]

    def step(masked, kb, carry):
        m, l, acc = carry
        k0 = pl.multiple_of(kb * bk, bk)
        s = mm(k_ref[pl.ds(k0, bk), :], qt, 1, 0)
        if masked:
            s = jnp.where(visible(kb, bk, i * bq, bq, start), s, NEG)
        m_new = jnp.maximum(m, jnp.max(s, axis=0, keepdims=True))
        p = jnp.exp2((s - m_new) * scale)
        alpha = jnp.exp2((m - m_new) * scale)
        l = l * alpha + jnp.sum(p, axis=0, keepdims=True)
        acc = acc * alpha + mm(vt_ref[:, pl.ds(k0, bk)], p.astype(BF16), 1, 0)
        return m_new, l, acc

    carry = (jnp.full((1, bq), NEG, F32), jnp.zeros((1, bq), F32), jnp.zeros((hd, bq), F32))
    carry = lax.fori_loop(lo, mid, functools.partial(step, True), carry)
    carry = lax.fori_loop(mid, hi, functools.partial(step, False), carry)
    m, l, acc = lax.fori_loop(hi, top, functools.partial(step, True), carry)
    ot_ref[...] = (acc / l).astype(BF16)
    lse_ref[...] = m * scale + jnp.log2(l)


def document_starts(seg):
    t = seg.shape[0]
    wide = 128
    pos = jnp.arange(t, dtype=jnp.int32).reshape(t // wide, wide)
    before = jnp.concatenate([seg[:1], seg[:-1]])
    mark = jnp.where((seg != before).reshape(pos.shape), pos, 0)
    lane = jnp.arange(wide)
    inner = jnp.max(jnp.where(lane[None, :, None] >= lane[None, None, :], mark[:, None, :], 0), axis=-1)
    row = jnp.arange(t // wide)
    prior = jnp.max(jnp.where(row[:, None] > row[None, :], inner[:, -1][None, :], 0), axis=-1)
    return jnp.maximum(inner, prior[:, None]).reshape(t)


def block_table(seg, start, bq, bk):
    t = seg.shape[0]
    nq = t // bq
    q0 = jnp.arange(nq, dtype=jnp.int32) * bq
    first = start.reshape(nq, bq)[:, 0]
    last = start.reshape(nq, bq)[:, -1]
    lo = first // bk
    hi = q0 // bk
    top = (q0 + bq + bk - 1) // bk
    mid = jnp.clip((last + bk - 1) // bk, lo, hi)
    return jnp.stack([lo, mid, hi, top])


def attention_forward(k, qkvt, start, tab, bq, bk):
    t, hd = k.shape
    return pl.pallas_call(
        functools.partial(attn_fwd_kernel, bk),
        grid_spec=pltpu.PrefetchScalarGridSpec(
            num_scalar_prefetch=1,
            grid=(t // bq,),
            in_specs=[
                pl.BlockSpec((t, hd), lambda i, *_: (0, 0)),
                pl.BlockSpec((hd, bq), lambda i, *_: (0, i)),
                pl.BlockSpec((hd, t), lambda i, *_: (2, 0)),
                pl.BlockSpec((1, bq), lambda i, *_: (0, i)),
            ],
            out_specs=[pl.BlockSpec((hd, bq), lambda i, *_: (0, i)), pl.BlockSpec((1, bq), lambda i, *_: (0, i))],
        ),
        out_shape=[jax.ShapeDtypeStruct((hd, t), BF16), jax.ShapeDtypeStruct((1, t), F32)],
        compiler_params=pltpu.CompilerParams(vmem_limit_bytes=VMEM_LIMIT),
        cost_estimate=pl.CostEstimate(flops=16 * t * t * hd, bytes_accessed=8 * t * hd, transcendentals=t * t // 2),
        name='attn_fwd',
    )(tab, k, qkvt, qkvt, start)


def attn_bwd_kernel(bk, tab_ref, q_ref, k_ref, v_ref, t_ref, ot_ref, dot_ref, lse_ref, start_ref, d_ref, dk_acc, dv_acc):
    i = pl.program_id(0)
    bq, hd = q_ref.shape
    scale = LOG2E * hd ** -0.5
    t = k_ref.shape[0]

    @pl.when(i == 0)
    def _():
        dk_acc[...] = jnp.zeros_like(dk_acc)
        dv_acc[...] = jnp.zeros_like(dv_acc)

    c0 = pl.multiple_of(i * bq, bq)
    q = q_ref[...]
    qt = t_ref[:hd, pl.ds(c0, bq)]
    dot_blk = dot_ref[...]
    dot_wide = dot_blk.astype(F32)
    d_out = dot_wide.T.astype(BF16)
    delta = jnp.sum(dot_wide * ot_ref[...].astype(F32), axis=0, keepdims=True)
    lse = lse_ref[...]
    start = start_ref[...]
    lo, mid, hi, top = tab_ref[0, i], tab_ref[1, i], tab_ref[2, i], tab_ref[3, i]

    def step(masked, kb, dqt):
        k0 = pl.multiple_of(kb * bk, bk)
        rows = pl.ds(k0, bk)
        s = mm(k_ref[rows, :], qt, 1, 0)
        p = jnp.exp2(s * scale - lse)
        if masked:
            p = jnp.where(visible(kb, bk, i * bq, bq, start), p, 0.0)
        dp = mm(v_ref[rows, :], dot_blk, 1, 0)
        ds = (p * (dp - delta)).astype(BF16)
        dv_acc[rows, :] += mm(p.astype(BF16), d_out, 1, 0)
        dk_acc[rows, :] += mm(ds, q, 1, 0)
        return dqt + mm(t_ref[hd:2 * hd, rows], ds, 1, 0)

    dqt = jnp.zeros((hd, bq), F32)
    dqt = lax.fori_loop(lo, mid, functools.partial(step, True), dqt)
    dqt = lax.fori_loop(mid, hi, functools.partial(step, False), dqt)
    dqt = lax.fori_loop(hi, top, functools.partial(step, True), dqt)
    d_ref[pl.ds(c0, bq), :hd] = (dqt * hd ** -0.5).T.astype(BF16)

    @pl.when(i == pl.num_programs(0) - 1)
    def _():
        def put(r, _):
            rows = pl.ds(pl.multiple_of(r * bk, bk), bk)
            d_ref[rows, hd:2 * hd] = (dk_acc[rows, :] * hd ** -0.5).astype(BF16)
            d_ref[rows, 2 * hd:] = dv_acc[rows, :].astype(BF16)
            return 0

        lax.fori_loop(0, t // bk, put, 0)


def attention_backward(q, k, v, qkvt, ot, dot, lse, start, tab, bq, bk):
    t, hd = k.shape
    whole = lambda shape: pl.BlockSpec(shape, lambda i, *_: (0, 0))
    cols = lambda n: pl.BlockSpec((n, bq), lambda i, *_: (0, i))
    return pl.pallas_call(
        functools.partial(attn_bwd_kernel, bk),
        grid_spec=pltpu.PrefetchScalarGridSpec(
            num_scalar_prefetch=1,
            grid=(t // bq,),
            in_specs=[
                pl.BlockSpec((bq, hd), lambda i, *_: (i, 0)), whole((t, hd)), whole((t, hd)), whole((3 * hd, t)),
                cols(hd), cols(hd), cols(1), cols(1),
            ],
            out_specs=whole((t, 3 * hd)),
            scratch_shapes=[pltpu.VMEM((t, hd), F32), pltpu.VMEM((t, hd), F32)],
        ),
        out_shape=jax.ShapeDtypeStruct((t, 3 * hd), BF16),
        compiler_params=pltpu.CompilerParams(vmem_limit_bytes=VMEM_LIMIT),
        cost_estimate=pl.CostEstimate(flops=40 * t * t * hd, bytes_accessed=16 * t * hd, transcendentals=t * t // 2),
        name='attn_bwd',
    )(tab, q, k, v, qkvt, ot, dot, lse, start)


def exchange_kernel(n, src_of, dst_of, in_ref, out_ref, send_sem, recv_sem, own_sem):
    me = lax.axis_index('model')
    barrier = pltpu.get_barrier_semaphore()

    def hello(off, _):
        pl.semaphore_signal(barrier, inc=1, device_id={'model': lax.rem(me + off, n)}, device_id_type=MESH)
        return 0

    lax.fori_loop(1, n, hello, 0)
    own = pltpu.make_async_copy(src_of(in_ref, me), dst_of(out_ref, me), own_sem)
    own.start()
    pl.semaphore_wait(barrier, n - 1)

    def send(off, _):
        to = lax.rem(me + off, n)
        pltpu.make_async_remote_copy(
            src_ref=src_of(in_ref, to), dst_ref=dst_of(out_ref, me), send_sem=send_sem.at[off], recv_sem=recv_sem.at[off],
            device_id={'model': to}, device_id_type=MESH,
        ).start()
        return 0

    lax.fori_loop(1, n, send, 0)

    def finish(off, _):
        to = lax.rem(me + off, n)
        come = lax.rem(me - off + n, n)
        pltpu.make_async_remote_copy(
            src_ref=src_of(in_ref, to), dst_ref=dst_of(out_ref, come), send_sem=send_sem.at[off], recv_sem=recv_sem.at[off],
            device_id={'model': to}, device_id_type=MESH,
        ).wait()
        return 0

    lax.fori_loop(1, n, finish, 0)
    own.wait()


def exchange(n, value, out_shape, src_of, dst_of, collective_id, name):
    return pl.pallas_call(
        functools.partial(exchange_kernel, n, src_of, dst_of),
        out_shape=jax.ShapeDtypeStruct(out_shape, value.dtype),
        in_specs=[pl.BlockSpec(memory_space=pltpu.VMEM)],
        out_specs=pl.BlockSpec(memory_space=pltpu.VMEM),
        scratch_shapes=[pltpu.SemaphoreType.DMA((n,)), pltpu.SemaphoreType.DMA((n,)), pltpu.SemaphoreType.DMA],
        compiler_params=pltpu.CompilerParams(collective_id=collective_id, has_side_effects=True),
        cost_estimate=pl.CostEstimate(flops=2_000_000_000, bytes_accessed=2 * value.size * 2, transcendentals=0),
        name=name,
    )(value)


def column_block(width):
    return lambda ref, j: ref.at[:, pl.ds(pl.multiple_of(j * width, width), width)]


def leading(ref, j):
    return ref.at[j]


def whole_ref(ref, j):
    return ref


def ring_place(n, q):
    me = lax.axis_index('model')
    side = math.isqrt(n // 2)
    core = lax.rem(me, 2)
    chip = me // 2
    x = lax.rem(chip, side)
    y = chip // side
    turn = q // 2
    sign = 1 - 2 * lax.rem(q, 2)
    a = x * (1 - turn) + y * turn
    b = y * (1 - turn) + x * turn

    def chip_at(pa, pb):
        pa = lax.rem(pa + 2 * side, side)
        pb = lax.rem(pb + 2 * side, side)
        return (pb * (1 - turn) + pa * turn) * side + pa * (1 - turn) + pb * turn

    return side, core, sign, a, b, chip_at


def greet_neighbours(n):
    me = lax.axis_index('model')
    barrier = pltpu.get_barrier_semaphore()
    core = lax.rem(me, 2)
    pl.semaphore_signal(barrier, inc=1, device_id={'model': me + 1 - 2 * core}, device_id_type=MESH)

    def hello(q, _):
        side, core, sign, a, b, chip_at = ring_place(n, q)
        pl.semaphore_signal(barrier, inc=1, device_id={'model': chip_at(a + sign, b) * 2 + core}, device_id_type=MESH)
        return 0

    lax.fori_loop(0, 4, hello, 0)
    pl.semaphore_wait(barrier, 5)


def reduce_kernel(n, r_dim, l_ref, r_ref, out_ref, l_peer, r_peer, first, slot1, slot2, s_send, s_recv, p_send, p_recv, x_send, x_recv):
    me = lax.axis_index('model')
    my_core = lax.rem(me, 2)
    chips, _, tb, _ = l_ref.shape
    width = out_ref.shape[1] // 4
    side = math.isqrt(chips)
    greet_neighbours(n)
    peer = {'model': me + 1 - 2 * my_core}
    swap = [
        pltpu.make_async_remote_copy(src, dst, x_send.at[i], x_recv.at[i], device_id=peer, device_id_type=MESH)
        for i, (src, dst) in enumerate([(r_ref, r_peer), (l_ref.at[:, 1 - my_core], l_peer)])
    ]
    for copy in swap:
        copy.start()

    def partial(q, chip):
        cols = pl.ds(pl.multiple_of(q * width, width), width)
        mine, other = (r_ref[:, cols], r_peer[:, cols]) if r_dim == 0 else (r_ref[cols, :], r_peer[cols, :])
        return mm(l_ref[chip, my_core], mine, 1, r_dim) + mm(l_peer[chip], other, 1, r_dim)

    def hop(q, s, j, src):
        _, core, sign, a, b, chip_at = ring_place(n, q)
        at = (q * (side - 1) + s) * side + j
        return pltpu.make_async_remote_copy(
            src, slot1.at[at], s_send.at[at], s_recv.at[at], device_id={'model': chip_at(a + sign, b) * 2 + core}, device_id_type=MESH)

    def turn_hop(q, s, src):
        _, core, sign, a, b, chip_at = ring_place(n, q)
        at = q * (side - 1) + s
        return pltpu.make_async_remote_copy(
            src, slot2.at[at], p_send.at[at], p_recv.at[at], device_id={'model': chip_at(a, b + sign) * 2 + core}, device_id_type=MESH)

    def arrived(q, s, j):
        return (q * (side - 1) + s) * side + j

    for copy in swap:
        copy.wait()

    def start_round(t, _):
        j, q = t // 4, lax.rem(t, 4)
        _, _, sign, a, b, chip_at = ring_place(n, q)
        at = q * side + j
        first[at] = partial(q, chip_at(a - sign, b - sign * (1 + j))).astype(BF16)
        hop(q, 0, j, first.at[at]).start()
        return 0

    lax.fori_loop(0, 4 * side, start_round, 0)

    def middle_round(t, _):
        s, rest = 1 + t // (4 * side), lax.rem(t, 4 * side)
        j, q = rest // 4, lax.rem(rest, 4)
        _, _, sign, a, b, chip_at = ring_place(n, q)
        at = arrived(q, s - 1, j)
        own = partial(q, chip_at(a - sign * (1 + s), b - sign * (1 + j)))
        hop(q, s - 1, j, slot1.at[at]).wait_recv()
        slot1[at] = (slot1[at].astype(F32) + own).astype(BF16)
        hop(q, s, j, slot1.at[at]).start()
        return 0

    lax.fori_loop(0, 4 * side * (side - 2), middle_round, 0)

    def last_sum(q, j):
        _, _, sign, a, b, chip_at = ring_place(n, q)
        at = arrived(q, side - 2, j)
        own = partial(q, chip_at(a, b - sign * (1 + j)))
        hop(q, side - 2, j, slot1.at[at]).wait_recv()
        return at, slot1[at].astype(F32) + own

    def turn_first(q, _):
        at, total = last_sum(q, 0)
        slot1[at] = total.astype(BF16)
        turn_hop(q, 0, slot1.at[at]).start()
        return 0

    lax.fori_loop(0, 4, turn_first, 0)

    def turn_round(t, _):
        s, q = 1 + t // 4, lax.rem(t, 4)
        _, total = last_sum(q, s)
        at = q * (side - 1) + s - 1
        turn_hop(q, s - 1, slot2.at[at]).wait_recv()
        slot2[at] = (slot2[at].astype(F32) + total).astype(BF16)
        turn_hop(q, s, slot2.at[at]).start()
        return 0

    lax.fori_loop(0, 4 * (side - 2), turn_round, 0)

    def turn_last(q, _):
        _, total = last_sum(q, side - 1)
        at = q * (side - 1) + side - 2
        turn_hop(q, side - 2, slot2.at[at]).wait_recv()
        out_ref[:, pl.ds(pl.multiple_of(q * width, width), width)] = (slot2[at].astype(F32) + total).astype(BF16)
        return 0

    lax.fori_loop(0, 4, turn_last, 0)

    def drain(t, _):
        q, s = t // (side - 1), lax.rem(t, side - 1)
        turn_hop(q, s, slot2.at[t]).wait_send()
        for j in range(side):
            hop(q, s, j, slot1.at[t * side + j]).wait_send()
        return 0

    lax.fori_loop(0, 4 * (side - 1), drain, 0)


def matmul_reduce_scatter(n, left, right, r_dim, collective_id, name):
    t, k = left.shape
    f = right.shape[1 - r_dim]
    chips = n // 2
    side = math.isqrt(chips)
    tb = t // n
    hops = 4 * (side - 1)
    vmem = pl.BlockSpec(memory_space=pltpu.VMEM)
    return pl.pallas_call(
        functools.partial(reduce_kernel, n, r_dim),
        out_shape=jax.ShapeDtypeStruct((tb, f), BF16),
        in_specs=[vmem, vmem],
        out_specs=vmem,
        scratch_shapes=[
            pltpu.VMEM((chips, tb, k), BF16),
            pltpu.VMEM(right.shape, BF16),
            pltpu.VMEM((4 * side, tb, f // 4), BF16),
            pltpu.VMEM((hops * side, tb, f // 4), BF16),
            pltpu.VMEM((hops, tb, f // 4), BF16),
            pltpu.SemaphoreType.DMA((hops * side,)), pltpu.SemaphoreType.DMA((hops * side,)),
            pltpu.SemaphoreType.DMA((hops,)), pltpu.SemaphoreType.DMA((hops,)),
            pltpu.SemaphoreType.DMA((2,)), pltpu.SemaphoreType.DMA((2,)),
        ],
        compiler_params=pltpu.CompilerParams(collective_id=collective_id, has_side_effects=True, vmem_limit_bytes=40 * 1024 * 1024),
        cost_estimate=pl.CostEstimate(flops=40_000_000_000, bytes_accessed=4 * t * k, transcendentals=0),
        name=name,
    )(left.reshape(chips, 2, tb, k), right)


def ln_rows(z, gain):
    wide = z.astype(F32)
    mean = jnp.mean(wide, axis=-1, keepdims=True)
    cen = wide - mean
    rstd = lax.rsqrt(jnp.mean(cen * cen, axis=-1, keepdims=True) + LN_EPS)
    hat = cen * rstd
    return (hat * gain.astype(F32)).astype(BF16), hat, rstd


def ln_back(d_out, hat, rstd, gain):
    d_wide = d_out.astype(F32)
    d_hat = d_wide * gain.astype(F32)
    mean_a = jnp.mean(d_hat, axis=-1, keepdims=True)
    mean_b = jnp.mean(d_hat * hat, axis=-1, keepdims=True)
    return (rstd * (d_hat - mean_a - hat * mean_b)).astype(BF16), jnp.sum(d_wide * hat, axis=0)


def gelu_tanh(up_proj):
    return jax.nn.gelu(up_proj.astype(F32), approximate=True).astype(BF16)


def solution(mesh):
    n = mesh.shape['model']

    def local_step(x_in, seg_ids, gain_one, w_qkv, w_out, gain_two, w_up, w_down, d_y):
        x = x_in[0]
        dy = d_y[0]
        seg = seg_ids[0]
        t, h = x.shape
        n_local, hd = w_out.shape[:2]
        inner = n * n_local * hd
        ts = t // n
        bq = min(512, t)
        bk = min(512, t)
        me = lax.axis_index('model')

        wo_full = lax.all_gather(w_out, 'model', axis=0, tiled=True).reshape(inner, h)

        start = document_starts(seg)
        tab = block_table(seg, start, bq, bk)
        start_row = start.reshape(1, t)

        a_full, q, k, v, qkvt = ln_qkv(x, gain_one, w_qkv.T)
        ot, lse = attention_forward(k, qkvt, start_row, tab, bq, bk)
        o_mine = exchange(n, ot, (n, hd, ts), column_block(ts), leading, 0, 'heads_to_tokens')

        x_s = lax.dynamic_slice(x, (me * ts, 0), (ts, h))
        dy_s = lax.dynamic_slice(dy, (me * ts, 0), (ts, h))
        proj = mm(o_mine.reshape(inner, ts), wo_full, 0, 0)
        resid = (x_s.astype(F32) + proj).astype(BF16)
        b1_s, hat_two, rstd_two = ln_rows(resid, gain_two)
        b1 = lax.all_gather(b1_s, 'model', axis=0, tiled=True)

        d_gelu = mm(dy, w_down, 1, 1).astype(BF16)
        up = mm(b1, w_up, 1, 0).astype(BF16)
        gelu_out, gelu_pull = jax.vjp(gelu_tanh, up)
        (d_up,) = gelu_pull(d_gelu)
        d_b1 = matmul_reduce_scatter(n, d_up, w_up, 1, 3, 'reduce_d_b1')
        late_gelu, d_b1 = lax.optimization_barrier((gelu_out, d_b1))
        part_two = matmul_reduce_scatter(n, late_gelu, w_down, 0, 4, 'reduce_y')
        late_gelu, late_up, part_two = lax.optimization_barrier((late_gelu, d_up, part_two))
        d_w_down = mm(late_gelu, dy, 0, 0).astype(BF16)
        d_w_up = mm(b1, late_up, 0, 0).astype(BF16)

        d_ln, d_gain_two = ln_back(d_b1, hat_two, rstd_two, gain_two)
        d_resid_s = dy_s + d_ln
        d_heads = mm(wo_full, d_resid_s, 1, 1).astype(BF16).reshape(n, hd, ts)
        dot = exchange(n, d_heads, (hd, t), leading, column_block(ts), 1, 'tokens_to_heads')
        d_resid = lax.all_gather(d_resid_s, 'model', axis=0, tiled=True)

        d_qkv = attention_backward(q, k, v, qkvt, ot, dot, lse, start_row, tab, bq, bk)
        y_s = (resid.astype(F32) + part_two.astype(F32)).astype(BF16)
        y_out = lax.all_gather(y_s[None], 'model', axis=1, tiled=True)
        d_norm = matmul_reduce_scatter(n, d_qkv, w_qkv.T, 0, 5, 'reduce_d_x')
        d_w_qkv = mm(a_full, d_qkv, 0, 0).astype(BF16)
        d_w_out = mm(ot, d_resid, 1, 0).astype(BF16)

        _, hat_one, rstd_one = ln_rows(x_s, gain_one)
        d_ln, d_gain_one = ln_back(d_norm, hat_one, rstd_one, gain_one)
        d_x = lax.all_gather((d_resid_s + d_ln)[None], 'model', axis=1, tiled=True)
        gains = jnp.concatenate([d_gain_one, d_gain_two]).reshape(1, 2 * h)
        gains = exchange(n, gains, (n, 1, 2 * h), whole_ref, leading, 2, 'gain_sums')
        gains = jnp.sum(gains, axis=(0, 1)).astype(BF16)
        return (y_out, d_x, d_w_qkv, d_w_out.reshape(n_local, hd, h), d_w_up, d_w_down, gains[:h], gains[h:])

    in_specs = (P('data'), P('data'), P(), P(None, 'model'), P('model'), P(), P(None, 'model'), P('model'), P('data'))
    out_specs = (P('data'), P('data'), P('data', 'model'), P(('data', 'model')), P('data', 'model'), P(('data', 'model')), P('data'), P('data'))
    return jax.shard_map(local_step, mesh=mesh, in_specs=in_specs, out_specs=out_specs, check_vma=False)
```

```python
import functools
import math

import jax
import jax.numpy as jnp
from jax import lax
from jax.experimental import pallas as pl
from jax.experimental.pallas import tpu as pltpu
from jax.sharding import PartitionSpec as P


LN_EPS = 1e-5
LOG2E = 1.4426950408889634
NEG = -1e30
MESH = pl.DeviceIdType.MESH
VMEM_LIMIT = 60 * 1024 * 1024
F32 = jnp.float32
BF16 = jnp.bfloat16


def mm(a, b, ca, cb):
    return lax.dot_general(a, b, (((ca,), (cb,)), ((), ())), preferred_element_type=F32)


def ln_qkv_kernel(x_ref, g_ref, w_ref, a_ref, q_ref, k_ref, v_ref, t_ref):
    x = x_ref[...].astype(F32)
    mean = jnp.mean(x, axis=-1, keepdims=True)
    cen = x - mean
    var = jnp.mean(cen * cen, axis=-1, keepdims=True)
    a = (cen * lax.rsqrt(var + LN_EPS) * g_ref[...].astype(F32)).astype(BF16)
    a_ref[...] = a
    qkv = mm(a, w_ref[...], 1, 1)
    t_ref[...] = qkv.T.astype(BF16)
    hd = q_ref.shape[1]
    qkv = qkv.astype(BF16)
    q_ref[...] = qkv[:, :hd]
    k_ref[...] = qkv[:, hd:2 * hd]
    v_ref[...] = qkv[:, 2 * hd:]


def ln_qkv(x, g, w):
    t, h = x.shape
    c = w.shape[0]
    hd = c // 3
    bt = min(512, t)
    row = lambda n: pl.BlockSpec((bt, n), lambda i: (i, 0))
    return pl.pallas_call(
        ln_qkv_kernel,
        grid=(t // bt,),
        in_specs=[row(h), pl.BlockSpec((1, h), lambda i: (0, 0)), pl.BlockSpec((c, h), lambda i: (0, 0))],
        out_specs=[row(h), row(hd), row(hd), row(hd), pl.BlockSpec((c, bt), lambda i: (0, i))],
        out_shape=[jax.ShapeDtypeStruct((t, h), BF16)] + [jax.ShapeDtypeStruct((t, hd), BF16)] * 3 + [jax.ShapeDtypeStruct((c, t), BF16)],
        compiler_params=pltpu.CompilerParams(vmem_limit_bytes=VMEM_LIMIT),
        cost_estimate=pl.CostEstimate(flops=2 * t * h * c + 20 * t * h, bytes_accessed=4 * t * h, transcendentals=0),
        name='ln_qkv',
    )(x, g.reshape(1, h), w)


def visible(kb, bk, q0, bq, start):
    k_pos = kb * bk + lax.broadcasted_iota(jnp.int32, (bk, bq), 0)
    q_pos = q0 + lax.broadcasted_iota(jnp.int32, (bk, bq), 1)
    return (k_pos <= q_pos) & (k_pos >= start)


def attn_fwd_kernel(bk, tab_ref, k_ref, qt_ref, vt_ref, start_ref, ot_ref, lse_ref):
    i = pl.program_id(0)
    bq = qt_ref.shape[1]
    hd = qt_ref.shape[0]
    scale = LOG2E * hd ** -0.5
    qt = qt_ref[...]
    start = start_ref[...]
    lo, mid, hi, top = tab_ref[0, i], tab_ref[1, i], tab_ref[2, i], tab_ref[3, i]

    def step(masked, kb, carry):
        m, l, acc = carry
        k0 = pl.multiple_of(kb * bk, bk)
        s = mm(k_ref[pl.ds(k0, bk), :], qt, 1, 0)
        if masked:
            s = jnp.where(visible(kb, bk, i * bq, bq, start), s, NEG)
        m_new = jnp.maximum(m, jnp.max(s, axis=0, keepdims=True))
        p = jnp.exp2((s - m_new) * scale)
        alpha = jnp.exp2((m - m_new) * scale)
        l = l * alpha + jnp.sum(p, axis=0, keepdims=True)
        acc = acc * alpha + mm(vt_ref[:, pl.ds(k0, bk)], p.astype(BF16), 1, 0)
        return m_new, l, acc

    carry = (jnp.full((1, bq), NEG, F32), jnp.zeros((1, bq), F32), jnp.zeros((hd, bq), F32))
    carry = lax.fori_loop(lo, mid, functools.partial(step, True), carry)
    carry = lax.fori_loop(mid, hi, functools.partial(step, False), carry)
    m, l, acc = lax.fori_loop(hi, top, functools.partial(step, True), carry)
    ot_ref[...] = (acc / l).astype(BF16)
    lse_ref[...] = m * scale + jnp.log2(l)


def document_starts(seg):
    t = seg.shape[0]
    wide = 128
    pos = jnp.arange(t, dtype=jnp.int32).reshape(t // wide, wide)
    before = jnp.concatenate([seg[:1], seg[:-1]])
    mark = jnp.where((seg != before).reshape(pos.shape), pos, 0)
    lane = jnp.arange(wide)
    inner = jnp.max(jnp.where(lane[None, :, None] >= lane[None, None, :], mark[:, None, :], 0), axis=-1)
    row = jnp.arange(t // wide)
    prior = jnp.max(jnp.where(row[:, None] > row[None, :], inner[:, -1][None, :], 0), axis=-1)
    return jnp.maximum(inner, prior[:, None]).reshape(t)


def block_table(seg, start, bq, bk):
    t = seg.shape[0]
    nq = t // bq
    q0 = jnp.arange(nq, dtype=jnp.int32) * bq
    first = start.reshape(nq, bq)[:, 0]
    last = start.reshape(nq, bq)[:, -1]
    lo = first // bk
    hi = q0 // bk
    top = (q0 + bq + bk - 1) // bk
    mid = jnp.clip((last + bk - 1) // bk, lo, hi)
    return jnp.stack([lo, mid, hi, top])


def attention_forward(k, qkvt, start, tab, bq, bk):
    t, hd = k.shape
    return pl.pallas_call(
        functools.partial(attn_fwd_kernel, bk),
        grid_spec=pltpu.PrefetchScalarGridSpec(
            num_scalar_prefetch=1,
            grid=(t // bq,),
            in_specs=[
                pl.BlockSpec((t, hd), lambda i, *_: (0, 0)),
                pl.BlockSpec((hd, bq), lambda i, *_: (0, i)),
                pl.BlockSpec((hd, t), lambda i, *_: (2, 0)),
                pl.BlockSpec((1, bq), lambda i, *_: (0, i)),
            ],
            out_specs=[pl.BlockSpec((hd, bq), lambda i, *_: (0, i)), pl.BlockSpec((1, bq), lambda i, *_: (0, i))],
        ),
        out_shape=[jax.ShapeDtypeStruct((hd, t), BF16), jax.ShapeDtypeStruct((1, t), F32)],
        compiler_params=pltpu.CompilerParams(vmem_limit_bytes=VMEM_LIMIT),
        cost_estimate=pl.CostEstimate(flops=16 * t * t * hd, bytes_accessed=8 * t * hd, transcendentals=t * t // 2),
        name='attn_fwd',
    )(tab, k, qkvt, qkvt, start)


def attn_bwd_kernel(bk, tab_ref, q_ref, k_ref, v_ref, t_ref, ot_ref, dot_ref, lse_ref, start_ref, d_ref, dk_acc, dv_acc):
    i = pl.program_id(0)
    bq, hd = q_ref.shape
    scale = LOG2E * hd ** -0.5
    t = k_ref.shape[0]

    @pl.when(i == 0)
    def _():
        dk_acc[...] = jnp.zeros_like(dk_acc)
        dv_acc[...] = jnp.zeros_like(dv_acc)

    c0 = pl.multiple_of(i * bq, bq)
    q = q_ref[...]
    qt = t_ref[:hd, pl.ds(c0, bq)]
    dot_blk = dot_ref[...]
    dot_wide = dot_blk.astype(F32)
    d_out = dot_wide.T.astype(BF16)
    delta = jnp.sum(dot_wide * ot_ref[...].astype(F32), axis=0, keepdims=True)
    lse = lse_ref[...]
    start = start_ref[...]
    lo, mid, hi, top = tab_ref[0, i], tab_ref[1, i], tab_ref[2, i], tab_ref[3, i]

    def step(masked, kb, dqt):
        k0 = pl.multiple_of(kb * bk, bk)
        rows = pl.ds(k0, bk)
        s = mm(k_ref[rows, :], qt, 1, 0)
        p = jnp.exp2(s * scale - lse)
        if masked:
            p = jnp.where(visible(kb, bk, i * bq, bq, start), p, 0.0)
        dp = mm(v_ref[rows, :], dot_blk, 1, 0)
        ds = (p * (dp - delta)).astype(BF16)
        dv_acc[rows, :] += mm(p.astype(BF16), d_out, 1, 0)
        dk_acc[rows, :] += mm(ds, q, 1, 0)
        return dqt + mm(t_ref[hd:2 * hd, rows], ds, 1, 0)

    dqt = jnp.zeros((hd, bq), F32)
    dqt = lax.fori_loop(lo, mid, functools.partial(step, True), dqt)
    dqt = lax.fori_loop(mid, hi, functools.partial(step, False), dqt)
    dqt = lax.fori_loop(hi, top, functools.partial(step, True), dqt)
    d_ref[pl.ds(c0, bq), :hd] = (dqt * hd ** -0.5).T.astype(BF16)

    @pl.when(i == pl.num_programs(0) - 1)
    def _():
        def put(r, _):
            rows = pl.ds(pl.multiple_of(r * bk, bk), bk)
            d_ref[rows, hd:2 * hd] = (dk_acc[rows, :] * hd ** -0.5).astype(BF16)
            d_ref[rows, 2 * hd:] = dv_acc[rows, :].astype(BF16)
            return 0

        lax.fori_loop(0, t // bk, put, 0)


def attention_backward(q, k, v, qkvt, ot, dot, lse, start, tab, bq, bk):
    t, hd = k.shape
    whole = lambda shape: pl.BlockSpec(shape, lambda i, *_: (0, 0))
    cols = lambda n: pl.BlockSpec((n, bq), lambda i, *_: (0, i))
    return pl.pallas_call(
        functools.partial(attn_bwd_kernel, bk),
        grid_spec=pltpu.PrefetchScalarGridSpec(
            num_scalar_prefetch=1,
            grid=(t // bq,),
            in_specs=[
                pl.BlockSpec((bq, hd), lambda i, *_: (i, 0)), whole((t, hd)), whole((t, hd)), whole((3 * hd, t)),
                cols(hd), cols(hd), cols(1), cols(1),
            ],
            out_specs=whole((t, 3 * hd)),
            scratch_shapes=[pltpu.VMEM((t, hd), F32), pltpu.VMEM((t, hd), F32)],
        ),
        out_shape=jax.ShapeDtypeStruct((t, 3 * hd), BF16),
        compiler_params=pltpu.CompilerParams(vmem_limit_bytes=VMEM_LIMIT),
        cost_estimate=pl.CostEstimate(flops=40 * t * t * hd, bytes_accessed=16 * t * hd, transcendentals=t * t // 2),
        name='attn_bwd',
    )(tab, q, k, v, qkvt, ot, dot, lse, start)


def exchange_kernel(n, src_of, dst_of, in_ref, out_ref, send_sem, recv_sem, own_sem):
    me = lax.axis_index('model')
    barrier = pltpu.get_barrier_semaphore()

    def hello(off, _):
        pl.semaphore_signal(barrier, inc=1, device_id={'model': lax.rem(me + off, n)}, device_id_type=MESH)
        return 0

    lax.fori_loop(1, n, hello, 0)
    own = pltpu.make_async_copy(src_of(in_ref, me), dst_of(out_ref, me), own_sem)
    own.start()
    pl.semaphore_wait(barrier, n - 1)

    def send(off, _):
        to = lax.rem(me + off, n)
        pltpu.make_async_remote_copy(
            src_ref=src_of(in_ref, to), dst_ref=dst_of(out_ref, me), send_sem=send_sem.at[off], recv_sem=recv_sem.at[off],
            device_id={'model': to}, device_id_type=MESH,
        ).start()
        return 0

    lax.fori_loop(1, n, send, 0)

    def finish(off, _):
        to = lax.rem(me + off, n)
        come = lax.rem(me - off + n, n)
        pltpu.make_async_remote_copy(
            src_ref=src_of(in_ref, to), dst_ref=dst_of(out_ref, come), send_sem=send_sem.at[off], recv_sem=recv_sem.at[off],
            device_id={'model': to}, device_id_type=MESH,
        ).wait()
        return 0

    lax.fori_loop(1, n, finish, 0)
    own.wait()


def exchange(n, value, out_shape, src_of, dst_of, collective_id):
    return pl.pallas_call(
        functools.partial(exchange_kernel, n, src_of, dst_of),
        out_shape=jax.ShapeDtypeStruct(out_shape, value.dtype),
        in_specs=[pl.BlockSpec(memory_space=pltpu.VMEM)],
        out_specs=pl.BlockSpec(memory_space=pltpu.VMEM),
        scratch_shapes=[pltpu.SemaphoreType.DMA((n,)), pltpu.SemaphoreType.DMA((n,)), pltpu.SemaphoreType.DMA],
        compiler_params=pltpu.CompilerParams(collective_id=collective_id, has_side_effects=True),
        cost_estimate=pl.CostEstimate(flops=2_000_000_000, bytes_accessed=2 * value.size * 2, transcendentals=0),
    )(value)


def column_block(width):
    return lambda ref, j: ref.at[:, pl.ds(pl.multiple_of(j * width, width), width)]


def leading(ref, j):
    return ref.at[j]


def whole_ref(ref, j):
    return ref


def ring_place(n, q):
    me = lax.axis_index('model')
    side = math.isqrt(n // 2)
    core = lax.rem(me, 2)
    chip = me // 2
    x = lax.rem(chip, side)
    y = chip // side
    turn = q // 2
    sign = 1 - 2 * lax.rem(q, 2)
    a = x * (1 - turn) + y * turn
    b = y * (1 - turn) + x * turn

    def chip_at(pa, pb):
        pa = lax.rem(pa + 2 * side, side)
        pb = lax.rem(pb + 2 * side, side)
        return (pb * (1 - turn) + pa * turn) * side + pa * (1 - turn) + pb * turn

    return side, core, sign, a, b, chip_at


def greet_neighbours(n):
    me = lax.axis_index('model')
    barrier = pltpu.get_barrier_semaphore()
    core = lax.rem(me, 2)
    pl.semaphore_signal(barrier, inc=1, device_id={'model': me + 1 - 2 * core}, device_id_type=MESH)

    def hello(q, _):
        _, core, sign, a, b, chip_at = ring_place(n, q)
        pl.semaphore_signal(barrier, inc=1, device_id={'model': chip_at(a + sign, b) * 2 + core}, device_id_type=MESH)
        return 0

    lax.fori_loop(0, 4, hello, 0)
    pl.semaphore_wait(barrier, 5)


def reduce_kernel(n, r_dim, l_ref, r_ref, out_ref, l_peer, r_peer, first, slot1, slot2, s_send, s_recv, p_send, p_recv, x_send, x_recv):
    me = lax.axis_index('model')
    my_core = lax.rem(me, 2)
    chips, _, _, _ = l_ref.shape
    width = out_ref.shape[1] // 4
    side = math.isqrt(chips)
    greet_neighbours(n)
    peer = {'model': me + 1 - 2 * my_core}
    swap = [
        pltpu.make_async_remote_copy(src, dst, x_send.at[i], x_recv.at[i], device_id=peer, device_id_type=MESH)
        for i, (src, dst) in enumerate([(r_ref, r_peer), (l_ref.at[:, 1 - my_core], l_peer)])
    ]
    for copy in swap:
        copy.start()

    def partial(q, chip):
        cols = pl.ds(pl.multiple_of(q * width, width), width)
        mine, other = (r_ref[:, cols], r_peer[:, cols]) if r_dim == 0 else (r_ref[cols, :], r_peer[cols, :])
        return mm(l_ref[chip, my_core], mine, 1, r_dim) + mm(l_peer[chip], other, 1, r_dim)

    def hop(q, s, j, src):
        _, core, sign, a, b, chip_at = ring_place(n, q)
        at = (q * (side - 1) + s) * side + j
        return pltpu.make_async_remote_copy(
            src, slot1.at[at], s_send.at[at], s_recv.at[at], device_id={'model': chip_at(a + sign, b) * 2 + core}, device_id_type=MESH)

    def turn_hop(q, s, src):
        _, core, sign, a, b, chip_at = ring_place(n, q)
        at = q * (side - 1) + s
        return pltpu.make_async_remote_copy(
            src, slot2.at[at], p_send.at[at], p_recv.at[at], device_id={'model': chip_at(a, b + sign) * 2 + core}, device_id_type=MESH)

    def arrived(q, s, j):
        return (q * (side - 1) + s) * side + j

    for copy in swap:
        copy.wait()

    def start_round(t, _):
        j, q = t // 4, lax.rem(t, 4)
        _, _, sign, a, b, chip_at = ring_place(n, q)
        at = q * side + j
        first[at] = partial(q, chip_at(a - sign, b - sign * (1 + j))).astype(BF16)
        hop(q, 0, j, first.at[at]).start()
        return 0

    lax.fori_loop(0, 4 * side, start_round, 0)

    def middle_round(t, _):
        s, rest = 1 + t // (4 * side), lax.rem(t, 4 * side)
        j, q = rest // 4, lax.rem(rest, 4)
        _, _, sign, a, b, chip_at = ring_place(n, q)
        at = arrived(q, s - 1, j)
        own = partial(q, chip_at(a - sign * (1 + s), b - sign * (1 + j)))
        hop(q, s - 1, j, slot1.at[at]).wait_recv()
        slot1[at] = (slot1[at].astype(F32) + own).astype(BF16)
        hop(q, s, j, slot1.at[at]).start()
        return 0

    lax.fori_loop(0, 4 * side * (side - 2), middle_round, 0)

    def last_sum(q, j):
        _, _, sign, a, b, chip_at = ring_place(n, q)
        at = arrived(q, side - 2, j)
        own = partial(q, chip_at(a, b - sign * (1 + j)))
        hop(q, side - 2, j, slot1.at[at]).wait_recv()
        return at, slot1[at].astype(F32) + own

    def turn_first(q, _):
        at, total = last_sum(q, 0)
        slot1[at] = total.astype(BF16)
        turn_hop(q, 0, slot1.at[at]).start()
        return 0

    lax.fori_loop(0, 4, turn_first, 0)

    def turn_round(t, _):
        s, q = 1 + t // 4, lax.rem(t, 4)
        _, total = last_sum(q, s)
        at = q * (side - 1) + s - 1
        turn_hop(q, s - 1, slot2.at[at]).wait_recv()
        slot2[at] = (slot2[at].astype(F32) + total).astype(BF16)
        turn_hop(q, s, slot2.at[at]).start()
        return 0

    lax.fori_loop(0, 4 * (side - 2), turn_round, 0)

    def turn_last(q, _):
        _, total = last_sum(q, side - 1)
        at = q * (side - 1) + side - 2
        turn_hop(q, side - 2, slot2.at[at]).wait_recv()
        out_ref[:, pl.ds(pl.multiple_of(q * width, width), width)] = (slot2[at].astype(F32) + total).astype(BF16)
        return 0

    lax.fori_loop(0, 4, turn_last, 0)

    def drain(t, _):
        q, s = t // (side - 1), lax.rem(t, side - 1)
        turn_hop(q, s, slot2.at[t]).wait_send()
        for j in range(side):
            hop(q, s, j, slot1.at[t * side + j]).wait_send()
        return 0

    lax.fori_loop(0, 4 * (side - 1), drain, 0)


def matmul_reduce_scatter(n, left, right, r_dim, collective_id):
    t, k = left.shape
    f = right.shape[1 - r_dim]
    chips = n // 2
    side = math.isqrt(chips)
    tb = t // n
    hops = 4 * (side - 1)
    vmem = pl.BlockSpec(memory_space=pltpu.VMEM)
    return pl.pallas_call(
        functools.partial(reduce_kernel, n, r_dim),
        out_shape=jax.ShapeDtypeStruct((tb, f), BF16),
        in_specs=[vmem, vmem],
        out_specs=vmem,
        scratch_shapes=[
            pltpu.VMEM((chips, tb, k), BF16),
            pltpu.VMEM(right.shape, BF16),
            pltpu.VMEM((4 * side, tb, f // 4), BF16),
            pltpu.VMEM((hops * side, tb, f // 4), BF16),
            pltpu.VMEM((hops, tb, f // 4), BF16),
            pltpu.SemaphoreType.DMA((hops * side,)), pltpu.SemaphoreType.DMA((hops * side,)),
            pltpu.SemaphoreType.DMA((hops,)), pltpu.SemaphoreType.DMA((hops,)),
            pltpu.SemaphoreType.DMA((2,)), pltpu.SemaphoreType.DMA((2,)),
        ],
        compiler_params=pltpu.CompilerParams(collective_id=collective_id, has_side_effects=True, vmem_limit_bytes=40 * 1024 * 1024),
        cost_estimate=pl.CostEstimate(flops=40_000_000_000, bytes_accessed=4 * t * k, transcendentals=0),
    )(left.reshape(chips, 2, tb, k), right)


def gelu_parts(up):
    c = math.sqrt(2.0 / math.pi)
    sq = up * up
    th = jnp.tanh(c * (up + 0.044715 * (sq * up)))
    cdf = 0.5 + 0.5 * th
    slope = cdf + up * (0.5 * (1.0 - th * th)) * (c + (3 * 0.044715 * c) * sq)
    return up * cdf, slope


def gather_mlp_kernel(n, own_ref, up_ref, down_ref, dy_ref, b1_ref, gelu_ref, d_up_ref,
                      b1, acc, dg, dy_buf, a_send, a_recv, b_send, b_recv, x_send, x_recv, dy_sem, out_sem):
    me = lax.axis_index('model')
    my_core = lax.rem(me, 2)
    _, h = own_ref.shape
    width = h // 4
    side = math.isqrt(n // 2)
    rounds = side * side
    peer = {'model': me + 1 - 2 * my_core}

    def dy_copy(t):
        return pltpu.make_async_copy(dy_ref.at[t], dy_buf.at[lax.rem(t, 2)], dy_sem.at[lax.rem(t, 2)])

    dy_copy(0).start()
    dy_copy(1).start()
    greet_neighbours(n)

    def cols_of(q):
        return pl.ds(pl.multiple_of(q * width, width), width)

    def place(q, r):
        _, _, sign, a, b, chip_at = ring_place(n, q)
        return chip_at(a - sign * lax.rem(r, side), b - sign * (r // side))

    def along_a(q, j, src, blk):
        _, core, sign, a, b, chip_at = ring_place(n, q)
        at = q * (side - 1) + j
        return pltpu.make_async_remote_copy(
            src, b1.at[blk, :, cols_of(q)], a_send.at[at], a_recv.at[at], device_id={'model': chip_at(a + sign, b) * 2 + core}, device_id_type=MESH)

    def along_b(q, r, src, blk):
        _, core, sign, a, b, chip_at = ring_place(n, q)
        at = q * (rounds - side) + r
        return pltpu.make_async_remote_copy(
            src, b1.at[blk, :, cols_of(q)], b_send.at[at], b_recv.at[at], device_id={'model': chip_at(a, b + sign) * 2 + core}, device_id_type=MESH)

    def across(q, r, src, blk):
        at = q * rounds + r
        return pltpu.make_async_remote_copy(
            src, b1.at[blk, :, cols_of(q)], x_send.at[at], x_recv.at[at], device_id=peer, device_id_type=MESH)

    def keep(q, blk):
        cols = cols_of(q)
        pltpu.make_async_copy(b1.at[blk, :, cols], b1_ref.at[blk, :, cols], out_sem).start()

    def add_up(q, blk, value):
        acc[blk] += mm(value, up_ref[cols_of(q), :], 1, 0)

    def back_proj(t):
        dy_copy(t).wait()
        dg[t] = mm(dy_buf[lax.rem(t, 2)], down_ref[...], 1, 1).astype(BF16)

        @pl.when(t + 2 < n)
        def _():
            dy_copy(t + 2).start()

    def own_round(q, _):
        cols = cols_of(q)
        src = own_ref.at[:, cols]
        along_a(q, 0, src, me).start()
        along_b(q, 0, src, me).start()
        across(q, 0, src, me).start()
        return 0

    lax.fori_loop(0, 4, own_round, 0)
    acc[...] = jnp.zeros_like(acc)
    b1[me] = own_ref[...]
    acc[me] = mm(own_ref[...], up_ref[...], 1, 0)

    def pass_on(t):
        r, q = t // 4, lax.rem(t, 4)
        s, j = r // side, lax.rem(r, side)
        blk = place(q, r) * 2 + my_core
        src = b1.at[blk, :, cols_of(q)]

        @pl.when(s == 0)
        def _():
            along_a(q, j - 1, src, blk).wait_recv()

            @pl.when(j < side - 1)
            def _():
                along_a(q, j, src, blk).start()

        @pl.when(s > 0)
        def _():
            along_b(q, r - side, src, blk).wait_recv()

        @pl.when(s < side - 1)
        def _():
            along_b(q, r, src, blk).start()

        across(q, r, src, blk).start()
        keep(q, blk)
        add_up(q, blk, b1[blk, :, cols_of(q)])
        return 0

    def take_across(q, r):
        blk = place(q, r) * 2 + 1 - my_core
        across(q, r, b1.at[blk, :, cols_of(q)], blk).wait_recv()
        keep(q, blk)
        add_up(q, blk, b1[blk, :, cols_of(q)])

    def main_round(t, _):
        pass_on(t)
        r, q = t // 4, lax.rem(t, 4)
        take_across(q, r - 1)

        @pl.when(lax.rem(t, 2) == 0)
        def _():
            back_proj(t // 2 - 2)

        return 0

    lax.fori_loop(4, 4 * rounds, main_round, 0)
    back_proj(n - 2)
    back_proj(n - 1)

    def final_across(q, _):
        take_across(q, rounds - 1)
        keep(q, me)
        return 0

    lax.fori_loop(0, 4, final_across, 0)

    def activate(t, _):
        up = acc[t].astype(BF16).astype(F32)
        value, slope = gelu_parts(up)
        gelu_ref[t] = value.astype(BF16)
        d_up_ref[t] = (dg[t].astype(F32) * slope).astype(BF16)
        return 0

    lax.fori_loop(0, n, activate, 0)

    def drain(t, _):
        q, r = t // rounds, lax.rem(t, rounds)
        blk = place(q, r) * 2 + my_core
        src = b1.at[blk, :, cols_of(q)]
        across(q, r, src, blk).wait_send()

        @pl.when(r < rounds - side)
        def _():
            along_b(q, r, src, blk).wait_send()

        @pl.when(r < side - 1)
        def _():
            along_a(q, r, src, blk).wait_send()

        return 0

    lax.fori_loop(0, 4 * rounds, drain, 0)
    pltpu.make_async_copy(b1, b1_ref, out_sem).wait()


def gather_mlp(n, own, w_up, w_down, dy, collective_id):
    tb, h = own.shape
    f = w_up.shape[1]
    side = math.isqrt(n // 2)
    rounds = side * side
    vmem = pl.BlockSpec(memory_space=pltpu.VMEM)
    anyspace = pl.BlockSpec(memory_space=pl.ANY)
    a_hops, b_hops, x_hops = 4 * (side - 1), 4 * (rounds - side), 4 * rounds
    sems = [pltpu.SemaphoreType.DMA((k,)) for k in (a_hops, a_hops, b_hops, b_hops, x_hops, x_hops, 2)]
    return pl.pallas_call(
        functools.partial(gather_mlp_kernel, n),
        out_shape=[
            jax.ShapeDtypeStruct((n, tb, h), BF16), jax.ShapeDtypeStruct((n, tb, f), BF16), jax.ShapeDtypeStruct((n, tb, f), BF16),
        ],
        in_specs=[vmem, vmem, vmem, anyspace],
        out_specs=[anyspace, vmem, vmem],
        scratch_shapes=[
            pltpu.VMEM((n, tb, h), BF16), pltpu.VMEM((n, tb, f), F32), pltpu.VMEM((n, tb, f), BF16), pltpu.VMEM((2, tb, h), BF16),
            *sems, pltpu.SemaphoreType.DMA,
        ],
        compiler_params=pltpu.CompilerParams(collective_id=collective_id, has_side_effects=True, vmem_limit_bytes=50 * 1024 * 1024),
        cost_estimate=pl.CostEstimate(flops=40_000_000_000, bytes_accessed=4 * n * tb * h, transcendentals=0),
        name='gather_mlp',
    )(own, w_up, w_down, dy.reshape(n, tb, h))


def ln_rows(z, gain):
    wide = z.astype(F32)
    mean = jnp.mean(wide, axis=-1, keepdims=True)
    cen = wide - mean
    rstd = lax.rsqrt(jnp.mean(cen * cen, axis=-1, keepdims=True) + LN_EPS)
    hat = cen * rstd
    return (hat * gain.astype(F32)).astype(BF16), hat, rstd


def ln_back(d_out, hat, rstd, gain):
    d_wide = d_out.astype(F32)
    d_hat = d_wide * gain.astype(F32)
    mean_a = jnp.mean(d_hat, axis=-1, keepdims=True)
    mean_b = jnp.mean(d_hat * hat, axis=-1, keepdims=True)
    return (rstd * (d_hat - mean_a - hat * mean_b)).astype(BF16), jnp.sum(d_wide * hat, axis=0)


def solution(mesh):
    n = mesh.shape['model']

    def layer(x_in, seg_ids, gain_one, w_qkv, w_out, gain_two, w_up, w_down, d_y):
        x = x_in[0]
        dy = d_y[0]
        seg = seg_ids[0]
        t, h = x.shape
        n_local, hd = w_out.shape[:2]
        inner = n * n_local * hd
        ts = t // n
        bq = min(512, t)
        bk = min(512, t)
        me = lax.axis_index('model')

        wo_full = lax.all_gather(w_out, 'model', axis=0, tiled=True).reshape(inner, h)

        start = document_starts(seg)
        tab = block_table(seg, start, bq, bk)
        start_row = start.reshape(1, t)

        a_full, q, k, v, qkvt = ln_qkv(x, gain_one, w_qkv.T)
        ot, lse = attention_forward(k, qkvt, start_row, tab, bq, bk)
        o_mine = exchange(n, ot, (n, hd, ts), column_block(ts), leading, 0)

        x_s = lax.dynamic_slice(x, (me * ts, 0), (ts, h))
        dy_s = lax.dynamic_slice(dy, (me * ts, 0), (ts, h))
        proj = mm(o_mine.reshape(inner, ts), wo_full, 0, 0)
        resid = (x_s.astype(F32) + proj).astype(BF16)
        b1_s, hat_two, rstd_two = ln_rows(resid, gain_two)
        b1, gelu_out, d_up = (z.reshape(t, z.shape[-1]) for z in gather_mlp(n, b1_s, w_up, w_down, dy, 6))
        d_b1 = matmul_reduce_scatter(n, d_up, w_up, 1, 3)
        late_gelu, d_b1 = lax.optimization_barrier((gelu_out, d_b1))
        part_two = matmul_reduce_scatter(n, late_gelu, w_down, 0, 4)
        late_gelu, late_up, part_two = lax.optimization_barrier((late_gelu, d_up, part_two))
        d_w_down = mm(late_gelu, dy, 0, 0).astype(BF16)
        d_w_up = mm(b1, late_up, 0, 0).astype(BF16)

        d_ln, d_gain_two = ln_back(d_b1, hat_two, rstd_two, gain_two)
        d_resid_s = dy_s + d_ln
        d_heads = mm(wo_full, d_resid_s, 1, 1).astype(BF16).reshape(n, hd, ts)
        dot = exchange(n, d_heads, (hd, t), leading, column_block(ts), 1)
        d_resid = lax.all_gather(d_resid_s, 'model', axis=0, tiled=True)

        d_qkv = attention_backward(q, k, v, qkvt, ot, dot, lse, start_row, tab, bq, bk)
        y_s = (resid.astype(F32) + part_two.astype(F32)).astype(BF16)
        y_out = lax.all_gather(y_s[None], 'model', axis=1, tiled=True)
        d_norm = matmul_reduce_scatter(n, d_qkv, w_qkv.T, 0, 5)
        d_w_qkv = mm(a_full, d_qkv, 0, 0).astype(BF16)
        d_w_out = mm(ot, d_resid, 1, 0).astype(BF16)

        _, hat_one, rstd_one = ln_rows(x_s, gain_one)
        d_ln, d_gain_one = ln_back(d_norm, hat_one, rstd_one, gain_one)
        d_x = lax.all_gather((d_resid_s + d_ln)[None], 'model', axis=1, tiled=True)
        gains = jnp.concatenate([d_gain_one, d_gain_two]).reshape(1, 2 * h)
        gains = exchange(n, gains, (n, 1, 2 * h), whole_ref, leading, 2)
        gains = jnp.sum(gains, axis=(0, 1)).astype(BF16)
        return (y_out, d_x, d_w_qkv, d_w_out.reshape(n_local, hd, h), d_w_up, d_w_down, gains[:h], gains[h:])

    in_specs = (P('data'), P('data'), P(), P(None, 'model'), P('model'), P(), P(None, 'model'), P('model'), P('data'))
    out_specs = (P('data'), P('data'), P('data', 'model'), P(('data', 'model')), P('data', 'model'), P(('data', 'model')), P('data'), P('data'))
    return jax.shard_map(layer, mesh=mesh, in_specs=in_specs, out_specs=out_specs, check_vma=False)
```

```python
import functools
import math

import jax
import jax.numpy as jnp
from jax import lax
from jax.experimental import pallas as pl
from jax.experimental.pallas import tpu as pltpu
from jax.sharding import PartitionSpec as P


LN_EPS = 1e-5
LOG2E = 1.4426950408889634
NEG = -1e30
MESH = pl.DeviceIdType.MESH
VMEM_LIMIT = 60 * 1024 * 1024
F32 = jnp.float32
BF16 = jnp.bfloat16


def mm(a, b, ca, cb):
    return lax.dot_general(a, b, (((ca,), (cb,)), ((), ())), preferred_element_type=F32)


def ln_qkv_kernel(x_ref, g_ref, w_ref, a_ref, q_ref, k_ref, v_ref, t_ref):
    x = x_ref[...].astype(F32)
    mean = jnp.mean(x, axis=-1, keepdims=True)
    cen = x - mean
    var = jnp.mean(cen * cen, axis=-1, keepdims=True)
    a = (cen * lax.rsqrt(var + LN_EPS) * g_ref[...].astype(F32)).astype(BF16)
    a_ref[...] = a
    qkv = mm(a, w_ref[...], 1, 1)
    t_ref[...] = qkv.T.astype(BF16)
    hd = q_ref.shape[1]
    qkv = qkv.astype(BF16)
    q_ref[...] = qkv[:, :hd]
    k_ref[...] = qkv[:, hd:2 * hd]
    v_ref[...] = qkv[:, 2 * hd:]


def ln_qkv(x, g, w):
    t, h = x.shape
    c = w.shape[0]
    hd = c // 3
    bt = min(512, t)
    row = lambda n: pl.BlockSpec((bt, n), lambda i: (i, 0))
    return pl.pallas_call(
        ln_qkv_kernel,
        grid=(t // bt,),
        in_specs=[row(h), pl.BlockSpec((1, h), lambda i: (0, 0)), pl.BlockSpec((c, h), lambda i: (0, 0))],
        out_specs=[row(h), row(hd), row(hd), row(hd), pl.BlockSpec((c, bt), lambda i: (0, i))],
        out_shape=[jax.ShapeDtypeStruct((t, h), BF16)] + [jax.ShapeDtypeStruct((t, hd), BF16)] * 3 + [jax.ShapeDtypeStruct((c, t), BF16)],
        compiler_params=pltpu.CompilerParams(vmem_limit_bytes=VMEM_LIMIT),
        cost_estimate=pl.CostEstimate(flops=2 * t * h * c + 20 * t * h, bytes_accessed=4 * t * h, transcendentals=0),
        name='ln_qkv',
    )(x, g.reshape(1, h), w)


def visible(kb, bk, q0, bq, start):
    k_pos = kb * bk + lax.broadcasted_iota(jnp.int32, (bk, bq), 0)
    q_pos = q0 + lax.broadcasted_iota(jnp.int32, (bk, bq), 1)
    return (k_pos <= q_pos) & (k_pos >= start)


def masked_block(t, lo, mid, hi):
    return jnp.where(t < mid - lo, lo + t, hi + t - (mid - lo))


def attn_fwd_kernel(bk, tab_ref, k_ref, qt_ref, vt_ref, start_ref, ot_ref, lse_ref):
    i = pl.program_id(0)
    bq = qt_ref.shape[1]
    hd = qt_ref.shape[0]
    scale = LOG2E * hd ** -0.5
    qt = qt_ref[...]
    start = start_ref[...]
    lo, mid, hi, top = tab_ref[0, i], tab_ref[1, i], tab_ref[2, i], tab_ref[3, i]

    def step(masked, kb, carry):
        m, l, acc = carry
        k0 = pl.multiple_of(kb * bk, bk)
        s = mm(k_ref[pl.ds(k0, bk), :], qt, 1, 0)
        if masked:
            s = jnp.where(visible(kb, bk, i * bq, bq, start), s, NEG)
        m_new = jnp.maximum(m, jnp.max(s, axis=0, keepdims=True))
        p = jnp.exp2((s - m_new) * scale)
        alpha = jnp.exp2((m - m_new) * scale)
        l = l * alpha + jnp.sum(p, axis=0, keepdims=True)
        acc = acc * alpha + mm(vt_ref[:, pl.ds(k0, bk)], p.astype(BF16), 1, 0)
        return m_new, l, acc

    carry = (jnp.full((1, bq), NEG, F32), jnp.zeros((1, bq), F32), jnp.zeros((hd, bq), F32))
    carry = lax.fori_loop(mid, hi, functools.partial(step, False), carry)
    m, l, acc = lax.fori_loop(0, mid - lo + top - hi, lambda t, c: step(True, masked_block(t, lo, mid, hi), c), carry)
    ot_ref[...] = (acc / l).astype(BF16)
    lse_ref[...] = m * scale + jnp.log2(l)


def document_starts(seg):
    t = seg.shape[0]
    wide = 128
    pos = jnp.arange(t, dtype=jnp.int32).reshape(t // wide, wide)
    before = jnp.concatenate([seg[:1], seg[:-1]])
    mark = jnp.where((seg != before).reshape(pos.shape), pos, 0)
    lane = jnp.arange(wide)
    inner = jnp.max(jnp.where(lane[None, :, None] >= lane[None, None, :], mark[:, None, :], 0), axis=-1)
    row = jnp.arange(t // wide)
    prior = jnp.max(jnp.where(row[:, None] > row[None, :], inner[:, -1][None, :], 0), axis=-1)
    return jnp.maximum(inner, prior[:, None]).reshape(t)


def block_table(seg, start, bq, bk):
    t = seg.shape[0]
    nq = t // bq
    q0 = jnp.arange(nq, dtype=jnp.int32) * bq
    first = start.reshape(nq, bq)[:, 0]
    last = start.reshape(nq, bq)[:, -1]
    lo = first // bk
    hi = q0 // bk
    top = (q0 + bq + bk - 1) // bk
    mid = jnp.clip((last + bk - 1) // bk, lo, hi)
    return jnp.stack([lo, mid, hi, top])


def attention_forward(k, qkvt, start, tab, bq, bk):
    t, hd = k.shape
    return pl.pallas_call(
        functools.partial(attn_fwd_kernel, bk),
        grid_spec=pltpu.PrefetchScalarGridSpec(
            num_scalar_prefetch=1,
            grid=(t // bq,),
            in_specs=[
                pl.BlockSpec((t, hd), lambda i, *_: (0, 0)),
                pl.BlockSpec((hd, bq), lambda i, *_: (0, i)),
                pl.BlockSpec((hd, t), lambda i, *_: (2, 0)),
                pl.BlockSpec((1, bq), lambda i, *_: (0, i)),
            ],
            out_specs=[pl.BlockSpec((hd, bq), lambda i, *_: (0, i)), pl.BlockSpec((1, bq), lambda i, *_: (0, i))],
        ),
        out_shape=[jax.ShapeDtypeStruct((hd, t), BF16), jax.ShapeDtypeStruct((1, t), F32)],
        compiler_params=pltpu.CompilerParams(vmem_limit_bytes=VMEM_LIMIT),
        cost_estimate=pl.CostEstimate(flops=16 * t * t * hd, bytes_accessed=8 * t * hd, transcendentals=t * t // 2),
        name='attn_fwd',
    )(tab, k, qkvt, qkvt, start)


def attn_bwd_kernel(bk, tab_ref, q_ref, k_ref, v_ref, t_ref, ot_ref, dot_ref, lse_ref, start_ref, d_ref, dk_acc, dv_acc):
    i = pl.program_id(0)
    bq, hd = q_ref.shape
    scale = LOG2E * hd ** -0.5
    t = k_ref.shape[0]

    @pl.when(i == 0)
    def _():
        dk_acc[...] = jnp.zeros_like(dk_acc)
        dv_acc[...] = jnp.zeros_like(dv_acc)

    c0 = pl.multiple_of(i * bq, bq)
    q = q_ref[...]
    qt = t_ref[:hd, pl.ds(c0, bq)]
    dot_blk = dot_ref[...]
    dot_wide = dot_blk.astype(F32)
    d_out = dot_wide.T.astype(BF16)
    delta = jnp.sum(dot_wide * ot_ref[...].astype(F32), axis=0, keepdims=True)
    lse = lse_ref[...]
    start = start_ref[...]
    lo, mid, hi, top = tab_ref[0, i], tab_ref[1, i], tab_ref[2, i], tab_ref[3, i]

    def step(masked, kb, dqt):
        k0 = pl.multiple_of(kb * bk, bk)
        rows = pl.ds(k0, bk)
        s = mm(k_ref[rows, :], qt, 1, 0)
        p = jnp.exp2(s * scale - lse)
        if masked:
            p = jnp.where(visible(kb, bk, i * bq, bq, start), p, 0.0)
        dp = mm(v_ref[rows, :], dot_blk, 1, 0)
        ds = (p * (dp - delta)).astype(BF16)
        dv_acc[rows, :] += mm(p.astype(BF16), d_out, 1, 0)
        dk_acc[rows, :] += mm(ds, q, 1, 0)
        return dqt + mm(t_ref[hd:2 * hd, rows], ds, 1, 0)

    dqt = jnp.zeros((hd, bq), F32)
    dqt = lax.fori_loop(mid, hi, functools.partial(step, False), dqt)
    dqt = lax.fori_loop(0, mid - lo + top - hi, lambda t, c: step(True, masked_block(t, lo, mid, hi), c), dqt)
    d_ref[pl.ds(c0, bq), :hd] = (dqt * hd ** -0.5).T.astype(BF16)

    @pl.when(i == pl.num_programs(0) - 1)
    def _():
        def put(r, _):
            rows = pl.ds(pl.multiple_of(r * bk, bk), bk)
            d_ref[rows, hd:2 * hd] = (dk_acc[rows, :] * hd ** -0.5).astype(BF16)
            d_ref[rows, 2 * hd:] = dv_acc[rows, :].astype(BF16)
            return 0

        lax.fori_loop(0, t // bk, put, 0)


def attention_backward(q, k, v, qkvt, ot, dot, lse, start, tab, bq, bk):
    t, hd = k.shape
    whole = lambda shape: pl.BlockSpec(shape, lambda i, *_: (0, 0))
    cols = lambda n: pl.BlockSpec((n, bq), lambda i, *_: (0, i))
    return pl.pallas_call(
        functools.partial(attn_bwd_kernel, bk),
        grid_spec=pltpu.PrefetchScalarGridSpec(
            num_scalar_prefetch=1,
            grid=(t // bq,),
            in_specs=[
                pl.BlockSpec((bq, hd), lambda i, *_: (i, 0)), whole((t, hd)), whole((t, hd)), whole((3 * hd, t)),
                cols(hd), cols(hd), cols(1), cols(1),
            ],
            out_specs=whole((t, 3 * hd)),
            scratch_shapes=[pltpu.VMEM((t, hd), F32), pltpu.VMEM((t, hd), F32)],
        ),
        out_shape=jax.ShapeDtypeStruct((t, 3 * hd), BF16),
        compiler_params=pltpu.CompilerParams(vmem_limit_bytes=VMEM_LIMIT),
        cost_estimate=pl.CostEstimate(flops=40 * t * t * hd, bytes_accessed=16 * t * hd, transcendentals=t * t // 2),
        name='attn_bwd',
    )(tab, q, k, v, qkvt, ot, dot, lse, start)


def exchange_kernel(n, src_of, dst_of, in_ref, out_ref, send_sem, recv_sem, own_sem):
    me = lax.axis_index('model')
    barrier = pltpu.get_barrier_semaphore()

    def hello(off, _):
        pl.semaphore_signal(barrier, inc=1, device_id={'model': lax.rem(me + off, n)}, device_id_type=MESH)
        return 0

    lax.fori_loop(1, n, hello, 0)
    own = pltpu.make_async_copy(src_of(in_ref, me), dst_of(out_ref, me), own_sem)
    own.start()
    pl.semaphore_wait(barrier, n - 1)

    def send(off, _):
        to = lax.rem(me + off, n)
        pltpu.make_async_remote_copy(
            src_ref=src_of(in_ref, to), dst_ref=dst_of(out_ref, me), send_sem=send_sem.at[off], recv_sem=recv_sem.at[off],
            device_id={'model': to}, device_id_type=MESH,
        ).start()
        return 0

    lax.fori_loop(1, n, send, 0)

    def finish(off, _):
        to = lax.rem(me + off, n)
        come = lax.rem(me - off + n, n)
        pltpu.make_async_remote_copy(
            src_ref=src_of(in_ref, to), dst_ref=dst_of(out_ref, come), send_sem=send_sem.at[off], recv_sem=recv_sem.at[off],
            device_id={'model': to}, device_id_type=MESH,
        ).wait()
        return 0

    lax.fori_loop(1, n, finish, 0)
    own.wait()


def exchange(n, value, out_shape, src_of, dst_of, collective_id):
    return pl.pallas_call(
        functools.partial(exchange_kernel, n, src_of, dst_of),
        out_shape=jax.ShapeDtypeStruct(out_shape, value.dtype),
        in_specs=[pl.BlockSpec(memory_space=pltpu.VMEM)],
        out_specs=pl.BlockSpec(memory_space=pltpu.VMEM),
        scratch_shapes=[pltpu.SemaphoreType.DMA((n,)), pltpu.SemaphoreType.DMA((n,)), pltpu.SemaphoreType.DMA],
        compiler_params=pltpu.CompilerParams(collective_id=collective_id, has_side_effects=True),
        cost_estimate=pl.CostEstimate(flops=2_000_000_000, bytes_accessed=2 * value.size * 2, transcendentals=0),
    )(value)


def column_block(width):
    return lambda ref, j: ref.at[:, pl.ds(pl.multiple_of(j * width, width), width)]


def leading(ref, j):
    return ref.at[j]


def whole_ref(ref, j):
    return ref


def ring_place(n, q):
    me = lax.axis_index('model')
    side = math.isqrt(n // 2)
    core = lax.rem(me, 2)
    chip = me // 2
    x = lax.rem(chip, side)
    y = chip // side
    turn = q // 2
    sign = 1 - 2 * lax.rem(q, 2)
    a = x * (1 - turn) + y * turn
    b = y * (1 - turn) + x * turn

    def chip_at(pa, pb):
        pa = lax.rem(pa + 2 * side, side)
        pb = lax.rem(pb + 2 * side, side)
        return (pb * (1 - turn) + pa * turn) * side + pa * (1 - turn) + pb * turn

    return side, core, sign, a, b, chip_at


def greet_neighbours(n):
    me = lax.axis_index('model')
    barrier = pltpu.get_barrier_semaphore()
    core = lax.rem(me, 2)
    pl.semaphore_signal(barrier, inc=1, device_id={'model': me + 1 - 2 * core}, device_id_type=MESH)

    def hello(q, _):
        _, core, sign, a, b, chip_at = ring_place(n, q)
        pl.semaphore_signal(barrier, inc=1, device_id={'model': chip_at(a + sign, b) * 2 + core}, device_id_type=MESH)
        return 0

    lax.fori_loop(0, 4, hello, 0)
    pl.semaphore_wait(barrier, 5)


def reduce_kernel(n, r_dim, l_ref, r_ref, out_ref, l_peer, r_peer, part, first, slot1, slot2, s_send, s_recv, p_send, p_recv, x_send, x_recv):
    me = lax.axis_index('model')
    my_core = lax.rem(me, 2)
    side, _, _, tb, k = l_ref.shape
    width = out_ref.shape[1] // 4
    greet_neighbours(n)
    peer = {'model': me + 1 - 2 * my_core}
    swap = [
        pltpu.make_async_remote_copy(src, dst, x_send.at[i], x_recv.at[i], device_id=peer, device_id_type=MESH)
        for i, (src, dst) in enumerate([(r_ref, r_peer), (l_ref.at[:, :, 1 - my_core], l_peer)])
    ]
    for copy in swap:
        copy.start()

    def group(s, q):
        _, _, sign, a, _, _ = ring_place(n, q)
        at = lax.rem(a - sign * (1 + s) + 2 * side, side)
        mine, other = (l_ref[:, at, my_core], l_peer[:, at]) if q < 2 else (l_ref[at, :, my_core], l_peer[at])
        cols = pl.ds(q * width, width)
        r_mine, r_other = (r_ref[:, cols], r_peer[:, cols]) if r_dim == 0 else (r_ref[cols, :], r_peer[cols, :])
        total = mm(mine.reshape(side * tb, k), r_mine, 1, r_dim) + mm(other.reshape(side * tb, k), r_other, 1, r_dim)
        part[lax.rem(s, 2), q] = total.reshape(side, tb, width)

    def own_part(q, s, j):
        _, _, sign, _, b, _ = ring_place(n, q)
        return part[lax.rem(s, 2), q, lax.rem(b - sign * (1 + j) + 2 * side, side)]

    def hop(q, s, j, src):
        _, core, sign, a, b, chip_at = ring_place(n, q)
        at = (q * (side - 1) + s) * side + j
        return pltpu.make_async_remote_copy(
            src, slot1.at[at], s_send.at[at], s_recv.at[at], device_id={'model': chip_at(a + sign, b) * 2 + core}, device_id_type=MESH)

    def turn_hop(q, s, src):
        _, core, sign, a, b, chip_at = ring_place(n, q)
        at = q * (side - 1) + s
        return pltpu.make_async_remote_copy(
            src, slot2.at[at], p_send.at[at], p_recv.at[at], device_id={'model': chip_at(a, b + sign) * 2 + core}, device_id_type=MESH)

    def arrived(q, s, j):
        return (q * (side - 1) + s) * side + j

    for copy in swap:
        copy.wait()

    def start_step(s, _):
        for q in range(4):
            group(s, q)

            @pl.when(s == 0)
            def _():
                def start_round(j, _):
                    at = q * side + j
                    first[at] = own_part(q, 0, j).astype(BF16)
                    hop(q, 0, j, first.at[at]).start()
                    return 0

                lax.fori_loop(0, side, start_round, 0)

        return 0

    lax.fori_loop(0, 2, start_step, 0)

    def middle_round(t, _):
        s, rest = 1 + t // (4 * side), lax.rem(t, 4 * side)
        j, q = rest // 4, lax.rem(rest, 4)
        at = arrived(q, s - 1, j)
        hop(q, s - 1, j, slot1.at[at]).wait_recv()
        slot1[at] = (slot1[at].astype(F32) + own_part(q, s, j)).astype(BF16)
        hop(q, s, j, slot1.at[at]).start()
        for ahead in range(4):
            @pl.when((q == 3) & (j == ahead))
            def _():
                group(s + 1, ahead)

        return 0

    lax.fori_loop(0, 4 * side * (side - 2), middle_round, 0)

    def last_sum(q, j):
        at = arrived(q, side - 2, j)
        hop(q, side - 2, j, slot1.at[at]).wait_recv()
        return at, slot1[at].astype(F32) + own_part(q, side - 1, j)

    def turn_first(q, _):
        at, total = last_sum(q, 0)
        slot1[at] = total.astype(BF16)
        turn_hop(q, 0, slot1.at[at]).start()
        return 0

    lax.fori_loop(0, 4, turn_first, 0)

    def turn_round(t, _):
        s, q = 1 + t // 4, lax.rem(t, 4)
        _, total = last_sum(q, s)
        at = q * (side - 1) + s - 1
        turn_hop(q, s - 1, slot2.at[at]).wait_recv()
        slot2[at] = (slot2[at].astype(F32) + total).astype(BF16)
        turn_hop(q, s, slot2.at[at]).start()
        return 0

    lax.fori_loop(0, 4 * (side - 2), turn_round, 0)

    def turn_last(q, _):
        _, total = last_sum(q, side - 1)
        at = q * (side - 1) + side - 2
        turn_hop(q, side - 2, slot2.at[at]).wait_recv()
        out_ref[:, pl.ds(pl.multiple_of(q * width, width), width)] = (slot2[at].astype(F32) + total).astype(BF16)
        return 0

    lax.fori_loop(0, 4, turn_last, 0)

    def drain(t, _):
        q, s = t // (side - 1), lax.rem(t, side - 1)
        turn_hop(q, s, slot2.at[t]).wait_send()
        for j in range(side):
            hop(q, s, j, slot1.at[t * side + j]).wait_send()
        return 0

    lax.fori_loop(0, 4 * (side - 1), drain, 0)


def matmul_reduce_scatter(n, left, right, r_dim, collective_id):
    t, k = left.shape
    f = right.shape[1 - r_dim]
    chips = n // 2
    side = math.isqrt(chips)
    tb = t // n
    hops = 4 * (side - 1)
    vmem = pl.BlockSpec(memory_space=pltpu.VMEM)
    return pl.pallas_call(
        functools.partial(reduce_kernel, n, r_dim),
        out_shape=jax.ShapeDtypeStruct((tb, f), BF16),
        in_specs=[vmem, vmem],
        out_specs=vmem,
        scratch_shapes=[
            pltpu.VMEM((side, side, tb, k), BF16),
            pltpu.VMEM(right.shape, BF16),
            pltpu.VMEM((2, 4, side, tb, f // 4), F32),
            pltpu.VMEM((4 * side, tb, f // 4), BF16),
            pltpu.VMEM((hops * side, tb, f // 4), BF16),
            pltpu.VMEM((hops, tb, f // 4), BF16),
            pltpu.SemaphoreType.DMA((hops * side,)), pltpu.SemaphoreType.DMA((hops * side,)),
            pltpu.SemaphoreType.DMA((hops,)), pltpu.SemaphoreType.DMA((hops,)),
            pltpu.SemaphoreType.DMA((2,)), pltpu.SemaphoreType.DMA((2,)),
        ],
        compiler_params=pltpu.CompilerParams(collective_id=collective_id, has_side_effects=True, vmem_limit_bytes=48 * 1024 * 1024),
        cost_estimate=pl.CostEstimate(flops=40_000_000_000, bytes_accessed=4 * t * k, transcendentals=0),
    )(left.reshape(side, side, 2, tb, k), right)


def gelu_parts(up):
    c = math.sqrt(2.0 / math.pi)
    sq = up * up
    th = jnp.tanh(c * (up + 0.044715 * (sq * up)))
    cdf = 0.5 + 0.5 * th
    slope = cdf + up * (0.5 * (1.0 - th * th)) * (c + (3 * 0.044715 * c) * sq)
    return up * cdf, slope


def gather_mlp_kernel(n, own_ref, up_ref, down_ref, dy_ref, b1_ref, gelu_ref, d_up_ref,
                      b1, acc, dg, dy_buf, a_send, a_recv, b_send, b_recv, x_send, x_recv, dy_sem, out_sem):
    me = lax.axis_index('model')
    my_core = lax.rem(me, 2)
    tb, h = own_ref.shape
    f = up_ref.shape[1]
    width = h // 4
    side = math.isqrt(n // 2)
    rounds = side * side
    n_dy, _, _ = dy_ref.shape
    peer = {'model': me + 1 - 2 * my_core}

    def dy_copy(t):
        return pltpu.make_async_copy(dy_ref.at[t], dy_buf.at[lax.rem(t, 2)], dy_sem.at[lax.rem(t, 2)])

    dy_copy(jnp.int32(0)).start()
    dy_copy(jnp.int32(1)).start()
    greet_neighbours(n)

    def cols_of(q):
        return pl.ds(pl.multiple_of(q * width, width), width)

    def quarter(q, r, core):
        _, _, sign, a, b, chip_at = ring_place(n, q)
        chip = chip_at(a - sign * lax.rem(r, side), b - sign * (r // side))
        return b1.at[chip // side, lax.rem(chip, side), core, :, cols_of(q)]

    def along_a(q, j, src):
        _, core, sign, a, b, chip_at = ring_place(n, q)
        at = q * (side - 1) + j
        return pltpu.make_async_remote_copy(
            src, quarter(q, j, core), a_send.at[at], a_recv.at[at], device_id={'model': chip_at(a + sign, b) * 2 + core}, device_id_type=MESH)

    def along_b(q, r, src):
        _, core, sign, a, b, chip_at = ring_place(n, q)
        at = q * (rounds - side) + r
        return pltpu.make_async_remote_copy(
            src, quarter(q, r, core), b_send.at[at], b_recv.at[at], device_id={'model': chip_at(a, b + sign) * 2 + core}, device_id_type=MESH)

    def across(q, r, src, core):
        at = q * rounds + r
        return pltpu.make_async_remote_copy(
            src, quarter(q, r, core), x_send.at[at], x_recv.at[at], device_id=peer, device_id_type=MESH)

    def back_proj(t):
        dy_copy(t).wait()
        dg[t] = mm(dy_buf[lax.rem(t, 2)], down_ref[...], 1, 1).astype(BF16)

        @pl.when(t + 2 < n_dy)
        def _():
            dy_copy(t + 2).start()

    def own_round(q, _):
        src = own_ref.at[:, cols_of(q)]
        along_a(q, 0, src).start()
        along_b(q, 0, src).start()
        across(q, 0, src, my_core).start()
        return 0

    lax.fori_loop(0, 4, own_round, 0)
    b1[me // (2 * side), lax.rem(me // 2, side), my_core] = own_ref[...]
    acc[...] = jnp.zeros_like(acc)

    def add_up(s, q, core):
        _, _, sign, _, b, _ = ring_place(n, q)
        at = lax.rem(b - sign * s + 2 * side, side)
        cols = pl.ds(q * width, width)
        if q < 2:
            pltpu.make_async_copy(b1.at[at, :, core, :, cols], b1_ref.at[at, :, core, :, cols], out_sem).start()
            value = b1[at, :, core, :, cols].reshape(side * tb, width)
        else:
            pltpu.make_async_copy(b1.at[:, at, core, :, cols], b1_ref.at[:, at, core, :, cols], out_sem).start()
            value = b1[:, at, core, :, cols].reshape(side * tb, width)
        more = mm(value, up_ref[cols, :], 1, 0).reshape(side, tb, f)
        if q < 2:
            acc[at, :, core] += more
        else:
            acc[:, at, core] += more

    def take_step(s, q):
        add_up(s, q, my_core)
        for j in range(side):
            r = s * side + j
            across(q, r, quarter(q, r, 1 - my_core), 1 - my_core).wait_recv()
        add_up(s, q, 1 - my_core)

    def main_round(t, _):
        r, q = t // 4, lax.rem(t, 4)
        s, j = r // side, lax.rem(r, side)
        src = quarter(q, r, my_core)

        @pl.when(s == 0)
        def _():
            along_a(q, j - 1, src).wait_recv()

            @pl.when(j < side - 1)
            def _():
                along_a(q, j, src).start()

        @pl.when(s > 0)
        def _():
            along_b(q, r - side, src).wait_recv()

        @pl.when(s < side - 1)
        def _():
            along_b(q, r, src).start()

        across(q, r, src, my_core).start()
        for late in range(4):
            @pl.when((q == 3) & (j == late) & (s > 0))
            def _():
                take_step(s - 1, late)

        @pl.when((q == 1) & (lax.rem(r, 2) == 1))
        def _():
            back_proj(r // 2)

        return 0

    lax.fori_loop(4, 4 * rounds, main_round, 0)
    for q in range(4):
        take_step(jnp.int32(side - 1), q)

    def activate(t, _):
        chip, core = t // 2, lax.rem(t, 2)
        piece, rows = t // 4, pl.ds(pl.multiple_of(lax.rem(t, 4) * tb, tb), tb)
        up = acc[chip // side, lax.rem(chip, side), core].astype(BF16).astype(F32)
        value, slope = gelu_parts(up)
        gelu_ref[piece, rows, :] = value.astype(BF16)
        d_up_ref[piece, rows, :] = (dg[piece, rows, :].astype(F32) * slope).astype(BF16)
        return 0

    lax.fori_loop(0, n, activate, 0)

    def drain(t, _):
        q, r = t // rounds, lax.rem(t, rounds)
        src = quarter(q, r, my_core)
        across(q, r, src, my_core).wait_send()

        @pl.when(r < rounds - side)
        def _():
            along_b(q, r, src).wait_send()

        @pl.when(r < side - 1)
        def _():
            along_a(q, r, src).wait_send()

        return 0

    lax.fori_loop(0, 4 * rounds, drain, 0)
    pltpu.make_async_copy(b1, b1_ref, out_sem).wait()


def gather_mlp(n, own, w_up, w_down, dy, collective_id):
    tb, h = own.shape
    f = w_up.shape[1]
    side = math.isqrt(n // 2)
    rounds = side * side
    vmem = pl.BlockSpec(memory_space=pltpu.VMEM)
    anyspace = pl.BlockSpec(memory_space=pl.ANY)
    a_hops, b_hops, x_hops = 4 * (side - 1), 4 * (rounds - side), 4 * rounds
    sems = [pltpu.SemaphoreType.DMA((k,)) for k in (a_hops, a_hops, b_hops, b_hops, x_hops, x_hops, 2)]
    return pl.pallas_call(
        functools.partial(gather_mlp_kernel, n),
        out_shape=[
            jax.ShapeDtypeStruct((side, side, 2, tb, h), BF16), jax.ShapeDtypeStruct((n // 4, 4 * tb, f), BF16), jax.ShapeDtypeStruct((n // 4, 4 * tb, f), BF16),
        ],
        in_specs=[vmem, vmem, vmem, anyspace],
        out_specs=[anyspace, vmem, vmem],
        scratch_shapes=[
            pltpu.VMEM((side, side, 2, tb, h), BF16), pltpu.VMEM((side, side, 2, tb, f), F32),
            pltpu.VMEM((n // 4, 4 * tb, f), BF16), pltpu.VMEM((2, 4 * tb, h), BF16),
            *sems, pltpu.SemaphoreType.DMA,
        ],
        compiler_params=pltpu.CompilerParams(collective_id=collective_id, has_side_effects=True, vmem_limit_bytes=50 * 1024 * 1024),
        cost_estimate=pl.CostEstimate(flops=40_000_000_000, bytes_accessed=4 * n * tb * h, transcendentals=0),
        name='gather_mlp',
    )(own, w_up, w_down, dy.reshape(n // 4, 4 * tb, h))


def copy_kernel(src_ref, dst_ref):
    dst_ref[...] = src_ref[...]


def copy_rows(value):
    t, h = value.shape
    bt = min(512, t)
    row = pl.BlockSpec((bt, h), lambda i: (i, 0))
    return pl.pallas_call(
        copy_kernel, grid=(t // bt,), in_specs=[row], out_specs=row, out_shape=jax.ShapeDtypeStruct((t, h), value.dtype),
        cost_estimate=pl.CostEstimate(flops=10_000_000, bytes_accessed=4 * t * h, transcendentals=0),
    )(value)


def ln_rows(z, gain):
    wide = z.astype(F32)
    mean = jnp.mean(wide, axis=-1, keepdims=True)
    cen = wide - mean
    rstd = lax.rsqrt(jnp.mean(cen * cen, axis=-1, keepdims=True) + LN_EPS)
    hat = cen * rstd
    return (hat * gain.astype(F32)).astype(BF16), hat, rstd


def ln_back(d_out, hat, rstd, gain):
    d_wide = d_out.astype(F32)
    d_hat = d_wide * gain.astype(F32)
    mean_a = jnp.mean(d_hat, axis=-1, keepdims=True)
    mean_b = jnp.mean(d_hat * hat, axis=-1, keepdims=True)
    return (rstd * (d_hat - mean_a - hat * mean_b)).astype(BF16), jnp.sum(d_wide * hat, axis=0)


def solution(mesh):
    n = mesh.shape['model']

    def layer(x_in, seg_ids, gain_one, w_qkv, w_out, gain_two, w_up, w_down, d_y):
        x = x_in[0]
        dy = d_y[0]
        seg = seg_ids[0]
        t, h = x.shape
        n_local, hd = w_out.shape[:2]
        inner = n * n_local * hd
        ts = t // n
        bq = min(512, t)
        bk = min(512, t)
        me = lax.axis_index('model')

        wo_full = lax.all_gather(w_out, 'model', axis=0, tiled=True).reshape(inner, h)

        start = document_starts(seg)
        tab = block_table(seg, start, bq, bk)
        start_row = start.reshape(1, t)

        a_full, q, k, v, qkvt = ln_qkv(x, gain_one, w_qkv.T)
        ot, lse = attention_forward(k, qkvt, start_row, tab, bq, bk)
        o_mine = exchange(n, ot, (n, hd, ts), column_block(ts), leading, 0)

        x_s = lax.dynamic_slice(x, (me * ts, 0), (ts, h))
        dy_s = lax.dynamic_slice(dy, (me * ts, 0), (ts, h))
        proj = mm(o_mine.reshape(inner, ts), wo_full, 0, 0)
        resid = (x_s.astype(F32) + proj).astype(BF16)
        b1_s, hat_two, rstd_two = ln_rows(resid, gain_two)
        b1, gelu_out, d_up = (z.reshape(t, z.shape[-1]) for z in gather_mlp(n, b1_s, w_up, w_down, dy, 6))
        d_b1 = matmul_reduce_scatter(n, d_up, w_up, 1, 3)
        d_ln, d_gain_two = ln_back(d_b1, hat_two, rstd_two, gain_two)
        d_resid_s = dy_s + d_ln
        d_resid = lax.all_gather(d_resid_s, 'model', axis=0, tiled=True)
        late_gelu, _ = lax.optimization_barrier((gelu_out, d_resid_s))
        part_two = matmul_reduce_scatter(n, late_gelu, w_down, 0, 4)
        late_gelu, late_up, part_two = lax.optimization_barrier((late_gelu, d_up, part_two))
        d_w_down = mm(late_gelu, dy, 0, 0).astype(BF16)
        d_w_up = mm(b1, late_up, 0, 0).astype(BF16)

        d_heads = mm(wo_full, d_resid_s, 1, 1).astype(BF16).reshape(n, hd, ts)
        dot = exchange(n, d_heads, (hd, t), leading, column_block(ts), 1)

        d_qkv = attention_backward(q, k, v, qkvt, ot, dot, lse, start_row, tab, bq, bk)
        y_s = (resid.astype(F32) + part_two.astype(F32)).astype(BF16)
        y_out = lax.all_gather(y_s, 'model', axis=0, tiled=True)
        y_out = copy_rows(y_out)[None]
        d_norm = matmul_reduce_scatter(n, d_qkv, w_qkv.T, 0, 5)
        d_w_qkv = mm(a_full, d_qkv, 0, 0).astype(BF16)
        d_w_out = mm(ot, d_resid, 1, 0).astype(BF16)

        _, hat_one, rstd_one = ln_rows(x_s, gain_one)
        d_ln, d_gain_one = ln_back(d_norm, hat_one, rstd_one, gain_one)
        d_x = lax.all_gather((d_resid_s + d_ln)[None], 'model', axis=1, tiled=True)
        gains = jnp.concatenate([d_gain_one, d_gain_two]).reshape(1, 2 * h)
        gains = exchange(n, gains, (n, 1, 2 * h), whole_ref, leading, 2)
        gains = jnp.sum(gains, axis=(0, 1)).astype(BF16)
        return (y_out, d_x, d_w_qkv, d_w_out.reshape(n_local, hd, h), d_w_up, d_w_down, gains[:h], gains[h:])

    in_specs = (P('data'), P('data'), P(), P(None, 'model'), P('model'), P(), P(None, 'model'), P('model'), P('data'))
    out_specs = (P('data'), P('data'), P('data', 'model'), P(('data', 'model')), P('data', 'model'), P(('data', 'model')), P('data'), P('data'))
    return jax.shard_map(layer, mesh=mesh, in_specs=in_specs, out_specs=out_specs, check_vma=False)
```

```python
import functools
import math

import jax
import jax.numpy as jnp
from jax import lax
from jax.experimental import pallas as pl
from jax.experimental.pallas import tpu as pltpu
from jax.sharding import PartitionSpec as P


LN_EPS = 1e-5
LOG2E = 1.4426950408889634
NEG = -1e30
MESH = pl.DeviceIdType.MESH
VMEM_LIMIT = 60 * 1024 * 1024
F32 = jnp.float32
BF16 = jnp.bfloat16


def mm(a, b, ca, cb):
    return lax.dot_general(a, b, (((ca,), (cb,)), ((), ())), preferred_element_type=F32)


def ln_qkv_kernel(x_ref, g_ref, w_ref, a_ref, q_ref, k_ref, v_ref, t_ref):
    x = x_ref[...].astype(F32)
    mean = jnp.mean(x, axis=-1, keepdims=True)
    cen = x - mean
    var = jnp.mean(cen * cen, axis=-1, keepdims=True)
    a = (cen * lax.rsqrt(var + LN_EPS) * g_ref[...].astype(F32)).astype(BF16)
    a_ref[...] = a
    qkv = mm(a, w_ref[...], 1, 1)
    t_ref[...] = qkv.T.astype(BF16)
    hd = q_ref.shape[1]
    qkv = qkv.astype(BF16)
    q_ref[...] = qkv[:, :hd]
    k_ref[...] = qkv[:, hd:2 * hd]
    v_ref[...] = qkv[:, 2 * hd:]


def ln_qkv(x, g, w):
    t, h = x.shape
    c = w.shape[0]
    hd = c // 3
    bt = min(512, t)
    row = lambda n: pl.BlockSpec((bt, n), lambda i: (i, 0))
    return pl.pallas_call(
        ln_qkv_kernel,
        grid=(t // bt,),
        in_specs=[row(h), pl.BlockSpec((1, h), lambda i: (0, 0)), pl.BlockSpec((c, h), lambda i: (0, 0))],
        out_specs=[row(h), row(hd), row(hd), row(hd), pl.BlockSpec((c, bt), lambda i: (0, i))],
        out_shape=[jax.ShapeDtypeStruct((t, h), BF16)] + [jax.ShapeDtypeStruct((t, hd), BF16)] * 3 + [jax.ShapeDtypeStruct((c, t), BF16)],
        compiler_params=pltpu.CompilerParams(vmem_limit_bytes=VMEM_LIMIT),
        cost_estimate=pl.CostEstimate(flops=2 * t * h * c + 20 * t * h, bytes_accessed=4 * t * h, transcendentals=0),
        name='ln_qkv',
    )(x, g.reshape(1, h), w)


def visible(kb, bk, q0, bq, start):
    k_pos = kb * bk + lax.broadcasted_iota(jnp.int32, (bk, bq), 0)
    q_pos = q0 + lax.broadcasted_iota(jnp.int32, (bk, bq), 1)
    return (k_pos <= q_pos) & (k_pos >= start)


def masked_block(t, lo, mid, hi):
    return jnp.where(t < mid - lo, lo + t, hi + t - (mid - lo))


def attn_fwd_kernel(bk, tab_ref, k_ref, qt_ref, vt_ref, start_ref, ot_ref, lse_ref):
    i = pl.program_id(0)
    bq = qt_ref.shape[1]
    hd = qt_ref.shape[0]
    scale = LOG2E * hd ** -0.5
    qt = qt_ref[...]
    start = start_ref[...]
    lo, mid, hi, top = tab_ref[0, i], tab_ref[1, i], tab_ref[2, i], tab_ref[3, i]

    def step(masked, kb, carry):
        m, l, acc = carry
        k0 = pl.multiple_of(kb * bk, bk)
        s = mm(k_ref[pl.ds(k0, bk), :], qt, 1, 0)
        if masked:
            s = jnp.where(visible(kb, bk, i * bq, bq, start), s, NEG)
        m_new = jnp.maximum(m, jnp.max(s, axis=0, keepdims=True))
        p = jnp.exp2((s - m_new) * scale)
        alpha = jnp.exp2((m - m_new) * scale)
        l = l * alpha + jnp.sum(p, axis=0, keepdims=True)
        acc = acc * alpha + mm(vt_ref[:, pl.ds(k0, bk)], p.astype(BF16), 1, 0)
        return m_new, l, acc

    carry = (jnp.full((1, bq), NEG, F32), jnp.zeros((1, bq), F32), jnp.zeros((hd, bq), F32))
    carry = lax.fori_loop(mid, hi, functools.partial(step, False), carry)
    m, l, acc = lax.fori_loop(0, mid - lo + top - hi, lambda t, c: step(True, masked_block(t, lo, mid, hi), c), carry)
    ot_ref[...] = (acc / l).astype(BF16)
    lse_ref[...] = m * scale + jnp.log2(l)


def document_starts(seg):
    t = seg.shape[0]
    wide = 128
    pos = jnp.arange(t, dtype=jnp.int32).reshape(t // wide, wide)
    before = jnp.concatenate([seg[:1], seg[:-1]])
    mark = jnp.where((seg != before).reshape(pos.shape), pos, 0)
    lane = jnp.arange(wide)
    inner = jnp.max(jnp.where(lane[None, :, None] >= lane[None, None, :], mark[:, None, :], 0), axis=-1)
    row = jnp.arange(t // wide)
    prior = jnp.max(jnp.where(row[:, None] > row[None, :], inner[:, -1][None, :], 0), axis=-1)
    return jnp.maximum(inner, prior[:, None]).reshape(t)


def block_table(seg, start, bq, bk):
    t = seg.shape[0]
    nq = t // bq
    q0 = jnp.arange(nq, dtype=jnp.int32) * bq
    first = start.reshape(nq, bq)[:, 0]
    last = start.reshape(nq, bq)[:, -1]
    lo = first // bk
    hi = q0 // bk
    top = (q0 + bq + bk - 1) // bk
    mid = jnp.clip((last + bk - 1) // bk, lo, hi)
    return jnp.stack([lo, mid, hi, top])


def attention_forward(k, qkvt, start, tab, bq, bk):
    t, hd = k.shape
    return pl.pallas_call(
        functools.partial(attn_fwd_kernel, bk),
        grid_spec=pltpu.PrefetchScalarGridSpec(
            num_scalar_prefetch=1,
            grid=(t // bq,),
            in_specs=[
                pl.BlockSpec((t, hd), lambda i, *_: (0, 0)),
                pl.BlockSpec((hd, bq), lambda i, *_: (0, i)),
                pl.BlockSpec((hd, t), lambda i, *_: (2, 0)),
                pl.BlockSpec((1, bq), lambda i, *_: (0, i)),
            ],
            out_specs=[pl.BlockSpec((hd, bq), lambda i, *_: (0, i)), pl.BlockSpec((1, bq), lambda i, *_: (0, i))],
        ),
        out_shape=[jax.ShapeDtypeStruct((hd, t), BF16), jax.ShapeDtypeStruct((1, t), F32)],
        compiler_params=pltpu.CompilerParams(vmem_limit_bytes=VMEM_LIMIT),
        cost_estimate=pl.CostEstimate(flops=16 * t * t * hd, bytes_accessed=8 * t * hd, transcendentals=t * t // 2),
        name='attn_fwd',
    )(tab, k, qkvt, qkvt, start)


def attn_bwd_kernel(bk, tab_ref, q_ref, k_ref, v_ref, t_ref, ot_ref, dot_ref, lse_ref, start_ref, d_ref, dk_acc, dv_acc):
    i = pl.program_id(0)
    bq, hd = q_ref.shape
    scale = LOG2E * hd ** -0.5
    t = k_ref.shape[0]

    @pl.when(i == 0)
    def _():
        dk_acc[...] = jnp.zeros_like(dk_acc)
        dv_acc[...] = jnp.zeros_like(dv_acc)

    c0 = pl.multiple_of(i * bq, bq)
    q = q_ref[...]
    qt = t_ref[:hd, pl.ds(c0, bq)]
    dot_blk = dot_ref[...]
    dot_wide = dot_blk.astype(F32)
    d_out = dot_wide.T.astype(BF16)
    delta = jnp.sum(dot_wide * ot_ref[...].astype(F32), axis=0, keepdims=True)
    lse = lse_ref[...]
    start = start_ref[...]
    lo, mid, hi, top = tab_ref[0, i], tab_ref[1, i], tab_ref[2, i], tab_ref[3, i]

    def step(masked, kb, dqt):
        k0 = pl.multiple_of(kb * bk, bk)
        rows = pl.ds(k0, bk)
        s = mm(k_ref[rows, :], qt, 1, 0)
        p = jnp.exp2(s * scale - lse)
        if masked:
            p = jnp.where(visible(kb, bk, i * bq, bq, start), p, 0.0)
        dp = mm(v_ref[rows, :], dot_blk, 1, 0)
        ds = (p * (dp - delta)).astype(BF16)
        dv_acc[rows, :] += mm(p.astype(BF16), d_out, 1, 0)
        dk_acc[rows, :] += mm(ds, q, 1, 0)
        return dqt + mm(t_ref[hd:2 * hd, rows], ds, 1, 0)

    dqt = jnp.zeros((hd, bq), F32)
    dqt = lax.fori_loop(mid, hi, functools.partial(step, False), dqt)
    dqt = lax.fori_loop(0, mid - lo + top - hi, lambda t, c: step(True, masked_block(t, lo, mid, hi), c), dqt)
    d_ref[pl.ds(c0, bq), :hd] = (dqt * hd ** -0.5).T.astype(BF16)

    @pl.when(i == pl.num_programs(0) - 1)
    def _():
        def put(r, _):
            rows = pl.ds(pl.multiple_of(r * bk, bk), bk)
            d_ref[rows, hd:2 * hd] = (dk_acc[rows, :] * hd ** -0.5).astype(BF16)
            d_ref[rows, 2 * hd:] = dv_acc[rows, :].astype(BF16)
            return 0

        lax.fori_loop(0, t // bk, put, 0)


def attention_backward(q, k, v, qkvt, ot, dot, lse, start, tab, bq, bk):
    t, hd = k.shape
    whole = lambda shape: pl.BlockSpec(shape, lambda i, *_: (0, 0))
    cols = lambda n: pl.BlockSpec((n, bq), lambda i, *_: (0, i))
    return pl.pallas_call(
        functools.partial(attn_bwd_kernel, bk),
        grid_spec=pltpu.PrefetchScalarGridSpec(
            num_scalar_prefetch=1,
            grid=(t // bq,),
            in_specs=[
                pl.BlockSpec((bq, hd), lambda i, *_: (i, 0)), whole((t, hd)), whole((t, hd)), whole((3 * hd, t)),
                cols(hd), cols(hd), cols(1), cols(1),
            ],
            out_specs=whole((t, 3 * hd)),
            scratch_shapes=[pltpu.VMEM((t, hd), F32), pltpu.VMEM((t, hd), F32)],
        ),
        out_shape=jax.ShapeDtypeStruct((t, 3 * hd), BF16),
        compiler_params=pltpu.CompilerParams(vmem_limit_bytes=VMEM_LIMIT),
        cost_estimate=pl.CostEstimate(flops=40 * t * t * hd, bytes_accessed=16 * t * hd, transcendentals=t * t // 2),
        name='attn_bwd',
    )(tab, q, k, v, qkvt, ot, dot, lse, start)


def exchange_kernel(n, src_of, dst_of, in_ref, out_ref, send_sem, recv_sem, own_sem):
    me = lax.axis_index('model')
    barrier = pltpu.get_barrier_semaphore()

    def hello(off, _):
        pl.semaphore_signal(barrier, inc=1, device_id={'model': lax.rem(me + off, n)}, device_id_type=MESH)
        return 0

    lax.fori_loop(1, n, hello, 0)
    own = pltpu.make_async_copy(src_of(in_ref, me), dst_of(out_ref, me), own_sem)
    own.start()
    pl.semaphore_wait(barrier, n - 1)

    def send(off, _):
        to = lax.rem(me + off, n)
        pltpu.make_async_remote_copy(
            src_ref=src_of(in_ref, to), dst_ref=dst_of(out_ref, me), send_sem=send_sem.at[off], recv_sem=recv_sem.at[off],
            device_id={'model': to}, device_id_type=MESH,
        ).start()
        return 0

    lax.fori_loop(1, n, send, 0)

    def finish(off, _):
        to = lax.rem(me + off, n)
        come = lax.rem(me - off + n, n)
        pltpu.make_async_remote_copy(
            src_ref=src_of(in_ref, to), dst_ref=dst_of(out_ref, come), send_sem=send_sem.at[off], recv_sem=recv_sem.at[off],
            device_id={'model': to}, device_id_type=MESH,
        ).wait()
        return 0

    lax.fori_loop(1, n, finish, 0)
    own.wait()


def exchange(n, value, out_shape, src_of, dst_of, collective_id):
    return pl.pallas_call(
        functools.partial(exchange_kernel, n, src_of, dst_of),
        out_shape=jax.ShapeDtypeStruct(out_shape, value.dtype),
        in_specs=[pl.BlockSpec(memory_space=pltpu.VMEM)],
        out_specs=pl.BlockSpec(memory_space=pltpu.VMEM),
        scratch_shapes=[pltpu.SemaphoreType.DMA((n,)), pltpu.SemaphoreType.DMA((n,)), pltpu.SemaphoreType.DMA],
        compiler_params=pltpu.CompilerParams(collective_id=collective_id, has_side_effects=True),
        cost_estimate=pl.CostEstimate(flops=2_000_000_000, bytes_accessed=2 * value.size * 2, transcendentals=0),
    )(value)


def column_block(width):
    return lambda ref, j: ref.at[:, pl.ds(pl.multiple_of(j * width, width), width)]


def leading(ref, j):
    return ref.at[j]


def ring_place(n, q):
    me = lax.axis_index('model')
    side = math.isqrt(n // 2)
    core = lax.rem(me, 2)
    chip = me // 2
    x = lax.rem(chip, side)
    y = chip // side
    turn = q // 2
    sign = 1 - 2 * lax.rem(q, 2)
    a = x * (1 - turn) + y * turn
    b = y * (1 - turn) + x * turn

    def chip_at(pa, pb):
        pa = lax.rem(pa + 2 * side, side)
        pb = lax.rem(pb + 2 * side, side)
        return (pb * (1 - turn) + pa * turn) * side + pa * (1 - turn) + pb * turn

    return side, core, sign, a, b, chip_at


def greet_neighbours(n):
    me = lax.axis_index('model')
    barrier = pltpu.get_barrier_semaphore()
    core = lax.rem(me, 2)
    pl.semaphore_signal(barrier, inc=1, device_id={'model': me + 1 - 2 * core}, device_id_type=MESH)

    def hello(q, _):
        _, core, sign, a, b, chip_at = ring_place(n, q)
        pl.semaphore_signal(barrier, inc=1, device_id={'model': chip_at(a + sign, b) * 2 + core}, device_id_type=MESH)
        return 0

    lax.fori_loop(0, 4, hello, 0)
    pl.semaphore_wait(barrier, 5)


def reduce_kernel(n, r_dim, l_ref, r_ref, out_ref, l_peer, r_peer, part, first, slot1, slot2, s_send, s_recv, p_send, p_recv, x_send, x_recv):
    me = lax.axis_index('model')
    my_core = lax.rem(me, 2)
    side, _, _, tb, k = l_ref.shape
    width = out_ref.shape[1] // 4
    greet_neighbours(n)
    peer = {'model': me + 1 - 2 * my_core}
    swap = [
        pltpu.make_async_remote_copy(src, dst, x_send.at[i], x_recv.at[i], device_id=peer, device_id_type=MESH)
        for i, (src, dst) in enumerate([(r_ref, r_peer), (l_ref.at[:, :, 1 - my_core], l_peer)])
    ]
    for copy in swap:
        copy.start()

    def group(s, q):
        _, _, sign, a, _, _ = ring_place(n, q)
        at = lax.rem(a - sign * (1 + s) + 2 * side, side)
        mine, other = (l_ref[:, at, my_core], l_peer[:, at]) if q < 2 else (l_ref[at, :, my_core], l_peer[at])
        cols = pl.ds(q * width, width)
        r_mine, r_other = (r_ref[:, cols], r_peer[:, cols]) if r_dim == 0 else (r_ref[cols, :], r_peer[cols, :])
        total = mm(mine.reshape(side * tb, k), r_mine, 1, r_dim) + mm(other.reshape(side * tb, k), r_other, 1, r_dim)
        part[lax.rem(s, 2), q] = total.reshape(side, tb, width)

    def own_part(q, s, j):
        _, _, sign, _, b, _ = ring_place(n, q)
        return part[lax.rem(s, 2), q, lax.rem(b - sign * (1 + j) + 2 * side, side)]

    def hop(q, s, j, src):
        _, core, sign, a, b, chip_at = ring_place(n, q)
        at = (q * (side - 1) + s) * side + j
        return pltpu.make_async_remote_copy(
            src, slot1.at[at], s_send.at[at], s_recv.at[at], device_id={'model': chip_at(a + sign, b) * 2 + core}, device_id_type=MESH)

    def turn_hop(q, s, src):
        _, core, sign, a, b, chip_at = ring_place(n, q)
        at = q * (side - 1) + s
        return pltpu.make_async_remote_copy(
            src, slot2.at[at], p_send.at[at], p_recv.at[at], device_id={'model': chip_at(a, b + sign) * 2 + core}, device_id_type=MESH)

    def arrived(q, s, j):
        return (q * (side - 1) + s) * side + j

    for copy in swap:
        copy.wait()

    def start_step(s, _):
        for q in range(4):
            group(s, q)

            @pl.when(s == 0)
            def _():
                def start_round(j, _):
                    at = q * side + j
                    first[at] = own_part(q, 0, j).astype(BF16)
                    hop(q, 0, j, first.at[at]).start()
                    return 0

                lax.fori_loop(0, side, start_round, 0)

        return 0

    lax.fori_loop(0, 2, start_step, 0)

    def middle_round(t, _):
        s, rest = 1 + t // (4 * side), lax.rem(t, 4 * side)
        j, q = rest // 4, lax.rem(rest, 4)
        at = arrived(q, s - 1, j)
        hop(q, s - 1, j, slot1.at[at]).wait_recv()
        slot1[at] = (slot1[at].astype(F32) + own_part(q, s, j)).astype(BF16)
        hop(q, s, j, slot1.at[at]).start()
        for ahead in range(4):
            @pl.when((q == 3) & (j == ahead))
            def _():
                group(s + 1, ahead)

        return 0

    lax.fori_loop(0, 4 * side * (side - 2), middle_round, 0)

    def last_sum(q, j):
        at = arrived(q, side - 2, j)
        hop(q, side - 2, j, slot1.at[at]).wait_recv()
        return at, slot1[at].astype(F32) + own_part(q, side - 1, j)

    def turn_first(q, _):
        at, total = last_sum(q, 0)
        slot1[at] = total.astype(BF16)
        turn_hop(q, 0, slot1.at[at]).start()
        return 0

    lax.fori_loop(0, 4, turn_first, 0)

    def turn_round(t, _):
        s, q = 1 + t // 4, lax.rem(t, 4)
        _, total = last_sum(q, s)
        at = q * (side - 1) + s - 1
        turn_hop(q, s - 1, slot2.at[at]).wait_recv()
        slot2[at] = (slot2[at].astype(F32) + total).astype(BF16)
        turn_hop(q, s, slot2.at[at]).start()
        return 0

    lax.fori_loop(0, 4 * (side - 2), turn_round, 0)

    def turn_last(q, _):
        _, total = last_sum(q, side - 1)
        at = q * (side - 1) + side - 2
        turn_hop(q, side - 2, slot2.at[at]).wait_recv()
        out_ref[:, pl.ds(pl.multiple_of(q * width, width), width)] = (slot2[at].astype(F32) + total).astype(BF16)
        return 0

    lax.fori_loop(0, 4, turn_last, 0)

    def drain(t, _):
        q, s = t // (side - 1), lax.rem(t, side - 1)
        turn_hop(q, s, slot2.at[t]).wait_send()
        for j in range(side):
            hop(q, s, j, slot1.at[t * side + j]).wait_send()
        return 0

    lax.fori_loop(0, 4 * (side - 1), drain, 0)


def matmul_reduce_scatter(n, left, right, r_dim, collective_id):
    t, k = left.shape
    f = right.shape[1 - r_dim]
    chips = n // 2
    side = math.isqrt(chips)
    tb = t // n
    hops = 4 * (side - 1)
    vmem = pl.BlockSpec(memory_space=pltpu.VMEM)
    return pl.pallas_call(
        functools.partial(reduce_kernel, n, r_dim),
        out_shape=jax.ShapeDtypeStruct((tb, f), BF16),
        in_specs=[vmem, vmem],
        out_specs=vmem,
        scratch_shapes=[
            pltpu.VMEM((side, side, tb, k), BF16),
            pltpu.VMEM(right.shape, BF16),
            pltpu.VMEM((2, 4, side, tb, f // 4), F32),
            pltpu.VMEM((4 * side, tb, f // 4), BF16),
            pltpu.VMEM((hops * side, tb, f // 4), BF16),
            pltpu.VMEM((hops, tb, f // 4), BF16),
            pltpu.SemaphoreType.DMA((hops * side,)), pltpu.SemaphoreType.DMA((hops * side,)),
            pltpu.SemaphoreType.DMA((hops,)), pltpu.SemaphoreType.DMA((hops,)),
            pltpu.SemaphoreType.DMA((2,)), pltpu.SemaphoreType.DMA((2,)),
        ],
        compiler_params=pltpu.CompilerParams(collective_id=collective_id, has_side_effects=True, vmem_limit_bytes=48 * 1024 * 1024),
        cost_estimate=pl.CostEstimate(flops=40_000_000_000, bytes_accessed=4 * t * k, transcendentals=0),
    )(left.reshape(side, side, 2, tb, k), right)


def gelu_parts(up):
    c = math.sqrt(2.0 / math.pi)
    sq = up * up
    th = jnp.tanh(c * (up + 0.044715 * (sq * up)))
    cdf = 0.5 + 0.5 * th
    slope = cdf + up * (0.5 * (1.0 - th * th)) * (c + (3 * 0.044715 * c) * sq)
    return up * cdf, slope


def gather_mlp_kernel(n, own_ref, up_ref, down_ref, dy_ref, b1_ref, gelu_ref, d_up_ref,
                      b1, acc, dg, dy_buf, a_send, a_recv, b_send, b_recv, x_send, x_recv, dy_sem, out_sem):
    me = lax.axis_index('model')
    my_core = lax.rem(me, 2)
    tb, h = own_ref.shape
    f = up_ref.shape[1]
    width = h // 4
    side = math.isqrt(n // 2)
    rounds = side * side
    n_dy, _, _ = dy_ref.shape
    peer = {'model': me + 1 - 2 * my_core}

    def dy_copy(t):
        return pltpu.make_async_copy(dy_ref.at[t], dy_buf.at[lax.rem(t, 2)], dy_sem.at[lax.rem(t, 2)])

    dy_copy(jnp.int32(0)).start()
    dy_copy(jnp.int32(1)).start()
    greet_neighbours(n)

    def cols_of(q):
        return pl.ds(pl.multiple_of(q * width, width), width)

    def quarter(q, r, core):
        _, _, sign, a, b, chip_at = ring_place(n, q)
        chip = chip_at(a - sign * lax.rem(r, side), b - sign * (r // side))
        return b1.at[chip // side, lax.rem(chip, side), core, :, cols_of(q)]

    def along_a(q, j, src):
        _, core, sign, a, b, chip_at = ring_place(n, q)
        at = q * (side - 1) + j
        return pltpu.make_async_remote_copy(
            src, quarter(q, j, core), a_send.at[at], a_recv.at[at], device_id={'model': chip_at(a + sign, b) * 2 + core}, device_id_type=MESH)

    def along_b(q, r, src):
        _, core, sign, a, b, chip_at = ring_place(n, q)
        at = q * (rounds - side) + r
        return pltpu.make_async_remote_copy(
            src, quarter(q, r, core), b_send.at[at], b_recv.at[at], device_id={'model': chip_at(a, b + sign) * 2 + core}, device_id_type=MESH)

    def across(q, r, src, core):
        at = q * rounds + r
        return pltpu.make_async_remote_copy(
            src, quarter(q, r, core), x_send.at[at], x_recv.at[at], device_id=peer, device_id_type=MESH)

    def back_proj(t):
        dy_copy(t).wait()
        dg[t] = mm(dy_buf[lax.rem(t, 2)], down_ref[...], 1, 1).astype(BF16)

        @pl.when(t + 2 < n_dy)
        def _():
            dy_copy(t + 2).start()

    def own_round(q, _):
        src = own_ref.at[:, cols_of(q)]
        along_a(q, 0, src).start()
        along_b(q, 0, src).start()
        across(q, 0, src, my_core).start()
        return 0

    lax.fori_loop(0, 4, own_round, 0)
    b1[me // (2 * side), lax.rem(me // 2, side), my_core] = own_ref[...]
    acc[...] = jnp.zeros_like(acc)

    def add_up(s, q, core):
        _, _, sign, _, b, _ = ring_place(n, q)
        at = lax.rem(b - sign * s + 2 * side, side)
        cols = pl.ds(q * width, width)
        if q < 2:
            pltpu.make_async_copy(b1.at[at, :, core, :, cols], b1_ref.at[at, :, core, :, cols], out_sem).start()
            value = b1[at, :, core, :, cols].reshape(side * tb, width)
        else:
            pltpu.make_async_copy(b1.at[:, at, core, :, cols], b1_ref.at[:, at, core, :, cols], out_sem).start()
            value = b1[:, at, core, :, cols].reshape(side * tb, width)
        more = mm(value, up_ref[cols, :], 1, 0).reshape(side, tb, f)
        if q < 2:
            acc[at, :, core] += more
        else:
            acc[:, at, core] += more

    def take_step(s, q):
        add_up(s, q, my_core)
        for j in range(side):
            r = s * side + j
            across(q, r, quarter(q, r, 1 - my_core), 1 - my_core).wait_recv()
        add_up(s, q, 1 - my_core)

    def main_round(t, _):
        r, q = t // 4, lax.rem(t, 4)
        s, j = r // side, lax.rem(r, side)
        src = quarter(q, r, my_core)

        @pl.when(s == 0)
        def _():
            along_a(q, j - 1, src).wait_recv()

            @pl.when(j < side - 1)
            def _():
                along_a(q, j, src).start()

        @pl.when(s > 0)
        def _():
            along_b(q, r - side, src).wait_recv()

        @pl.when(s < side - 1)
        def _():
            along_b(q, r, src).start()

        across(q, r, src, my_core).start()
        for late in range(4):
            @pl.when((q == 3) & (j == late) & (s > 0))
            def _():
                take_step(s - 1, late)

        @pl.when((q == 1) & (lax.rem(r, 2) == 1))
        def _():
            back_proj(r // 2)

        return 0

    lax.fori_loop(4, 4 * rounds, main_round, 0)
    for q in range(4):
        take_step(jnp.int32(side - 1), q)

    def activate(t, _):
        chip, core = t // 2, lax.rem(t, 2)
        piece, rows = t // 4, pl.ds(pl.multiple_of(lax.rem(t, 4) * tb, tb), tb)
        up = acc[chip // side, lax.rem(chip, side), core].astype(BF16).astype(F32)
        value, slope = gelu_parts(up)
        gelu_ref[piece, rows, :] = value.astype(BF16)
        d_up_ref[piece, rows, :] = (dg[piece, rows, :].astype(F32) * slope).astype(BF16)
        return 0

    lax.fori_loop(0, n, activate, 0)

    def drain(t, _):
        q, r = t // rounds, lax.rem(t, rounds)
        src = quarter(q, r, my_core)
        across(q, r, src, my_core).wait_send()

        @pl.when(r < rounds - side)
        def _():
            along_b(q, r, src).wait_send()

        @pl.when(r < side - 1)
        def _():
            along_a(q, r, src).wait_send()

        return 0

    lax.fori_loop(0, 4 * rounds, drain, 0)
    pltpu.make_async_copy(b1, b1_ref, out_sem).wait()


def gather_mlp(n, own, w_up, w_down, dy, collective_id):
    tb, h = own.shape
    f = w_up.shape[1]
    side = math.isqrt(n // 2)
    rounds = side * side
    vmem = pl.BlockSpec(memory_space=pltpu.VMEM)
    anyspace = pl.BlockSpec(memory_space=pl.ANY)
    a_hops, b_hops, x_hops = 4 * (side - 1), 4 * (rounds - side), 4 * rounds
    sems = [pltpu.SemaphoreType.DMA((k,)) for k in (a_hops, a_hops, b_hops, b_hops, x_hops, x_hops, 2)]
    return pl.pallas_call(
        functools.partial(gather_mlp_kernel, n),
        out_shape=[
            jax.ShapeDtypeStruct((side, side, 2, tb, h), BF16), jax.ShapeDtypeStruct((n // 4, 4 * tb, f), BF16), jax.ShapeDtypeStruct((n // 4, 4 * tb, f), BF16),
        ],
        in_specs=[vmem, vmem, vmem, anyspace],
        out_specs=[anyspace, vmem, vmem],
        scratch_shapes=[
            pltpu.VMEM((side, side, 2, tb, h), BF16), pltpu.VMEM((side, side, 2, tb, f), F32),
            pltpu.VMEM((n // 4, 4 * tb, f), BF16), pltpu.VMEM((2, 4 * tb, h), BF16),
            *sems, pltpu.SemaphoreType.DMA,
        ],
        compiler_params=pltpu.CompilerParams(collective_id=collective_id, has_side_effects=True, vmem_limit_bytes=50 * 1024 * 1024),
        cost_estimate=pl.CostEstimate(flops=40_000_000_000, bytes_accessed=4 * n * tb * h, transcendentals=0),
        name='gather_mlp',
    )(own, w_up, w_down, dy.reshape(n // 4, 4 * tb, h))


def copy_kernel(src_ref, dst_ref):
    dst_ref[...] = src_ref[...].reshape(dst_ref.shape)


def copy_half(pair, half):
    n, _, tb, h = pair.shape
    per = min(4, n)
    return pl.pallas_call(
        copy_kernel, grid=(n // per,),
        in_specs=[pl.BlockSpec((per, 1, tb, h), lambda i: (i, half, 0, 0))], out_specs=pl.BlockSpec((per * tb, h), lambda i: (i, 0)),
        out_shape=jax.ShapeDtypeStruct((n * tb, h), pair.dtype),
        cost_estimate=pl.CostEstimate(flops=10_000_000, bytes_accessed=4 * n * tb * h, transcendentals=0),
    )(pair)


def out_grad_kernel(ot_ref, src_ref, out_ref, acc):
    i = pl.program_id(0)

    @pl.when(i == 0)
    def _():
        acc[...] = jnp.zeros_like(acc)

    h = src_ref.shape[-1]
    acc[...] += mm(ot_ref[...], src_ref[...].reshape(-1, h), 1, 0)

    @pl.when(i == pl.num_programs(0) - 1)
    def _():
        out_ref[...] = acc[...].astype(BF16)


def out_grad(ot, pair, half):
    n, _, tb, h = pair.shape
    hd = ot.shape[0]
    per = min(4, n)
    return pl.pallas_call(
        out_grad_kernel, grid=(n // per,),
        in_specs=[pl.BlockSpec((hd, per * tb), lambda i: (0, i)), pl.BlockSpec((per, 1, tb, h), lambda i: (i, half, 0, 0))],
        out_specs=pl.BlockSpec((hd, h), lambda i: (0, 0)),
        out_shape=jax.ShapeDtypeStruct((hd, h), BF16),
        scratch_shapes=[pltpu.VMEM((hd, h), F32)],
        cost_estimate=pl.CostEstimate(flops=2 * n * tb * h * hd, bytes_accessed=2 * n * tb * h, transcendentals=0), name='out_grad',
    )(ot, pair)


def sum_kernel(n, in_ref, out_ref, land, mine, s_send, s_recv, b_send, b_recv):
    me = lax.axis_index('model')
    barrier = pltpu.get_barrier_semaphore()

    def hello(off, _):
        pl.semaphore_signal(barrier, inc=1, device_id={'model': lax.rem(me + off, n)}, device_id_type=MESH)
        return 0

    lax.fori_loop(1, n, hello, 0)
    land[me] = in_ref[me]
    pl.semaphore_wait(barrier, n - 1)

    def scatter(off, slot):
        to = lax.rem(me + off, n)
        return pltpu.make_async_remote_copy(
            in_ref.at[to], land.at[slot], s_send.at[off], s_recv.at[off], device_id={'model': to}, device_id_type=MESH)

    def spread(off, slot):
        return pltpu.make_async_remote_copy(
            mine, out_ref.at[slot], b_send.at[off], b_recv.at[off], device_id={'model': lax.rem(me + off, n)}, device_id_type=MESH)

    def each(body):
        def step(off, _):
            body(off, lax.rem(me - off + n, n))
            return 0

        lax.fori_loop(1, n, step, 0)

    each(lambda off, come: scatter(off, me).start())
    each(lambda off, come: scatter(off, come).wait())
    mine[...] = jnp.sum(land[...], axis=0)
    each(lambda off, come: spread(off, me).start())
    out_ref[me] = mine[...]
    each(lambda off, come: spread(off, come).wait())


def sum_over_devices(n, value, collective_id):
    piece = (1, value.size // n)
    vmem = pl.BlockSpec(memory_space=pltpu.VMEM)
    return pl.pallas_call(
        functools.partial(sum_kernel, n),
        out_shape=jax.ShapeDtypeStruct((n, *piece), F32),
        in_specs=[vmem], out_specs=vmem,
        scratch_shapes=[pltpu.VMEM((n, *piece), F32), pltpu.VMEM(piece, F32)] + [pltpu.SemaphoreType.DMA((n,))] * 4,
        compiler_params=pltpu.CompilerParams(collective_id=collective_id, has_side_effects=True),
        cost_estimate=pl.CostEstimate(flops=1_000_000_000, bytes_accessed=value.size * 8, transcendentals=0),
        name='gain_sums',
    )(value.reshape(n, *piece)).reshape(value.shape)


def ln_rows(z, gain):
    wide = z.astype(F32)
    mean = jnp.mean(wide, axis=-1, keepdims=True)
    cen = wide - mean
    rstd = lax.rsqrt(jnp.mean(cen * cen, axis=-1, keepdims=True) + LN_EPS)
    hat = cen * rstd
    return (hat * gain.astype(F32)).astype(BF16), hat, rstd


def ln_back(d_out, hat, rstd, gain):
    d_wide = d_out.astype(F32)
    d_hat = d_wide * gain.astype(F32)
    mean_a = jnp.mean(d_hat, axis=-1, keepdims=True)
    mean_b = jnp.mean(d_hat * hat, axis=-1, keepdims=True)
    return (rstd * (d_hat - mean_a - hat * mean_b)).astype(BF16), jnp.sum(d_wide * hat, axis=0)


def solution(mesh):
    n = mesh.shape['model']

    def layer(x_in, seg_ids, gain_one, w_qkv, w_out, gain_two, w_up, w_down, d_y):
        x = x_in[0]
        dy = d_y[0]
        seg = seg_ids[0]
        t, h = x.shape
        n_local, hd = w_out.shape[:2]
        inner = n * n_local * hd
        ts = t // n
        bq = min(512, t)
        bk = min(512, t)
        me = lax.axis_index('model')

        wo_full = lax.all_gather(w_out, 'model', axis=0, tiled=True).reshape(inner, h)

        start = document_starts(seg)
        tab = block_table(seg, start, bq, bk)
        start_row = start.reshape(1, t)

        a_full, q, k, v, qkvt = ln_qkv(x, gain_one, w_qkv.T)
        ot, lse = attention_forward(k, qkvt, start_row, tab, bq, bk)
        o_mine = exchange(n, ot, (n, hd, ts), column_block(ts), leading, 0)

        x_s = lax.dynamic_slice(x, (me * ts, 0), (ts, h))
        dy_s = lax.dynamic_slice(dy, (me * ts, 0), (ts, h))
        proj = mm(o_mine.reshape(inner, ts), wo_full, 0, 0)
        resid = (x_s.astype(F32) + proj).astype(BF16)
        b1_s, hat_two, rstd_two = ln_rows(resid, gain_two)
        b1, gelu_out, d_up = (z.reshape(t, z.shape[-1]) for z in gather_mlp(n, b1_s, w_up, w_down, dy, 6))
        d_b1 = matmul_reduce_scatter(n, d_up, w_up, 1, 3)
        late_gelu, d_b1 = lax.optimization_barrier((gelu_out, d_b1))
        d_ln, d_gain_two = ln_back(d_b1, hat_two, rstd_two, gain_two)
        d_resid_s = dy_s + d_ln
        part_two = matmul_reduce_scatter(n, late_gelu, w_down, 0, 4)
        late_gelu, late_up, part_two = lax.optimization_barrier((late_gelu, d_up, part_two))
        d_w_down = mm(late_gelu, dy, 0, 0).astype(BF16)
        d_w_up = mm(b1, late_up, 0, 0).astype(BF16)

        y_s = (resid.astype(F32) + part_two.astype(F32)).astype(BF16)
        pair = lax.all_gather(jnp.stack([y_s, d_resid_s]), 'model', axis=0, tiled=True).reshape(n, 2, ts, h)
        y_out = copy_half(pair, 0)[None]
        d_heads = mm(wo_full, d_resid_s, 1, 1).astype(BF16).reshape(n, hd, ts)
        dot = exchange(n, d_heads, (hd, t), leading, column_block(ts), 1)

        d_qkv = attention_backward(q, k, v, qkvt, ot, dot, lse, start_row, tab, bq, bk)
        d_norm = matmul_reduce_scatter(n, d_qkv, w_qkv.T, 0, 5)
        d_w_qkv = mm(a_full, d_qkv, 0, 0).astype(BF16)
        d_w_out = out_grad(ot, pair, 1)

        _, hat_one, rstd_one = ln_rows(x_s, gain_one)
        d_ln, d_gain_one = ln_back(d_norm, hat_one, rstd_one, gain_one)
        d_x = lax.all_gather((d_resid_s + d_ln)[None], 'model', axis=1, tiled=True)
        gains = sum_over_devices(n, jnp.concatenate([d_gain_one, d_gain_two]), 2).astype(BF16)
        return (y_out, d_x, d_w_qkv, d_w_out.reshape(n_local, hd, h), d_w_up, d_w_down, gains[:h], gains[h:])

    in_specs = (P('data'), P('data'), P(), P(None, 'model'), P('model'), P(), P(None, 'model'), P('model'), P('data'))
    out_specs = (P('data'), P('data'), P('data', 'model'), P(('data', 'model')), P('data', 'model'), P(('data', 'model')), P('data'), P('data'))
    return jax.shard_map(layer, mesh=mesh, in_specs=in_specs, out_specs=out_specs, check_vma=False)
```

```python
import functools
import math

import jax
import jax.numpy as jnp
from jax import lax
from jax.experimental import pallas as pl
from jax.experimental.pallas import tpu as pltpu
from jax.sharding import PartitionSpec as P


LN_EPS = 1e-5
LOG2E = 1.4426950408889634
NEG = -1e30
MESH = pl.DeviceIdType.MESH
VMEM_LIMIT = 60 * 1024 * 1024
F32 = jnp.float32
BF16 = jnp.bfloat16


def mm(a, b, ca, cb):
    return lax.dot_general(a, b, (((ca,), (cb,)), ((), ())), preferred_element_type=F32)


def cost(flops, moved):
    return pl.CostEstimate(flops=flops, bytes_accessed=moved, transcendentals=0)


def zero_map(*_):
    return (0, 0)


def ln_qkv_kernel(x_ref, g_ref, w_ref, a_ref, q_ref, k_ref, v_ref, t_ref):
    x = x_ref[...].astype(F32)
    mean = jnp.mean(x, axis=-1, keepdims=True)
    cen = x - mean
    var = jnp.mean(cen * cen, axis=-1, keepdims=True)
    a = (cen * lax.rsqrt(var + LN_EPS) * g_ref[...].astype(F32)).astype(BF16)
    a_ref[...] = a
    qkv = mm(a, w_ref[...], 1, 1)
    t_ref[...] = qkv.T.astype(BF16)
    hd = q_ref.shape[1]
    qkv = qkv.astype(BF16)
    q_ref[...] = qkv[:, :hd]
    k_ref[...] = qkv[:, hd:2 * hd]
    v_ref[...] = qkv[:, 2 * hd:]


def ln_qkv(x, g, w):
    t, h = x.shape
    c = w.shape[0]
    hd = c // 3
    bt = min(512, t)
    row = lambda n: pl.BlockSpec((bt, n), lambda i: (i, 0))
    return pl.pallas_call(
        ln_qkv_kernel,
        grid=(t // bt,),
        in_specs=[row(h), pl.BlockSpec((1, h), zero_map), pl.BlockSpec((c, h), zero_map)],
        out_specs=[row(h), row(hd), row(hd), row(hd), pl.BlockSpec((c, bt), lambda i: (0, i))],
        out_shape=[jax.ShapeDtypeStruct((t, h), BF16)] + [jax.ShapeDtypeStruct((t, hd), BF16)] * 3 + [jax.ShapeDtypeStruct((c, t), BF16)],
        compiler_params=pltpu.CompilerParams(vmem_limit_bytes=VMEM_LIMIT),
        cost_estimate=cost(2 * t * h * c + 20 * t * h, 4 * t * h),
        name='ln_qkv',
    )(x, g.reshape(1, h), w)


def visible(kb, bk, q0, bq, start):
    k_pos = kb * bk + lax.broadcasted_iota(jnp.int32, (bk, bq), 0)
    q_pos = q0 + lax.broadcasted_iota(jnp.int32, (bk, bq), 1)
    return (k_pos <= q_pos) & (k_pos >= start)


def masked_block(t, lo, mid, hi):
    return jnp.where(t < mid - lo, lo + t, hi + t - (mid - lo))


def attn_fwd_kernel(bk, tab_ref, k_ref, qt_ref, vt_ref, start_ref, ot_ref, lse_ref):
    i = pl.program_id(0)
    bq = qt_ref.shape[1]
    hd = qt_ref.shape[0]
    scale = LOG2E * hd ** -0.5
    qt = qt_ref[...]
    start = start_ref[...]
    lo, mid, hi, top = tab_ref[0, i], tab_ref[1, i], tab_ref[2, i], tab_ref[3, i]

    def step(masked, kb, carry):
        m, l, acc = carry
        k0 = pl.multiple_of(kb * bk, bk)
        s = mm(k_ref[pl.ds(k0, bk), :], qt, 1, 0)
        if masked:
            s = jnp.where(visible(kb, bk, i * bq, bq, start), s, NEG)
        m_new = jnp.maximum(m, jnp.max(s, axis=0, keepdims=True))
        p = jnp.exp2((s - m_new) * scale)
        alpha = jnp.exp2((m - m_new) * scale)
        l = l * alpha + jnp.sum(p, axis=0, keepdims=True)
        acc = acc * alpha + mm(vt_ref[:, pl.ds(k0, bk)], p.astype(BF16), 1, 0)
        return m_new, l, acc

    carry = (jnp.full((1, bq), NEG, F32), jnp.zeros((1, bq), F32), jnp.zeros((hd, bq), F32))
    carry = lax.fori_loop(mid, hi, functools.partial(step, False), carry)
    m, l, acc = lax.fori_loop(0, mid - lo + top - hi, lambda t, c: step(True, masked_block(t, lo, mid, hi), c), carry)
    ot_ref[...] = (acc / l).astype(BF16)
    lse_ref[...] = m * scale + jnp.log2(l)


def document_starts(seg):
    t = seg.shape[0]
    wide = 128
    pos = jnp.arange(t, dtype=jnp.int32).reshape(t // wide, wide)
    before = jnp.concatenate([seg[:1], seg[:-1]])
    mark = jnp.where((seg != before).reshape(pos.shape), pos, 0)
    lane = jnp.arange(wide)
    inner = jnp.max(jnp.where(lane[None, :, None] >= lane[None, None, :], mark[:, None, :], 0), axis=-1)
    row = jnp.arange(t // wide)
    prior = jnp.max(jnp.where(row[:, None] > row[None, :], inner[:, -1][None, :], 0), axis=-1)
    return jnp.maximum(inner, prior[:, None]).reshape(t)


def block_table(seg, start, bq, bk):
    t = seg.shape[0]
    nq = t // bq
    q0 = jnp.arange(nq, dtype=jnp.int32) * bq
    first = start.reshape(nq, bq)[:, 0]
    last = start.reshape(nq, bq)[:, -1]
    lo = first // bk
    hi = q0 // bk
    top = (q0 + bq + bk - 1) // bk
    mid = jnp.clip((last + bk - 1) // bk, lo, hi)
    return jnp.stack([lo, mid, hi, top])


def attention_forward(k, qkvt, start, tab, bq, bk):
    t, hd = k.shape
    return pl.pallas_call(
        functools.partial(attn_fwd_kernel, bk),
        grid_spec=pltpu.PrefetchScalarGridSpec(
            num_scalar_prefetch=1,
            grid=(t // bq,),
            in_specs=[
                pl.BlockSpec((t, hd), zero_map),
                pl.BlockSpec((hd, bq), lambda i, *_: (0, i)),
                pl.BlockSpec((hd, t), lambda i, *_: (2, 0)),
                pl.BlockSpec((1, bq), lambda i, *_: (0, i)),
            ],
            out_specs=[pl.BlockSpec((hd, bq), lambda i, *_: (0, i)), pl.BlockSpec((1, bq), lambda i, *_: (0, i))],
        ),
        out_shape=[jax.ShapeDtypeStruct((hd, t), BF16), jax.ShapeDtypeStruct((1, t), F32)],
        compiler_params=pltpu.CompilerParams(vmem_limit_bytes=VMEM_LIMIT),
        cost_estimate=cost(16 * t * t * hd, 8 * t * hd),
        name='attn_fwd',
    )(tab, k, qkvt, qkvt, start)


def attn_bwd_kernel(bk, tab_ref, q_ref, k_ref, v_ref, t_ref, ot_ref, dot_ref, lse_ref, start_ref, d_ref, dk_acc, dv_acc):
    i = pl.program_id(0)
    bq, hd = q_ref.shape
    scale = LOG2E * hd ** -0.5
    t = k_ref.shape[0]

    @pl.when(i == 0)
    def _():
        dk_acc[...] = jnp.zeros_like(dk_acc)
        dv_acc[...] = jnp.zeros_like(dv_acc)

    c0 = pl.multiple_of(i * bq, bq)
    q = q_ref[...]
    qt = t_ref[:hd, pl.ds(c0, bq)]
    dot_blk = dot_ref[...]
    dot_wide = dot_blk.astype(F32)
    d_out = dot_wide.T.astype(BF16)
    delta = jnp.sum(dot_wide * ot_ref[...].astype(F32), axis=0, keepdims=True)
    lse = lse_ref[...]
    start = start_ref[...]
    lo, mid, hi, top = tab_ref[0, i], tab_ref[1, i], tab_ref[2, i], tab_ref[3, i]

    def step(masked, kb, dqt):
        k0 = pl.multiple_of(kb * bk, bk)
        rows = pl.ds(k0, bk)
        s = mm(k_ref[rows, :], qt, 1, 0)
        p = jnp.exp2(s * scale - lse)
        if masked:
            p = jnp.where(visible(kb, bk, i * bq, bq, start), p, 0.0)
        dp = mm(v_ref[rows, :], dot_blk, 1, 0)
        ds = (p * (dp - delta)).astype(BF16)
        dv_acc[rows, :] += mm(p.astype(BF16), d_out, 1, 0)
        dk_acc[rows, :] += mm(ds, q, 1, 0)
        return dqt + mm(t_ref[hd:2 * hd, rows], ds, 1, 0)

    dqt = jnp.zeros((hd, bq), F32)
    dqt = lax.fori_loop(mid, hi, functools.partial(step, False), dqt)
    dqt = lax.fori_loop(0, mid - lo + top - hi, lambda t, c: step(True, masked_block(t, lo, mid, hi), c), dqt)
    d_ref[pl.ds(c0, bq), :hd] = (dqt * hd ** -0.5).T.astype(BF16)

    @pl.when(i == pl.num_programs(0) - 1)
    def _():
        def put(r, _):
            rows = pl.ds(pl.multiple_of(r * bk, bk), bk)
            d_ref[rows, hd:2 * hd] = (dk_acc[rows, :] * hd ** -0.5).astype(BF16)
            d_ref[rows, 2 * hd:] = dv_acc[rows, :].astype(BF16)
            return 0

        lax.fori_loop(0, t // bk, put, 0)


def attention_backward(q, k, v, qkvt, ot, dot, lse, start, tab, bq, bk):
    t, hd = k.shape
    whole = lambda shape: pl.BlockSpec(shape, zero_map)
    cols = lambda n: pl.BlockSpec((n, bq), lambda i, *_: (0, i))
    return pl.pallas_call(
        functools.partial(attn_bwd_kernel, bk),
        grid_spec=pltpu.PrefetchScalarGridSpec(
            num_scalar_prefetch=1,
            grid=(t // bq,),
            in_specs=[
                pl.BlockSpec((bq, hd), lambda i, *_: (i, 0)), whole((t, hd)), whole((t, hd)), whole((3 * hd, t)),
                cols(hd), cols(hd), cols(1), cols(1),
            ],
            out_specs=whole((t, 3 * hd)),
            scratch_shapes=[pltpu.VMEM((t, hd), F32), pltpu.VMEM((t, hd), F32)],
        ),
        out_shape=jax.ShapeDtypeStruct((t, 3 * hd), BF16),
        compiler_params=pltpu.CompilerParams(vmem_limit_bytes=VMEM_LIMIT),
        cost_estimate=cost(40 * t * t * hd, 16 * t * hd),
        name='attn_bwd',
    )(tab, q, k, v, qkvt, ot, dot, lse, start)


def exchange_kernel(n, src_of, dst_of, in_ref, out_ref, send_sem, recv_sem, own_sem):
    me = lax.axis_index('model')
    barrier = pltpu.get_barrier_semaphore()

    def hello(off, _):
        pl.semaphore_signal(barrier, inc=1, device_id={'model': lax.rem(me + off, n)}, device_id_type=MESH)
        return 0

    lax.fori_loop(1, n, hello, 0)
    own = pltpu.make_async_copy(src_of(in_ref, me), dst_of(out_ref, me), own_sem)
    own.start()
    pl.semaphore_wait(barrier, n - 1)

    def send(off, _):
        to = lax.rem(me + off, n)
        pltpu.make_async_remote_copy(
            src_ref=src_of(in_ref, to), dst_ref=dst_of(out_ref, me), send_sem=send_sem.at[off], recv_sem=recv_sem.at[off],
            device_id={'model': to}, device_id_type=MESH,
        ).start()
        return 0

    lax.fori_loop(1, n, send, 0)

    def finish(off, _):
        to = lax.rem(me + off, n)
        come = lax.rem(me - off + n, n)
        pltpu.make_async_remote_copy(
            src_ref=src_of(in_ref, to), dst_ref=dst_of(out_ref, come), send_sem=send_sem.at[off], recv_sem=recv_sem.at[off],
            device_id={'model': to}, device_id_type=MESH,
        ).wait()
        return 0

    lax.fori_loop(1, n, finish, 0)
    own.wait()


def exchange(n, value, out_shape, src_of, dst_of, collective_id):
    return pl.pallas_call(
        functools.partial(exchange_kernel, n, src_of, dst_of),
        out_shape=jax.ShapeDtypeStruct(out_shape, value.dtype),
        in_specs=[pl.BlockSpec(memory_space=pltpu.VMEM)],
        out_specs=pl.BlockSpec(memory_space=pltpu.VMEM),
        scratch_shapes=[pltpu.SemaphoreType.DMA((n,)), pltpu.SemaphoreType.DMA((n,)), pltpu.SemaphoreType.DMA],
        compiler_params=pltpu.CompilerParams(collective_id=collective_id, has_side_effects=True),
        cost_estimate=cost(2_000_000_000, 2 * value.size * 2),
    )(value)


def column_block(width):
    return lambda ref, j: ref.at[:, pl.ds(pl.multiple_of(j * width, width), width)]


def leading(ref, j):
    return ref.at[j]


def ring_place(n, q):
    me = lax.axis_index('model')
    side = math.isqrt(n // 2)
    core = lax.rem(me, 2)
    chip = me // 2
    x = lax.rem(chip, side)
    y = chip // side
    turn = q // 2
    sign = 1 - 2 * lax.rem(q, 2)
    a = x * (1 - turn) + y * turn
    b = y * (1 - turn) + x * turn

    def chip_at(pa, pb):
        pa = lax.rem(pa + 2 * side, side)
        pb = lax.rem(pb + 2 * side, side)
        return (pb * (1 - turn) + pa * turn) * side + pa * (1 - turn) + pb * turn

    return side, core, sign, a, b, chip_at


def greet_neighbours(n):
    me = lax.axis_index('model')
    barrier = pltpu.get_barrier_semaphore()
    core = lax.rem(me, 2)
    pl.semaphore_signal(barrier, inc=1, device_id={'model': me + 1 - 2 * core}, device_id_type=MESH)

    def hello(q, _):
        _, core, sign, a, b, chip_at = ring_place(n, q)
        pl.semaphore_signal(barrier, inc=1, device_id={'model': chip_at(a + sign, b) * 2 + core}, device_id_type=MESH)
        return 0

    lax.fori_loop(0, 4, hello, 0)
    pl.semaphore_wait(barrier, 5)


class Reduction:
    def __init__(self, n, r_dim, l_ref, r_ref, out_ref, scratch):
        self.n, self.r_dim, self.l_ref, self.r_ref, self.out_ref = n, r_dim, l_ref, r_ref, out_ref
        (self.l_peer, self.r_peer, self.part, self.first, self.slot1, self.slot2,
         self.s_send, self.s_recv, self.p_send, self.p_recv, self.x_send, self.x_recv) = scratch
        self.side, _, _, self.tb, self.k = l_ref.shape
        self.width = out_ref.shape[1] // 4
        me = lax.axis_index('model')
        self.my_core = lax.rem(me, 2)
        peer = {'model': me + 1 - 2 * self.my_core}
        pairs = [(r_ref, self.r_peer), (l_ref.at[:, :, 1 - self.my_core], self.l_peer)]
        self.swap = [
            pltpu.make_async_remote_copy(src, dst, self.x_send.at[i], self.x_recv.at[i], device_id=peer, device_id_type=MESH)
            for i, (src, dst) in enumerate(pairs)
        ]

    def wrap(self, pos):
        return lax.rem(pos + 2 * self.side, self.side)

    def group(self, s, q):
        _, _, sign, a, _, _ = ring_place(self.n, q)
        at = self.wrap(a - sign * (1 + s))
        l_ref, l_peer, core = self.l_ref, self.l_peer, self.my_core
        mine, other = (l_ref[:, at, core], l_peer[:, at]) if q < 2 else (l_ref[at, :, core], l_peer[at])
        cols = pl.ds(q * self.width, self.width)
        at_r = (slice(None), cols) if self.r_dim == 0 else (cols, slice(None))
        flat = (self.side * self.tb, self.k)
        total = mm(mine.reshape(flat), self.r_ref[at_r], 1, self.r_dim) + mm(other.reshape(flat), self.r_peer[at_r], 1, self.r_dim)
        self.part[lax.rem(s, 2), q] = total.reshape(self.side, self.tb, self.width)

    def own_part(self, q, s, j):
        _, _, sign, _, b, _ = ring_place(self.n, q)
        return self.part[lax.rem(s, 2), q, self.wrap(b - sign * (1 + j))]

    def hop(self, q, s, j, src):
        _, core, sign, a, b, chip_at = ring_place(self.n, q)
        at = self.arrived(q, s, j)
        return pltpu.make_async_remote_copy(
            src, self.slot1.at[at], self.s_send.at[at], self.s_recv.at[at],
            device_id={'model': chip_at(a + sign, b) * 2 + core}, device_id_type=MESH)

    def turn_hop(self, q, s, src):
        _, core, sign, a, b, chip_at = ring_place(self.n, q)
        at = q * (self.side - 1) + s
        return pltpu.make_async_remote_copy(
            src, self.slot2.at[at], self.p_send.at[at], self.p_recv.at[at],
            device_id={'model': chip_at(a, b + sign) * 2 + core}, device_id_type=MESH)

    def arrived(self, q, s, j):
        return (q * (self.side - 1) + s) * self.side + j

    def start_step(self, s):
        for q in range(4):
            self.group(s, q)

            @pl.when(s == 0)
            def _():
                def start_round(j, _):
                    src = self.first.at[q * self.side + j]
                    src[...] = self.own_part(q, 0, j).astype(BF16)
                    self.hop(q, 0, j, src).start()
                    return 0

                lax.fori_loop(0, self.side, start_round, 0)

    def received(self, q, s, j):
        slot = self.slot1.at[self.arrived(q, s - 1, j)]
        self.hop(q, s - 1, j, slot).wait_recv()
        return slot, slot[...].astype(F32) + self.own_part(q, s, j)

    def middle_round(self, t):
        s, rest = 1 + t // (4 * self.side), lax.rem(t, 4 * self.side)
        j, q = rest // 4, lax.rem(rest, 4)
        slot, total = self.received(q, s, j)
        slot[...] = total.astype(BF16)
        self.hop(q, s, j, slot).start()
        for ahead in range(4):
            @pl.when((q == 3) & (j == ahead))
            def _():
                self.group(s + 1, ahead)

    def turn_first(self, q):
        slot, total = self.received(q, self.side - 1, 0)
        slot[...] = total.astype(BF16)
        self.turn_hop(q, 0, slot).start()

    def turned(self, q, s):
        _, total = self.received(q, self.side - 1, s)
        slot = self.slot2.at[q * (self.side - 1) + s - 1]
        self.turn_hop(q, s - 1, slot).wait_recv()
        return slot, slot[...].astype(F32) + total

    def turn_round(self, t):
        s, q = 1 + t // 4, lax.rem(t, 4)
        slot, total = self.turned(q, s)
        slot[...] = total.astype(BF16)
        self.turn_hop(q, s, slot).start()

    def turn_last(self, q):
        _, total = self.turned(q, self.side - 1)
        self.out_ref[:, pl.ds(pl.multiple_of(q * self.width, self.width), self.width)] = total.astype(BF16)

    def drain(self, t):
        q, s = t // (self.side - 1), lax.rem(t, self.side - 1)
        self.turn_hop(q, s, self.slot2.at[t]).wait_send()
        for j in range(self.side):
            self.hop(q, s, j, self.slot1.at[t * self.side + j]).wait_send()


def reduce_kernel(n, r_dims, *refs):
    m = len(r_dims)
    lefts, rights, outs = refs[:m], refs[m:2 * m], refs[2 * m:3 * m]
    rest = refs[3 * m:]
    each = len(rest) // m
    todo = [
        Reduction(n, r_dims[i], lefts[i], rights[i], outs[i], rest[i * each:(i + 1) * each]) for i in range(m)
    ]
    side = todo[0].side
    greet_neighbours(n)
    for job in todo:
        for copy in job.swap:
            copy.start()
    for job in todo:
        for copy in job.swap:
            copy.wait()
        loop(2, [job.start_step])
    loop(4 * side * (side - 2), [job.middle_round for job in todo])
    loop(4, [job.turn_first for job in todo])
    loop(4 * (side - 2), [job.turn_round for job in todo])
    loop(4, [job.turn_last for job in todo])
    loop(4 * (side - 1), [job.drain for job in todo])


def loop(count, bodies):
    def step(t, _):
        for body in bodies:
            body(t)
        return 0

    lax.fori_loop(0, count, step, 0)


def matmul_reduce_scatter(n, jobs, collective_id):
    chips = n // 2
    side = math.isqrt(chips)
    hops = 4 * (side - 1)
    vmem = pl.BlockSpec(memory_space=pltpu.VMEM)
    lefts, rights, outs, scratch = [], [], [], []
    for left, right, r_dim in jobs:
        t, k = left.shape
        f, tb = right.shape[1 - r_dim], t // n
        lefts.append(left.reshape(side, side, 2, tb, k))
        rights.append(right)
        outs.append(jax.ShapeDtypeStruct((tb, f), BF16))
        piece = (tb, f // 4)
        scratch += [
            pltpu.VMEM((side, side, tb, k), BF16), pltpu.VMEM(right.shape, BF16), pltpu.VMEM((2, 4, side, *piece), F32),
            pltpu.VMEM((4 * side, *piece), BF16), pltpu.VMEM((hops * side, *piece), BF16), pltpu.VMEM((hops, *piece), BF16),
        ] + [pltpu.SemaphoreType.DMA((c,)) for c in (hops * side, hops * side, hops, hops, 2, 2)]
    return pl.pallas_call(
        functools.partial(reduce_kernel, n, [r_dim for _, _, r_dim in jobs]),
        out_shape=outs,
        in_specs=[vmem] * (2 * len(jobs)),
        out_specs=[vmem] * len(jobs),
        scratch_shapes=scratch,
        compiler_params=pltpu.CompilerParams(collective_id=collective_id, has_side_effects=True, vmem_limit_bytes=VMEM_LIMIT),
        cost_estimate=cost(40_000_000_000, 4 * t * k),
    )(*lefts, *rights)


def gelu_parts(up):
    c = math.sqrt(2.0 / math.pi)
    sq = up * up
    th = jnp.tanh(c * (up + 0.044715 * (sq * up)))
    cdf = 0.5 + 0.5 * th
    slope = cdf + up * (0.5 * (1.0 - th * th)) * (c + (3 * 0.044715 * c) * sq)
    return up * cdf, slope


def gather_mlp_kernel(n, own_ref, up_ref, down_ref, dy_ref, b1_ref, gelu_ref, d_up_ref,
                      b1, acc, dg, dy_buf, a_send, a_recv, b_send, b_recv, x_send, x_recv, dy_sem, out_sem):
    me = lax.axis_index('model')
    my_core = lax.rem(me, 2)
    tb, h = own_ref.shape
    f = up_ref.shape[1]
    width = h // 4
    side = math.isqrt(n // 2)
    rounds = side * side
    n_dy, _, _ = dy_ref.shape
    peer = {'model': me + 1 - 2 * my_core}

    def dy_copy(t):
        return pltpu.make_async_copy(dy_ref.at[t], dy_buf.at[lax.rem(t, 2)], dy_sem.at[lax.rem(t, 2)])

    dy_copy(jnp.int32(0)).start()
    dy_copy(jnp.int32(1)).start()
    greet_neighbours(n)

    def cols_of(q):
        return pl.ds(pl.multiple_of(q * width, width), width)

    def quarter(q, r, core):
        _, _, sign, a, b, chip_at = ring_place(n, q)
        chip = chip_at(a - sign * lax.rem(r, side), b - sign * (r // side))
        return b1.at[chip // side, lax.rem(chip, side), core, :, cols_of(q)]

    def along_a(q, j, src):
        _, core, sign, a, b, chip_at = ring_place(n, q)
        at = q * (side - 1) + j
        return pltpu.make_async_remote_copy(
            src, quarter(q, j, core), a_send.at[at], a_recv.at[at], device_id={'model': chip_at(a + sign, b) * 2 + core}, device_id_type=MESH)

    def along_b(q, r, src):
        _, core, sign, a, b, chip_at = ring_place(n, q)
        at = q * (rounds - side) + r
        return pltpu.make_async_remote_copy(
            src, quarter(q, r, core), b_send.at[at], b_recv.at[at], device_id={'model': chip_at(a, b + sign) * 2 + core}, device_id_type=MESH)

    def across(q, r, src, core):
        at = q * rounds + r
        return pltpu.make_async_remote_copy(
            src, quarter(q, r, core), x_send.at[at], x_recv.at[at], device_id=peer, device_id_type=MESH)

    def back_proj(t):
        dy_copy(t).wait()
        dg[t] = mm(dy_buf[lax.rem(t, 2)], down_ref[...], 1, 1).astype(BF16)

        @pl.when(t + 2 < n_dy)
        def _():
            dy_copy(t + 2).start()

    def own_round(q, _):
        src = own_ref.at[:, cols_of(q)]
        along_a(q, 0, src).start()
        along_b(q, 0, src).start()
        across(q, 0, src, my_core).start()
        return 0

    lax.fori_loop(0, 4, own_round, 0)
    b1[me // (2 * side), lax.rem(me // 2, side), my_core] = own_ref[...]
    acc[...] = jnp.zeros_like(acc)

    def add_up(s, q, core):
        _, _, sign, _, b, _ = ring_place(n, q)
        at = lax.rem(b - sign * s + 2 * side, side)
        cols = pl.ds(q * width, width)
        if q < 2:
            pltpu.make_async_copy(b1.at[at, :, core, :, cols], b1_ref.at[at, :, core, :, cols], out_sem).start()
            value = b1[at, :, core, :, cols].reshape(side * tb, width)
        else:
            pltpu.make_async_copy(b1.at[:, at, core, :, cols], b1_ref.at[:, at, core, :, cols], out_sem).start()
            value = b1[:, at, core, :, cols].reshape(side * tb, width)
        more = mm(value, up_ref[cols, :], 1, 0).reshape(side, tb, f)
        if q < 2:
            acc[at, :, core] += more
        else:
            acc[:, at, core] += more

    def take_step(s, q):
        add_up(s, q, my_core)
        for j in range(side):
            r = s * side + j
            across(q, r, quarter(q, r, 1 - my_core), 1 - my_core).wait_recv()
        add_up(s, q, 1 - my_core)

    def main_round(t, _):
        r, q = t // 4, lax.rem(t, 4)
        s, j = r // side, lax.rem(r, side)
        src = quarter(q, r, my_core)

        @pl.when(s == 0)
        def _():
            along_a(q, j - 1, src).wait_recv()

            @pl.when(j < side - 1)
            def _():
                along_a(q, j, src).start()

        @pl.when(s > 0)
        def _():
            along_b(q, r - side, src).wait_recv()

        @pl.when(s < side - 1)
        def _():
            along_b(q, r, src).start()

        across(q, r, src, my_core).start()
        for late in range(4):
            @pl.when((q == 3) & (j == late) & (s > 0))
            def _():
                take_step(s - 1, late)

        @pl.when((q == 1) & (lax.rem(r, 2) == 1))
        def _():
            back_proj(r // 2)

        return 0

    lax.fori_loop(4, 4 * rounds, main_round, 0)
    for q in range(4):
        take_step(jnp.int32(side - 1), q)

    def activate(t, _):
        chip, core = t // 2, lax.rem(t, 2)
        piece, rows = t // 4, pl.ds(pl.multiple_of(lax.rem(t, 4) * tb, tb), tb)
        up = acc[chip // side, lax.rem(chip, side), core].astype(BF16).astype(F32)
        value, slope = gelu_parts(up)
        gelu_ref[piece, rows, :] = value.astype(BF16)
        d_up_ref[piece, rows, :] = (dg[piece, rows, :].astype(F32) * slope).astype(BF16)
        return 0

    lax.fori_loop(0, n, activate, 0)

    def drain(t, _):
        q, r = t // rounds, lax.rem(t, rounds)
        src = quarter(q, r, my_core)
        across(q, r, src, my_core).wait_send()

        @pl.when(r < rounds - side)
        def _():
            along_b(q, r, src).wait_send()

        @pl.when(r < side - 1)
        def _():
            along_a(q, r, src).wait_send()

        return 0

    lax.fori_loop(0, 4 * rounds, drain, 0)
    pltpu.make_async_copy(b1, b1_ref, out_sem).wait()


def gather_mlp(n, own, w_up, w_down, dy, collective_id):
    tb, h = own.shape
    f = w_up.shape[1]
    side = math.isqrt(n // 2)
    rounds = side * side
    vmem = pl.BlockSpec(memory_space=pltpu.VMEM)
    anyspace = pl.BlockSpec(memory_space=pl.ANY)
    a_hops, b_hops, x_hops = 4 * (side - 1), 4 * (rounds - side), 4 * rounds
    sems = [pltpu.SemaphoreType.DMA((k,)) for k in (a_hops, a_hops, b_hops, b_hops, x_hops, x_hops, 2)]
    return pl.pallas_call(
        functools.partial(gather_mlp_kernel, n),
        out_shape=[
            jax.ShapeDtypeStruct((side, side, 2, tb, h), BF16), jax.ShapeDtypeStruct((n // 4, 4 * tb, f), BF16), jax.ShapeDtypeStruct((n // 4, 4 * tb, f), BF16),
        ],
        in_specs=[vmem, vmem, vmem, anyspace],
        out_specs=[anyspace, vmem, vmem],
        scratch_shapes=[
            pltpu.VMEM((side, side, 2, tb, h), BF16), pltpu.VMEM((side, side, 2, tb, f), F32),
            pltpu.VMEM((n // 4, 4 * tb, f), BF16), pltpu.VMEM((2, 4 * tb, h), BF16),
            *sems, pltpu.SemaphoreType.DMA,
        ],
        compiler_params=pltpu.CompilerParams(collective_id=collective_id, has_side_effects=True, vmem_limit_bytes=50 * 1024 * 1024),
        cost_estimate=cost(40_000_000_000, 4 * n * tb * h),
        name='gather_mlp',
    )(own, w_up, w_down, dy.reshape(n // 4, 4 * tb, h))


def copy_kernel(src_ref, dst_ref):
    dst_ref[...] = src_ref[...].reshape(dst_ref.shape)


def copy_half(pair, half):
    n, _, tb, h = pair.shape
    per = min(4, n)
    return pl.pallas_call(
        copy_kernel, grid=(n // per,),
        in_specs=[pl.BlockSpec((per, 1, tb, h), lambda i: (i, half, 0, 0))], out_specs=pl.BlockSpec((per * tb, h), lambda i: (i, 0)),
        out_shape=jax.ShapeDtypeStruct((n * tb, h), pair.dtype),
        cost_estimate=cost(10_000_000, 4 * n * tb * h),
    )(pair)


def out_grad_kernel(ot_ref, src_ref, out_ref, acc):
    i = pl.program_id(0)

    @pl.when(i == 0)
    def _():
        acc[...] = jnp.zeros_like(acc)

    h = src_ref.shape[-1]
    acc[...] += mm(ot_ref[...], src_ref[...].reshape(-1, h), 1, 0)

    @pl.when(i == pl.num_programs(0) - 1)
    def _():
        out_ref[...] = acc[...].astype(BF16)


def out_grad(ot, pair, half):
    n, _, tb, h = pair.shape
    hd = ot.shape[0]
    per = min(4, n)
    return pl.pallas_call(
        out_grad_kernel, grid=(n // per,),
        in_specs=[pl.BlockSpec((hd, per * tb), lambda i: (0, i)), pl.BlockSpec((per, 1, tb, h), lambda i: (i, half, 0, 0))],
        out_specs=pl.BlockSpec((hd, h), zero_map),
        out_shape=jax.ShapeDtypeStruct((hd, h), BF16),
        scratch_shapes=[pltpu.VMEM((hd, h), F32)],
        cost_estimate=cost(2 * n * tb * h * hd, 2 * n * tb * h), name='out_grad',
    )(ot, pair)


def sum_kernel(n, in_ref, out_ref, land, mine, s_send, s_recv, b_send, b_recv):
    me = lax.axis_index('model')
    barrier = pltpu.get_barrier_semaphore()

    def hello(off, _):
        pl.semaphore_signal(barrier, inc=1, device_id={'model': lax.rem(me + off, n)}, device_id_type=MESH)
        return 0

    lax.fori_loop(1, n, hello, 0)
    land[me] = in_ref[me]
    pl.semaphore_wait(barrier, n - 1)

    def scatter(off, slot):
        to = lax.rem(me + off, n)
        return pltpu.make_async_remote_copy(
            in_ref.at[to], land.at[slot], s_send.at[off], s_recv.at[off], device_id={'model': to}, device_id_type=MESH)

    def spread(off, slot):
        return pltpu.make_async_remote_copy(
            mine, out_ref.at[slot], b_send.at[off], b_recv.at[off], device_id={'model': lax.rem(me + off, n)}, device_id_type=MESH)

    def each(body):
        def step(off, _):
            body(off, lax.rem(me - off + n, n))
            return 0

        lax.fori_loop(1, n, step, 0)

    each(lambda off, come: scatter(off, me).start())
    each(lambda off, come: scatter(off, come).wait())
    mine[...] = jnp.sum(land[...], axis=0)
    each(lambda off, come: spread(off, me).start())
    out_ref[me] = mine[...]
    each(lambda off, come: spread(off, come).wait())


def sum_over_devices(n, value, collective_id):
    piece = (1, value.size // n)
    vmem = pl.BlockSpec(memory_space=pltpu.VMEM)
    return pl.pallas_call(
        functools.partial(sum_kernel, n),
        out_shape=jax.ShapeDtypeStruct((n, *piece), F32),
        in_specs=[vmem], out_specs=vmem,
        scratch_shapes=[pltpu.VMEM((n, *piece), F32), pltpu.VMEM(piece, F32)] + [pltpu.SemaphoreType.DMA((n,))] * 4,
        compiler_params=pltpu.CompilerParams(collective_id=collective_id, has_side_effects=True),
        cost_estimate=cost(1_000_000_000, value.size * 8),
        name='gain_sums',
    )(value.reshape(n, *piece)).reshape(value.shape)


def ln_rows(z, gain):
    wide = z.astype(F32)
    mean = jnp.mean(wide, axis=-1, keepdims=True)
    cen = wide - mean
    rstd = lax.rsqrt(jnp.mean(cen * cen, axis=-1, keepdims=True) + LN_EPS)
    hat = cen * rstd
    return (hat * gain.astype(F32)).astype(BF16), hat, rstd


def ln_back(d_out, hat, rstd, gain):
    d_wide = d_out.astype(F32)
    d_hat = d_wide * gain.astype(F32)
    mean_a = jnp.mean(d_hat, axis=-1, keepdims=True)
    mean_b = jnp.mean(d_hat * hat, axis=-1, keepdims=True)
    return (rstd * (d_hat - mean_a - hat * mean_b)).astype(BF16), jnp.sum(d_wide * hat, axis=0)


def solution(mesh):
    n = mesh.shape['model']

    def layer(x_in, seg_ids, gain_one, w_qkv, w_out, gain_two, w_up, w_down, d_y):
        x = x_in[0]
        dy = d_y[0]
        seg = seg_ids[0]
        t, h = x.shape
        n_local, hd = w_out.shape[:2]
        inner = n * n_local * hd
        ts = t // n
        bq = min(512, t)
        bk = min(512, t)
        me = lax.axis_index('model')

        wo_full = lax.all_gather(w_out, 'model', axis=0, tiled=True).reshape(inner, h)

        start = document_starts(seg)
        tab = block_table(seg, start, bq, bk)
        start_row = start.reshape(1, t)

        a_full, q, k, v, qkvt = ln_qkv(x, gain_one, w_qkv.T)
        ot, lse = attention_forward(k, qkvt, start_row, tab, bq, bk)
        o_mine = exchange(n, ot, (n, hd, ts), column_block(ts), leading, 0)

        x_s = lax.dynamic_slice(x, (me * ts, 0), (ts, h))
        dy_s = lax.dynamic_slice(dy, (me * ts, 0), (ts, h))
        proj = mm(o_mine.reshape(inner, ts), wo_full, 0, 0)
        resid = (x_s.astype(F32) + proj).astype(BF16)
        b1_s, hat_two, rstd_two = ln_rows(resid, gain_two)
        b1, gelu_out, d_up = (z.reshape(t, z.shape[-1]) for z in gather_mlp(n, b1_s, w_up, w_down, dy, 6))
        d_b1, part_two = matmul_reduce_scatter(n, [(d_up, w_up, 1), (gelu_out, w_down, 0)], 3)
        d_ln, d_gain_two = ln_back(d_b1, hat_two, rstd_two, gain_two)
        d_resid_s = dy_s + d_ln
        d_w_down = mm(gelu_out, dy, 0, 0).astype(BF16)
        d_w_up = mm(b1, d_up, 0, 0).astype(BF16)

        y_s = (resid.astype(F32) + part_two.astype(F32)).astype(BF16)
        pair = lax.all_gather(jnp.stack([y_s, d_resid_s]), 'model', axis=0, tiled=True).reshape(n, 2, ts, h)
        y_out = copy_half(pair, 0)[None]
        d_heads = mm(wo_full, d_resid_s, 1, 1).astype(BF16).reshape(n, hd, ts)
        dot = exchange(n, d_heads, (hd, t), leading, column_block(ts), 1)

        d_qkv = attention_backward(q, k, v, qkvt, ot, dot, lse, start_row, tab, bq, bk)
        (d_norm,) = matmul_reduce_scatter(n, [(d_qkv, w_qkv.T, 0)], 5)
        d_w_qkv = mm(a_full, d_qkv, 0, 0).astype(BF16)
        d_w_out = out_grad(ot, pair, 1)

        _, hat_one, rstd_one = ln_rows(x_s, gain_one)
        d_ln, d_gain_one = ln_back(d_norm, hat_one, rstd_one, gain_one)
        d_x = lax.all_gather((d_resid_s + d_ln)[None], 'model', axis=1, tiled=True)
        gains = sum_over_devices(n, jnp.concatenate([d_gain_one, d_gain_two]), 2).astype(BF16)
        return (y_out, d_x, d_w_qkv, d_w_out.reshape(n_local, hd, h), d_w_up, d_w_down, gains[:h], gains[h:])

    in_specs = (P('data'), P('data'), P(), P(None, 'model'), P('model'), P(), P(None, 'model'), P('model'), P('data'))
    out_specs = (P('data'), P('data'), P('data', 'model'), P(('data', 'model')), P('data', 'model'), P(('data', 'model')), P('data'), P('data'))
    return jax.shard_map(layer, mesh=mesh, in_specs=in_specs, out_specs=out_specs, check_vma=False)
```

```python
import functools
import math

import jax
import jax.numpy as jnp
from jax import lax
from jax.experimental import pallas as pl
from jax.experimental.pallas import tpu as pltpu
from jax.sharding import PartitionSpec as P


LN_EPS = 1e-5
LOG2E = 1.4426950408889634
NEG = -1e30
MESH = pl.DeviceIdType.MESH
VMEM_LIMIT = 60 * 1024 * 1024
F32 = jnp.float32
BF16 = jnp.bfloat16


def mm(a, b, ca, cb):
    return lax.dot_general(a, b, (((ca,), (cb,)), ((), ())), preferred_element_type=F32)


def cost(flops, moved):
    return pl.CostEstimate(flops=flops, bytes_accessed=moved, transcendentals=0)


def zero_map(*_):
    return (0, 0)


def ln_qkv_kernel(x_ref, g_ref, w_ref, a_ref, q_ref, k_ref, v_ref, t_ref):
    x = x_ref[...].astype(F32)
    mean = jnp.mean(x, axis=-1, keepdims=True)
    cen = x - mean
    var = jnp.mean(cen * cen, axis=-1, keepdims=True)
    a = (cen * lax.rsqrt(var + LN_EPS) * g_ref[...].astype(F32)).astype(BF16)
    a_ref[...] = a
    qkv = mm(a, w_ref[...], 1, 1)
    t_ref[...] = qkv.T.astype(BF16)
    hd = q_ref.shape[1]
    qkv = qkv.astype(BF16)
    q_ref[...] = qkv[:, :hd]
    k_ref[...] = qkv[:, hd:2 * hd]
    v_ref[...] = qkv[:, 2 * hd:]


def ln_qkv(x, g, w):
    t, h = x.shape
    c = w.shape[0]
    hd = c // 3
    bt = min(256, t)
    row = lambda n: pl.BlockSpec((bt, n), lambda i: (i, 0))
    return pl.pallas_call(
        ln_qkv_kernel,
        grid=(t // bt,),
        in_specs=[row(h), pl.BlockSpec((1, h), zero_map), pl.BlockSpec((c, h), zero_map)],
        out_specs=[row(h), row(hd), row(hd), row(hd), pl.BlockSpec((c, bt), lambda i: (0, i))],
        out_shape=[jax.ShapeDtypeStruct((t, h), BF16)] + [jax.ShapeDtypeStruct((t, hd), BF16)] * 3 + [jax.ShapeDtypeStruct((c, t), BF16)],
        compiler_params=pltpu.CompilerParams(vmem_limit_bytes=VMEM_LIMIT),
        cost_estimate=cost(2 * t * h * c + 20 * t * h, 4 * t * h),
        name='ln_qkv',
    )(x, g.reshape(1, h), w)


def visible(kb, bk, q0, bq, start):
    k_pos = kb * bk + lax.broadcasted_iota(jnp.int32, (bk, bq), 0)
    q_pos = q0 + lax.broadcasted_iota(jnp.int32, (bk, bq), 1)
    return (k_pos <= q_pos) & (k_pos >= start)


def masked_block(t, lo, mid, hi):
    return jnp.where(t < mid - lo, lo + t, hi + t - (mid - lo))


def attn_fwd_kernel(bk, tab_ref, k_ref, qt_ref, vt_ref, start_ref, ot_ref, lse_ref):
    i = pl.program_id(0)
    bq = qt_ref.shape[1]
    hd = qt_ref.shape[0]
    scale = LOG2E * hd ** -0.5
    qt = qt_ref[...]
    start = start_ref[...]
    lo, mid, hi, top = tab_ref[0, i], tab_ref[1, i], tab_ref[2, i], tab_ref[3, i]

    def step(masked, kb, carry):
        m, l, acc = carry
        k0 = pl.multiple_of(kb * bk, bk)
        s = mm(k_ref[pl.ds(k0, bk), :], qt, 1, 0)
        if masked:
            s = jnp.where(visible(kb, bk, i * bq, bq, start), s, NEG)
        m_new = jnp.maximum(m, jnp.max(s, axis=0, keepdims=True))
        p = jnp.exp2((s - m_new) * scale)
        alpha = jnp.exp2((m - m_new) * scale)
        l = l * alpha + jnp.sum(p, axis=0, keepdims=True)
        acc = acc * alpha + mm(vt_ref[:, pl.ds(k0, bk)], p.astype(BF16), 1, 0)
        return m_new, l, acc

    carry = (jnp.full((1, bq), NEG, F32), jnp.zeros((1, bq), F32), jnp.zeros((hd, bq), F32))
    carry = lax.fori_loop(mid, hi, functools.partial(step, False), carry)
    m, l, acc = lax.fori_loop(0, mid - lo + top - hi, lambda t, c: step(True, masked_block(t, lo, mid, hi), c), carry)
    ot_ref[...] = (acc / l).astype(BF16)
    lse_ref[...] = m * scale + jnp.log2(l)


def document_starts(seg):
    t = seg.shape[0]
    wide = 128
    pos = jnp.arange(t, dtype=jnp.int32).reshape(t // wide, wide)
    before = jnp.concatenate([seg[:1], seg[:-1]])
    mark = jnp.where((seg != before).reshape(pos.shape), pos, 0)
    lane = jnp.arange(wide)
    inner = jnp.max(jnp.where(lane[None, :, None] >= lane[None, None, :], mark[:, None, :], 0), axis=-1)
    row = jnp.arange(t // wide)
    prior = jnp.max(jnp.where(row[:, None] > row[None, :], inner[:, -1][None, :], 0), axis=-1)
    return jnp.maximum(inner, prior[:, None]).reshape(t)


def block_table(seg, start, bq, bk):
    t = seg.shape[0]
    nq = t // bq
    q0 = jnp.arange(nq, dtype=jnp.int32) * bq
    first = start.reshape(nq, bq)[:, 0]
    last = start.reshape(nq, bq)[:, -1]
    lo = first // bk
    hi = q0 // bk
    top = (q0 + bq + bk - 1) // bk
    mid = jnp.clip((last + bk - 1) // bk, lo, hi)
    return jnp.stack([lo, mid, hi, top])


def attention_forward(k, qkvt, start, tab, bq, bk):
    t, hd = k.shape
    return pl.pallas_call(
        functools.partial(attn_fwd_kernel, bk),
        grid_spec=pltpu.PrefetchScalarGridSpec(
            num_scalar_prefetch=1,
            grid=(t // bq,),
            in_specs=[
                pl.BlockSpec((t, hd), zero_map),
                pl.BlockSpec((hd, bq), lambda i, *_: (0, i)),
                pl.BlockSpec((hd, t), lambda i, *_: (2, 0)),
                pl.BlockSpec((1, bq), lambda i, *_: (0, i)),
            ],
            out_specs=[pl.BlockSpec((hd, bq), lambda i, *_: (0, i)), pl.BlockSpec((1, bq), lambda i, *_: (0, i))],
        ),
        out_shape=[jax.ShapeDtypeStruct((hd, t), BF16), jax.ShapeDtypeStruct((1, t), F32)],
        compiler_params=pltpu.CompilerParams(vmem_limit_bytes=VMEM_LIMIT),
        cost_estimate=cost(16 * t * t * hd, 8 * t * hd),
        name='attn_fwd',
    )(tab, k, qkvt, qkvt, start)


def attn_bwd_kernel(bk, tab_ref, q_ref, k_ref, v_ref, t_ref, ot_ref, dot_ref, lse_ref, start_ref, d_ref, dk_acc, dv_acc):
    i = pl.program_id(0)
    bq, hd = q_ref.shape
    scale = LOG2E * hd ** -0.5
    t = k_ref.shape[0]

    @pl.when(i == 0)
    def _():
        dk_acc[...] = jnp.zeros_like(dk_acc)
        dv_acc[...] = jnp.zeros_like(dv_acc)

    c0 = pl.multiple_of(i * bq, bq)
    q = q_ref[...]
    qt = t_ref[:hd, pl.ds(c0, bq)]
    dot_blk = dot_ref[...]
    dot_wide = dot_blk.astype(F32)
    d_out = dot_wide.T.astype(BF16)
    delta = jnp.sum(dot_wide * ot_ref[...].astype(F32), axis=0, keepdims=True)
    lse = lse_ref[...]
    start = start_ref[...]
    lo, mid, hi, top = tab_ref[0, i], tab_ref[1, i], tab_ref[2, i], tab_ref[3, i]

    def step(masked, kb, dqt):
        k0 = pl.multiple_of(kb * bk, bk)
        rows = pl.ds(k0, bk)
        s = mm(k_ref[rows, :], qt, 1, 0)
        p = jnp.exp2(s * scale - lse)
        if masked:
            p = jnp.where(visible(kb, bk, i * bq, bq, start), p, 0.0)
        dp = mm(v_ref[rows, :], dot_blk, 1, 0)
        ds = (p * (dp - delta)).astype(BF16)
        dv_acc[rows, :] += mm(p.astype(BF16), d_out, 1, 0)
        dk_acc[rows, :] += mm(ds, q, 1, 0)
        return dqt + mm(t_ref[hd:2 * hd, rows], ds, 1, 0)

    dqt = jnp.zeros((hd, bq), F32)
    dqt = lax.fori_loop(mid, hi, functools.partial(step, False), dqt)
    dqt = lax.fori_loop(0, mid - lo + top - hi, lambda t, c: step(True, masked_block(t, lo, mid, hi), c), dqt)
    d_ref[pl.ds(c0, bq), :hd] = (dqt * hd ** -0.5).T.astype(BF16)

    @pl.when(i == pl.num_programs(0) - 1)
    def _():
        def put(r, _):
            rows = pl.ds(pl.multiple_of(r * bk, bk), bk)
            d_ref[rows, hd:2 * hd] = (dk_acc[rows, :] * hd ** -0.5).astype(BF16)
            d_ref[rows, 2 * hd:] = dv_acc[rows, :].astype(BF16)
            return 0

        lax.fori_loop(0, t // bk, put, 0)


def attention_backward(q, k, v, qkvt, ot, dot, lse, start, tab, bq, bk):
    t, hd = k.shape
    whole = lambda shape: pl.BlockSpec(shape, zero_map)
    cols = lambda n: pl.BlockSpec((n, bq), lambda i, *_: (0, i))
    return pl.pallas_call(
        functools.partial(attn_bwd_kernel, bk),
        grid_spec=pltpu.PrefetchScalarGridSpec(
            num_scalar_prefetch=1,
            grid=(t // bq,),
            in_specs=[
                pl.BlockSpec((bq, hd), lambda i, *_: (i, 0)), whole((t, hd)), whole((t, hd)), whole((3 * hd, t)),
                cols(hd), cols(hd), cols(1), cols(1),
            ],
            out_specs=whole((t, 3 * hd)),
            scratch_shapes=[pltpu.VMEM((t, hd), F32), pltpu.VMEM((t, hd), F32)],
        ),
        out_shape=jax.ShapeDtypeStruct((t, 3 * hd), BF16),
        compiler_params=pltpu.CompilerParams(vmem_limit_bytes=VMEM_LIMIT),
        cost_estimate=cost(40 * t * t * hd, 16 * t * hd),
        name='attn_bwd',
    )(tab, q, k, v, qkvt, ot, dot, lse, start)


def exchange_kernel(n, src_of, dst_of, in_ref, out_ref, send_sem, recv_sem, own_sem):
    me = lax.axis_index('model')
    barrier = pltpu.get_barrier_semaphore()

    def hello(off, _):
        pl.semaphore_signal(barrier, inc=1, device_id={'model': lax.rem(me + off, n)}, device_id_type=MESH)
        return 0

    lax.fori_loop(1, n, hello, 0)
    own = pltpu.make_async_copy(src_of(in_ref, me), dst_of(out_ref, me), own_sem)
    own.start()
    pl.semaphore_wait(barrier, n - 1)

    def send(off, _):
        to = lax.rem(me + off, n)
        pltpu.make_async_remote_copy(
            src_ref=src_of(in_ref, to), dst_ref=dst_of(out_ref, me), send_sem=send_sem.at[off], recv_sem=recv_sem.at[off],
            device_id={'model': to}, device_id_type=MESH,
        ).start()
        return 0

    lax.fori_loop(1, n, send, 0)

    def finish(off, _):
        to = lax.rem(me + off, n)
        come = lax.rem(me - off + n, n)
        pltpu.make_async_remote_copy(
            src_ref=src_of(in_ref, to), dst_ref=dst_of(out_ref, come), send_sem=send_sem.at[off], recv_sem=recv_sem.at[off],
            device_id={'model': to}, device_id_type=MESH,
        ).wait()
        return 0

    lax.fori_loop(1, n, finish, 0)
    own.wait()


def exchange(n, value, out_shape, src_of, dst_of, collective_id):
    return pl.pallas_call(
        functools.partial(exchange_kernel, n, src_of, dst_of),
        out_shape=jax.ShapeDtypeStruct(out_shape, value.dtype),
        in_specs=[pl.BlockSpec(memory_space=pltpu.VMEM)],
        out_specs=pl.BlockSpec(memory_space=pltpu.VMEM),
        scratch_shapes=[pltpu.SemaphoreType.DMA((n,)), pltpu.SemaphoreType.DMA((n,)), pltpu.SemaphoreType.DMA],
        compiler_params=pltpu.CompilerParams(collective_id=collective_id, has_side_effects=True),
        cost_estimate=cost(2_000_000_000, 2 * value.size * 2),
    )(value)


def column_block(width):
    return lambda ref, j: ref.at[:, pl.ds(pl.multiple_of(j * width, width), width)]


def leading(ref, j):
    return ref.at[j]


def ring_place(n, q):
    me = lax.axis_index('model')
    side = math.isqrt(n // 2)
    core = lax.rem(me, 2)
    chip = me // 2
    x = lax.rem(chip, side)
    y = chip // side
    turn = q // 2
    sign = 1 - 2 * lax.rem(q, 2)
    a = x * (1 - turn) + y * turn
    b = y * (1 - turn) + x * turn

    def chip_at(pa, pb):
        pa = lax.rem(pa + 2 * side, side)
        pb = lax.rem(pb + 2 * side, side)
        return (pb * (1 - turn) + pa * turn) * side + pa * (1 - turn) + pb * turn

    return side, core, sign, a, b, chip_at


def greet_neighbours(n):
    me = lax.axis_index('model')
    barrier = pltpu.get_barrier_semaphore()
    core = lax.rem(me, 2)
    pl.semaphore_signal(barrier, inc=1, device_id={'model': me + 1 - 2 * core}, device_id_type=MESH)

    def hello(q, _):
        _, core, sign, a, b, chip_at = ring_place(n, q)
        pl.semaphore_signal(barrier, inc=1, device_id={'model': chip_at(a + sign, b) * 2 + core}, device_id_type=MESH)
        return 0

    lax.fori_loop(0, 4, hello, 0)
    pl.semaphore_wait(barrier, 5)


class Reduction:
    def __init__(self, n, r_dim, l_ref, r_ref, out_ref, scratch):
        self.n, self.r_dim, self.l_ref, self.r_ref, self.out_ref = n, r_dim, l_ref, r_ref, out_ref
        (self.l_peer, self.r_peer, self.part, self.first, self.slot1, self.slot2,
         self.s_send, self.s_recv, self.p_send, self.p_recv, self.x_send, self.x_recv) = scratch
        self.side, _, _, self.tb, self.k = l_ref.shape
        self.width = out_ref.shape[1] // 4
        me = lax.axis_index('model')
        self.my_core = lax.rem(me, 2)
        peer = {'model': me + 1 - 2 * self.my_core}
        pairs = [(r_ref, self.r_peer), (l_ref.at[:, :, 1 - self.my_core], self.l_peer)]
        self.swap = [
            pltpu.make_async_remote_copy(src, dst, self.x_send.at[i], self.x_recv.at[i], device_id=peer, device_id_type=MESH)
            for i, (src, dst) in enumerate(pairs)
        ]

    def wrap(self, pos):
        return lax.rem(pos + 2 * self.side, self.side)

    def group(self, s, q):
        _, _, sign, a, _, _ = ring_place(self.n, q)
        at = self.wrap(a - sign * (1 + s))
        l_ref, l_peer, core = self.l_ref, self.l_peer, self.my_core
        mine, other = (l_ref[:, at, core], l_peer[:, at]) if q < 2 else (l_ref[at, :, core], l_peer[at])
        cols = pl.ds(q * self.width, self.width)
        at_r = (slice(None), cols) if self.r_dim == 0 else (cols, slice(None))
        flat = (self.side * self.tb, self.k)
        total = mm(mine.reshape(flat), self.r_ref[at_r], 1, self.r_dim) + mm(other.reshape(flat), self.r_peer[at_r], 1, self.r_dim)
        self.part[lax.rem(s, 2), q] = total.reshape(self.side, self.tb, self.width)

    def own_part(self, q, s, j):
        _, _, sign, _, b, _ = ring_place(self.n, q)
        return self.part[lax.rem(s, 2), q, self.wrap(b - sign * (1 + j))]

    def hop(self, q, s, j, src):
        _, core, sign, a, b, chip_at = ring_place(self.n, q)
        at = self.arrived(q, s, j)
        return pltpu.make_async_remote_copy(
            src, self.slot1.at[at], self.s_send.at[at], self.s_recv.at[at],
            device_id={'model': chip_at(a + sign, b) * 2 + core}, device_id_type=MESH)

    def turn_hop(self, q, s, src):
        _, core, sign, a, b, chip_at = ring_place(self.n, q)
        at = q * (self.side - 1) + s
        return pltpu.make_async_remote_copy(
            src, self.slot2.at[at], self.p_send.at[at], self.p_recv.at[at],
            device_id={'model': chip_at(a, b + sign) * 2 + core}, device_id_type=MESH)

    def arrived(self, q, s, j):
        return (q * (self.side - 1) + s) * self.side + j

    def received(self, q, s, j):
        slot = self.slot1.at[self.arrived(q, s - 1, j)]
        self.hop(q, s - 1, j, slot).wait_recv()
        return slot, slot[...].astype(F32) + self.own_part(q, s, j)

    def middle_round(self, t):
        s, rest = t // (4 * self.side) - 1, lax.rem(t, 4 * self.side)
        j, q = rest // 4, lax.rem(rest, 4)

        @pl.when(s == 0)
        def _():
            src = self.first.at[q * self.side + j]
            src[...] = self.own_part(q, s, j).astype(BF16)
            self.hop(q, s, j, src).start()

        @pl.when(s > 0)
        def _():
            slot, total = self.received(q, s, j)
            slot[...] = total.astype(BF16)
            self.hop(q, s, j, slot).start()

        for ahead in range(4):
            @pl.when((q == 3) & (j == ahead))
            def _():
                self.group(s + 1, ahead)

    def turn_first(self, q):
        slot, total = self.received(q, self.side - 1, 0)
        slot[...] = total.astype(BF16)
        self.turn_hop(q, 0, slot).start()

    def turned(self, q, s):
        _, total = self.received(q, self.side - 1, s)
        slot = self.slot2.at[q * (self.side - 1) + s - 1]
        self.turn_hop(q, s - 1, slot).wait_recv()
        return slot, slot[...].astype(F32) + total

    def turn_round(self, t):
        s, q = 1 + t // 4, lax.rem(t, 4)
        slot, total = self.turned(q, s)
        slot[...] = total.astype(BF16)
        self.turn_hop(q, s, slot).start()

    def turn_last(self, q):
        _, total = self.turned(q, self.side - 1)
        self.out_ref[:, pl.ds(pl.multiple_of(q * self.width, self.width), self.width)] = total.astype(BF16)

    def drain(self, t):
        q, s = t // (self.side - 1), lax.rem(t, self.side - 1)
        self.turn_hop(q, s, self.slot2.at[t]).wait_send()
        for j in range(self.side):
            self.hop(q, s, j, self.slot1.at[t * self.side + j]).wait_send()


def reduce_kernel(n, r_dims, *refs):
    m = len(r_dims)
    lefts, rights, outs = refs[:m], refs[m:2 * m], refs[2 * m:3 * m]
    rest = refs[3 * m:]
    each = len(rest) // m
    todo = [
        Reduction(n, r_dims[i], lefts[i], rights[i], outs[i], rest[i * each:(i + 1) * each]) for i in range(m)
    ]
    side = todo[0].side
    greet_neighbours(n)
    for job in todo:
        for copy in job.swap:
            copy.start()
    for job in todo:
        for copy in job.swap:
            copy.wait()
    loop(4 * side * side, [job.middle_round for job in todo])
    loop(4, [job.turn_first for job in todo])
    loop(4 * (side - 2), [job.turn_round for job in todo])
    loop(4, [job.turn_last for job in todo])
    loop(4 * (side - 1), [job.drain for job in todo])


def loop(count, bodies):
    def step(t, _):
        for body in bodies:
            body(t)
        return 0

    lax.fori_loop(0, count, step, 0)


def matmul_reduce_scatter(n, jobs, collective_id):
    chips = n // 2
    side = math.isqrt(chips)
    hops = 4 * (side - 1)
    vmem = pl.BlockSpec(memory_space=pltpu.VMEM)
    lefts, rights, outs, scratch = [], [], [], []
    for left, right, r_dim in jobs:
        t, k = left.shape
        f, tb = right.shape[1 - r_dim], t // n
        lefts.append(left.reshape(side, side, 2, tb, k))
        rights.append(right)
        outs.append(jax.ShapeDtypeStruct((tb, f), BF16))
        piece = (tb, f // 4)
        scratch += [
            pltpu.VMEM((side, side, tb, k), BF16), pltpu.VMEM(right.shape, BF16), pltpu.VMEM((2, 4, side, *piece), F32),
            pltpu.VMEM((4 * side, *piece), BF16), pltpu.VMEM((hops * side, *piece), BF16), pltpu.VMEM((hops, *piece), BF16),
        ] + [pltpu.SemaphoreType.DMA((c,)) for c in (hops * side, hops * side, hops, hops, 2, 2)]
    return pl.pallas_call(
        functools.partial(reduce_kernel, n, [r_dim for _, _, r_dim in jobs]),
        out_shape=outs,
        in_specs=[vmem] * (2 * len(jobs)),
        out_specs=[vmem] * len(jobs),
        scratch_shapes=scratch,
        compiler_params=pltpu.CompilerParams(collective_id=collective_id, has_side_effects=True, vmem_limit_bytes=VMEM_LIMIT),
        cost_estimate=cost(40_000_000_000, 4 * t * k),
    )(*lefts, *rights)


def gelu_parts(up):
    c = math.sqrt(2.0 / math.pi)
    sq = up * up
    th = jnp.tanh(c * (up + 0.044715 * (sq * up)))
    cdf = 0.5 + 0.5 * th
    slope = cdf + up * (0.5 * (1.0 - th * th)) * (c + (3 * 0.044715 * c) * sq)
    return up * cdf, slope


def gather_mlp_kernel(n, own_ref, up_ref, down_ref, dy_ref, b1_ref, gelu_ref, d_up_ref,
                      b1, acc, dg, dy_buf, a_send, a_recv, b_send, b_recv, x_send, x_recv, dy_sem, out_sem):
    me = lax.axis_index('model')
    my_core = lax.rem(me, 2)
    tb, h = own_ref.shape
    f = up_ref.shape[1]
    width = h // 4
    side = math.isqrt(n // 2)
    rounds = side * side
    n_dy, _, _ = dy_ref.shape
    peer = {'model': me + 1 - 2 * my_core}

    def dy_copy(t):
        return pltpu.make_async_copy(dy_ref.at[t], dy_buf.at[lax.rem(t, 2)], dy_sem.at[lax.rem(t, 2)])

    dy_copy(jnp.int32(0)).start()
    dy_copy(jnp.int32(1)).start()
    greet_neighbours(n)

    def cols_of(q):
        return pl.ds(pl.multiple_of(q * width, width), width)

    def quarter(q, r, core):
        _, _, sign, a, b, chip_at = ring_place(n, q)
        chip = chip_at(a - sign * lax.rem(r, side), b - sign * (r // side))
        return b1.at[chip // side, lax.rem(chip, side), core, :, cols_of(q)]

    def along_a(q, j, src):
        _, core, sign, a, b, chip_at = ring_place(n, q)
        at = q * (side - 1) + j
        return pltpu.make_async_remote_copy(
            src, quarter(q, j, core), a_send.at[at], a_recv.at[at], device_id={'model': chip_at(a + sign, b) * 2 + core}, device_id_type=MESH)

    def along_b(q, r, src):
        _, core, sign, a, b, chip_at = ring_place(n, q)
        at = q * (rounds - side) + r
        return pltpu.make_async_remote_copy(
            src, quarter(q, r, core), b_send.at[at], b_recv.at[at], device_id={'model': chip_at(a, b + sign) * 2 + core}, device_id_type=MESH)

    def across(q, r, src, core):
        at = q * rounds + r
        return pltpu.make_async_remote_copy(
            src, quarter(q, r, core), x_send.at[at], x_recv.at[at], device_id=peer, device_id_type=MESH)

    def back_proj(t):
        dy_copy(t).wait()
        dg[t] = mm(dy_buf[lax.rem(t, 2)], down_ref[...], 1, 1).astype(BF16)

        @pl.when(t + 2 < n_dy)
        def _():
            dy_copy(t + 2).start()

    def own_round(q, _):
        src = own_ref.at[:, cols_of(q)]
        along_a(q, 0, src).start()
        along_b(q, 0, src).start()
        across(q, 0, src, my_core).start()
        return 0

    lax.fori_loop(0, 4, own_round, 0)
    b1[me // (2 * side), lax.rem(me // 2, side), my_core] = own_ref[...]
    acc[...] = jnp.zeros_like(acc)

    def add_up(s, q, core):
        _, _, sign, _, b, _ = ring_place(n, q)
        at = lax.rem(b - sign * s + 2 * side, side)
        cols = pl.ds(q * width, width)
        if q < 2:
            pltpu.make_async_copy(b1.at[at, :, core, :, cols], b1_ref.at[at, :, core, :, cols], out_sem).start()
            value = b1[at, :, core, :, cols].reshape(side * tb, width)
        else:
            pltpu.make_async_copy(b1.at[:, at, core, :, cols], b1_ref.at[:, at, core, :, cols], out_sem).start()
            value = b1[:, at, core, :, cols].reshape(side * tb, width)
        more = mm(value, up_ref[cols, :], 1, 0).reshape(side, tb, f)
        if q < 2:
            acc[at, :, core] += more
        else:
            acc[:, at, core] += more

    def take_step(s, q):
        add_up(s, q, my_core)
        for j in range(side):
            r = s * side + j
            across(q, r, quarter(q, r, 1 - my_core), 1 - my_core).wait_recv()
        add_up(s, q, 1 - my_core)

    def main_round(t, _):
        r, q = t // 4, lax.rem(t, 4)
        s, j = r // side, lax.rem(r, side)
        src = quarter(q, r, my_core)

        @pl.when(s == 0)
        def _():
            along_a(q, j - 1, src).wait_recv()

            @pl.when(j < side - 1)
            def _():
                along_a(q, j, src).start()

        @pl.when((s > 0) & (s < side))
        def _():
            along_b(q, r - side, src).wait_recv()

        @pl.when(s < side - 1)
        def _():
            along_b(q, r, src).start()

        @pl.when(s < side)
        def _():
            across(q, r, src, my_core).start()

        for late in range(4):
            @pl.when((q == 3) & (j == late) & (s > 0))
            def _():
                take_step(s - 1, late)

        @pl.when((q == 1) & (lax.rem(r, 2) == 1) & (s < side))
        def _():
            back_proj(r // 2)

        return 0

    lax.fori_loop(4, 4 * (rounds + side), main_round, 0)

    def activate(t, _):
        chip, core = t // 2, lax.rem(t, 2)
        piece, rows = t // 4, pl.ds(pl.multiple_of(lax.rem(t, 4) * tb, tb), tb)
        up = acc[chip // side, lax.rem(chip, side), core].astype(BF16).astype(F32)
        value, slope = gelu_parts(up)
        gelu_ref[piece, rows, :] = value.astype(BF16)
        d_up_ref[piece, rows, :] = (dg[piece, rows, :].astype(F32) * slope).astype(BF16)
        return 0

    lax.fori_loop(0, n, activate, 0)

    def drain(t, _):
        q, r = t // rounds, lax.rem(t, rounds)
        src = quarter(q, r, my_core)
        across(q, r, src, my_core).wait_send()

        @pl.when(r < rounds - side)
        def _():
            along_b(q, r, src).wait_send()

        @pl.when(r < side - 1)
        def _():
            along_a(q, r, src).wait_send()

        return 0

    lax.fori_loop(0, 4 * rounds, drain, 0)
    pltpu.make_async_copy(b1, b1_ref, out_sem).wait()


def gather_mlp(n, own, w_up, w_down, dy, collective_id):
    tb, h = own.shape
    f = w_up.shape[1]
    side = math.isqrt(n // 2)
    rounds = side * side
    vmem = pl.BlockSpec(memory_space=pltpu.VMEM)
    anyspace = pl.BlockSpec(memory_space=pl.ANY)
    a_hops, b_hops, x_hops = 4 * (side - 1), 4 * (rounds - side), 4 * rounds
    sems = [pltpu.SemaphoreType.DMA((k,)) for k in (a_hops, a_hops, b_hops, b_hops, x_hops, x_hops, 2)]
    return pl.pallas_call(
        functools.partial(gather_mlp_kernel, n),
        out_shape=[
            jax.ShapeDtypeStruct((side, side, 2, tb, h), BF16), jax.ShapeDtypeStruct((n // 4, 4 * tb, f), BF16), jax.ShapeDtypeStruct((n // 4, 4 * tb, f), BF16),
        ],
        in_specs=[vmem, vmem, vmem, anyspace],
        out_specs=[anyspace, vmem, vmem],
        scratch_shapes=[
            pltpu.VMEM((side, side, 2, tb, h), BF16), pltpu.VMEM((side, side, 2, tb, f), F32),
            pltpu.VMEM((n // 4, 4 * tb, f), BF16), pltpu.VMEM((2, 4 * tb, h), BF16),
            *sems, pltpu.SemaphoreType.DMA,
        ],
        compiler_params=pltpu.CompilerParams(collective_id=collective_id, has_side_effects=True, vmem_limit_bytes=50 * 1024 * 1024),
        cost_estimate=cost(40_000_000_000, 4 * n * tb * h),
        name='gather_mlp',
    )(own, w_up, w_down, dy.reshape(n // 4, 4 * tb, h))


def copy_kernel(src_ref, dst_ref):
    dst_ref[...] = src_ref[...].reshape(dst_ref.shape)


def copy_half(pair, half):
    n, _, tb, h = pair.shape
    per = min(2, n)
    return pl.pallas_call(
        copy_kernel, grid=(n // per,),
        in_specs=[pl.BlockSpec((per, 1, tb, h), lambda i: (i, half, 0, 0))], out_specs=pl.BlockSpec((per * tb, h), lambda i: (i, 0)),
        out_shape=jax.ShapeDtypeStruct((n * tb, h), pair.dtype),
        cost_estimate=cost(10_000_000, 4 * n * tb * h),
    )(pair)


def out_grad_kernel(ot_ref, src_ref, out_ref, acc):
    i = pl.program_id(0)

    @pl.when(i == 0)
    def _():
        acc[...] = jnp.zeros_like(acc)

    h = src_ref.shape[-1]
    acc[...] += mm(ot_ref[...], src_ref[...].reshape(-1, h), 1, 0)

    @pl.when(i == pl.num_programs(0) - 1)
    def _():
        out_ref[...] = acc[...].astype(BF16)


def out_grad(ot, pair, half):
    n, _, tb, h = pair.shape
    hd = ot.shape[0]
    per = min(2, n)
    return pl.pallas_call(
        out_grad_kernel, grid=(n // per,),
        in_specs=[pl.BlockSpec((hd, per * tb), lambda i: (0, i)), pl.BlockSpec((per, 1, tb, h), lambda i: (i, half, 0, 0))],
        out_specs=pl.BlockSpec((hd, h), zero_map),
        out_shape=jax.ShapeDtypeStruct((hd, h), BF16),
        scratch_shapes=[pltpu.VMEM((hd, h), F32)],
        cost_estimate=cost(2 * n * tb * h * hd, 2 * n * tb * h), name='out_grad',
    )(ot, pair)


def sum_kernel(n, in_ref, out_ref, land, mine, s_send, s_recv, b_send, b_recv):
    me = lax.axis_index('model')
    barrier = pltpu.get_barrier_semaphore()

    def hello(off, _):
        pl.semaphore_signal(barrier, inc=1, device_id={'model': lax.rem(me + off, n)}, device_id_type=MESH)
        return 0

    lax.fori_loop(1, n, hello, 0)
    land[me] = in_ref[me]
    pl.semaphore_wait(barrier, n - 1)

    def scatter(off, slot):
        to = lax.rem(me + off, n)
        return pltpu.make_async_remote_copy(
            in_ref.at[to], land.at[slot], s_send.at[off], s_recv.at[off], device_id={'model': to}, device_id_type=MESH)

    def spread(off, slot):
        return pltpu.make_async_remote_copy(
            mine, out_ref.at[slot], b_send.at[off], b_recv.at[off], device_id={'model': lax.rem(me + off, n)}, device_id_type=MESH)

    def each(body):
        def step(off, _):
            body(off, lax.rem(me - off + n, n))
            return 0

        lax.fori_loop(1, n, step, 0)

    each(lambda off, come: scatter(off, me).start())
    each(lambda off, come: scatter(off, come).wait())
    mine[...] = jnp.sum(land[...], axis=0)
    each(lambda off, come: spread(off, me).start())
    out_ref[me] = mine[...]
    each(lambda off, come: spread(off, come).wait())


def sum_over_devices(n, value, collective_id):
    piece = (1, value.size // n)
    vmem = pl.BlockSpec(memory_space=pltpu.VMEM)
    return pl.pallas_call(
        functools.partial(sum_kernel, n),
        out_shape=jax.ShapeDtypeStruct((n, *piece), F32),
        in_specs=[vmem], out_specs=vmem,
        scratch_shapes=[pltpu.VMEM((n, *piece), F32), pltpu.VMEM(piece, F32)] + [pltpu.SemaphoreType.DMA((n,))] * 4,
        compiler_params=pltpu.CompilerParams(collective_id=collective_id, has_side_effects=True),
        cost_estimate=cost(1_000_000_000, value.size * 8),
        name='gain_sums',
    )(value.reshape(n, *piece)).reshape(value.shape)


def ln_rows(z, gain):
    wide = z.astype(F32)
    mean = jnp.mean(wide, axis=-1, keepdims=True)
    cen = wide - mean
    rstd = lax.rsqrt(jnp.mean(cen * cen, axis=-1, keepdims=True) + LN_EPS)
    hat = cen * rstd
    return (hat * gain.astype(F32)).astype(BF16), hat, rstd


def ln_back(d_out, hat, rstd, gain):
    d_wide = d_out.astype(F32)
    d_hat = d_wide * gain.astype(F32)
    mean_a = jnp.mean(d_hat, axis=-1, keepdims=True)
    mean_b = jnp.mean(d_hat * hat, axis=-1, keepdims=True)
    return (rstd * (d_hat - mean_a - hat * mean_b)).astype(BF16), jnp.sum(d_wide * hat, axis=0)


def solution(mesh):
    n = mesh.shape['model']

    def layer(x_in, seg_ids, gain_one, w_qkv, w_out, gain_two, w_up, w_down, d_y):
        x = x_in[0]
        dy = d_y[0]
        seg = seg_ids[0]
        t, h = x.shape
        n_local, hd = w_out.shape[:2]
        inner = n * n_local * hd
        ts = t // n
        bq = min(512, t)
        bk = min(512, t)
        me = lax.axis_index('model')

        wo_full = lax.all_gather(w_out, 'model', axis=0, tiled=True).reshape(inner, h)

        start = document_starts(seg)
        tab = block_table(seg, start, bq, bk)
        start_row = start.reshape(1, t)

        a_full, q, k, v, qkvt = ln_qkv(x, gain_one, w_qkv.T)
        ot, lse = attention_forward(k, qkvt, start_row, tab, bq, bk)
        o_mine = exchange(n, ot, (n, hd, ts), column_block(ts), leading, 0)

        x_s = lax.dynamic_slice(x, (me * ts, 0), (ts, h))
        dy_s = lax.dynamic_slice(dy, (me * ts, 0), (ts, h))
        proj = mm(o_mine.reshape(inner, ts), wo_full, 0, 0)
        resid = (x_s.astype(F32) + proj).astype(BF16)
        b1_s, hat_two, rstd_two = ln_rows(resid, gain_two)
        b1, gelu_out, d_up = (z.reshape(t, z.shape[-1]) for z in gather_mlp(n, b1_s, w_up, w_down, dy, 6))
        d_b1, part_two = matmul_reduce_scatter(n, [(d_up, w_up, 1), (gelu_out, w_down, 0)], 3)
        d_ln, d_gain_two = ln_back(d_b1, hat_two, rstd_two, gain_two)
        d_resid_s = dy_s + d_ln
        d_w_down = mm(gelu_out, dy, 0, 0).astype(BF16)
        d_w_up = mm(b1, d_up, 0, 0).astype(BF16)

        y_s = (resid.astype(F32) + part_two.astype(F32)).astype(BF16)
        pair = lax.all_gather(jnp.stack([y_s, d_resid_s]), 'model', axis=0, tiled=True).reshape(n, 2, ts, h)
        y_out = copy_half(pair, 0)[None]
        d_heads = mm(wo_full, d_resid_s, 1, 1).astype(BF16).reshape(n, hd, ts)
        dot = exchange(n, d_heads, (hd, t), leading, column_block(ts), 1)

        d_qkv = attention_backward(q, k, v, qkvt, ot, dot, lse, start_row, tab, bq, bk)
        (d_norm,) = matmul_reduce_scatter(n, [(d_qkv, w_qkv.T, 0)], 5)
        d_w_qkv = mm(a_full, d_qkv, 0, 0).astype(BF16)
        d_w_out = out_grad(ot, pair, 1)

        _, hat_one, rstd_one = ln_rows(x_s, gain_one)
        d_ln, d_gain_one = ln_back(d_norm, hat_one, rstd_one, gain_one)
        d_x = lax.all_gather((d_resid_s + d_ln)[None], 'model', axis=1, tiled=True)
        gains = sum_over_devices(n, jnp.concatenate([d_gain_one, d_gain_two]), 2).astype(BF16)
        return (y_out, d_x, d_w_qkv, d_w_out.reshape(n_local, hd, h), d_w_up, d_w_down, gains[:h], gains[h:])

    in_specs = (P('data'), P('data'), P(), P(None, 'model'), P('model'), P(), P(None, 'model'), P('model'), P('data'))
    out_specs = (P('data'), P('data'), P('data', 'model'), P(('data', 'model')), P('data', 'model'), P(('data', 'model')), P('data'), P('data'))
    return jax.shard_map(layer, mesh=mesh, in_specs=in_specs, out_specs=out_specs, check_vma=False)
```
